256 devices in a mesh: space: 32 (over y, z_lo, core), scene: 8 (over x, z_hi).
Axes of the slice: x: 4, y: 4, z: 8 (z_hi: 2, z_lo: 4; z = z_hi * 4 + z_lo), core: 2. Of those that a mesh axis runs over, the one named last changes fastest.
Arguments:
- grad_out: bfloat16 [8, 64, 128, 256], P('scene', 'space'), may hold values from -6 to 6
- pre_second: bfloat16 [8, 64, 128, 256], P('scene', 'space'), may hold values from -6 to 6
- pre_first: bfloat16 [8, 64, 128, 256], P('scene', 'space'), may hold values from -6 to 6
- camera_bev: bfloat16 [8, 64, 128, 80], P('scene', 'space'), may hold values from -6 to 6
- lidar_bev: bfloat16 [8, 64, 128, 256], P('scene', 'space'), may hold values from -6 to 6
- weight_a: bfloat16 [256, 3024], replicated, may hold values from -0.109375 to 0.109375
- weight_b: bfloat16 [256, 2304], replicated, may hold values from -0.125 to 0.125
- depth_weights: bfloat16 [8, 118, 4096], P('scene', None, 'space'), may hold values from 0 to 1
- context: bfloat16 [8, 80, 4096], P('scene', None, 'space'), may hold values from -6 to 6
- block_list: int32 [32, 32, 1], P(None, 'space'), may hold values from -1 to 1, as said below
- point_slot: int32 [118, 4096], P(None, 'space'), may hold values from 0 to 4095, as said below
Outputs:
- weight_grad_a: float32 [256, 3024], P('space')
- weight_grad_b: float32 [256, 2304], P('space')
- grad_lidar: bfloat16 [8, 64, 128, 256], P('scene', 'space')
- grad_context: float32 [8, 80, 4096], P('scene', None, 'space')
- grad_depth: float32 [8, 118, 4096], P('scene', None, 'space')
The draws below stay inside these ranges and needn't reach their ends.
Inputs may be any that keep to these rules, and one draw needn't show every extreme that they name: block_list[d, s, k] is a block of 128 cells of device s's rows owed to frustum owner d, distinct within (d, s), or -1 for an empty slot; live slots come first; every owner has a live slot from itself; in every draw some owner has all 1 slots live from every device. point_slot[d, p] = (s + k) * 128 + q names cell q of the block in a live slot k from device s, for the owner of pixel p.
All inputs are finite; a program needn't handle non-finite values.
Results may differ from the reference program's by a relative error of at most 0.005.
Values may be sent and summed in bfloat16 or wider, within the bound.
No kernel may reach another device: no remote copies, remote signals or barrier semaphores. Data moves between devices by JAX's collectives and lax.ppermute only.
A program may use at most 64 MiB of HBM per device.

```python
import math
import jax
import jax.numpy as jnp
from jax import lax

CH = 256
LID = 256
CAM = 80
DEPTH = 118
ROWS_DEV = 2
COLS = 128
PIX_DEV = 128
BLOCK = 128
SLOTS = 1
ROWS = 64
PIX = 4096
SCENES = 8
N_SPACE = 32


def routing_tables(key):
    key = jax.random.fold_in(key, 1234)
    key_list = jax.random.split(key, 5)
    block_count = ROWS_DEV * COLS // BLOCK
    device_count = N_SPACE
    base_counts = jax.random.randint(key_list[0], (device_count, device_count), 0, SLOTS)
    base_counts = jnp.maximum(base_counts, jnp.eye(device_count, dtype=jnp.int32))
    heavy_owner = jax.random.randint(key_list[1], (device_count,), 0, 4) == 0
    forced_owner = jax.random.randint(key_list[2], (), 0, device_count)
    heavy_owner = jnp.logical_or(heavy_owner, jnp.arange(device_count) == forced_owner)
    slot_counts = jnp.where(heavy_owner[:, None], SLOTS, base_counts)
    block_scores = jax.random.randint(key_list[3], (device_count, device_count, block_count), 0, 1 << 20) * block_count + jnp.arange(block_count)
    block_order = jnp.argsort(block_scores, axis=-1)[..., :SLOTS].astype(jnp.int32)
    is_live = jnp.arange(SLOTS)[None, None, :] < slot_counts[..., None]
    listing = jnp.where(is_live, block_order, -1)
    flat_live = is_live.reshape(device_count, device_count * SLOTS)
    live_first = jnp.argsort(jnp.where(flat_live, 0, 1) * (device_count * SLOTS) + jnp.arange(device_count * SLOTS), axis=-1).astype(jnp.int32)
    live_total = jnp.sum(slot_counts, axis=1)
    raw_draws = jax.random.randint(key_list[4], (DEPTH, device_count, PIX_DEV), 0, 1 << 30)
    picked_cells = raw_draws % (live_total[None, :, None] * BLOCK)
    live_position = jnp.take_along_axis(jnp.broadcast_to(live_first[None], (DEPTH, device_count, device_count * SLOTS)), picked_cells // BLOCK, axis=2)
    point_index = live_position * BLOCK + picked_cells % BLOCK
    return (listing.astype(jnp.int32), point_index.reshape(DEPTH, device_count * PIX_DEV).astype(jnp.int32))


def draw_block_list(key, part):
    return routing_tables(key)[0]


def draw_point_slot(key, part):
    return routing_tables(key)[1]


def spiked(array, own_key, source, target, blocks, factor):
    def block_of(position):
        return (jnp.arange(array.shape[position]) // (array.shape[position] // blocks)).reshape((-1,) + (1,) * (array.ndim - 1 - position))

    one_side = jax.random.permutation(own_key, blocks)[block_of(target)]
    other_side = (block_of(target) + blocks // 2) % blocks
    return jnp.where((block_of(source) == one_side) | (block_of(source) == other_side), factor * array, array)


def shard_levels(own_key, shape, cuts, low, high):
    loudness, own = 1.0, jax.random.fold_in(own_key, 6)
    for position, shards_of in cuts:
        heights = jnp.exp(jax.random.uniform(jax.random.fold_in(own, position), (shards_of,), jnp.float32, low / len(cuts), high / len(cuts)))
        loudness = loudness * jnp.repeat(heights, shape[position] // shards_of).reshape([-1 if axis == position else 1 for axis in range(len(shape))])
    return loudness


def bell_draw(key, dims, deviation, most, cuts=(), held_as=jnp.bfloat16):
    factor_of = shard_levels(key, dims, cuts, -0.22, 0.18) if cuts else 1.0
    drawn = jax.random.normal(key, dims, jnp.float32) * deviation * factor_of
    return jnp.minimum(jnp.maximum(drawn, -most), most).astype(held_as)


def bell_draw_with(stream_key, dims, spread, bound, cuts, heavy, kind=jnp.bfloat16):
    drawn = spread * jax.random.normal(stream_key, dims, jnp.float32)
    if cuts:
        drawn = drawn * shard_levels(stream_key, dims, cuts, -0.22, 0.18)
    return jnp.clip(spiked(drawn, jax.random.fold_in(stream_key, 3), *heavy), -bound, bound).astype(kind)


def setup_inputs(seed: int = 0) -> dict:
    key_of = jax.random.split(jax.random.key(seed), 12)
    return {
        "grad_out": bell_draw_with(key_of[0], (SCENES, ROWS, COLS, CH), 1.0, 6.0, ((0, 8), (1, 32)), (1, 3, 32, 2.75)),
        "pre_second": bell_draw(key_of[1], (SCENES, ROWS, COLS, CH), 1.0, 6.0, ((0, 8), (1, 32))),
        "pre_first": bell_draw(key_of[2], (SCENES, ROWS, COLS, CH), 1.0, 6.0, ((0, 8), (1, 32))),
        "camera_bev": bell_draw(key_of[3], (SCENES, ROWS, COLS, CAM), 1.0, 6.0, ((0, 8), (1, 32))),
        "lidar_bev": bell_draw(key_of[4], (SCENES, ROWS, COLS, LID), 1.0, 6.0, ((0, 8), (1, 32))),
        "weight_a": bell_draw(key_of[5], (CH, 9 * (CAM + LID)), (9 * (CAM + LID)) ** -0.5, 0.109375),
        "weight_b": bell_draw(key_of[6], (CH, 9 * CH), (9 * CH) ** -0.5, 0.125),
        "depth_weights": jnp.clip(1.0 * jax.random.uniform(key_of[7], (SCENES, DEPTH, PIX), jnp.float32) ** shard_levels(key_of[7], (SCENES, DEPTH, PIX), ((0, 8), (2, 32)), -0.2, 0.2), 0.0, 1.0).astype(jnp.bfloat16),
        "context": bell_draw(key_of[8], (SCENES, CAM, PIX), 1.0, 6.0, ((0, 8), (2, 32))),
        "block_list": draw_block_list(jax.random.fold_in(key_of[11], 71), 0),
        "point_slot": draw_point_slot(jax.random.fold_in(key_of[11], 71), 0),
    }


def taps_of(padded):
    out_rows = padded.shape[0] - 2
    out_cols = padded.shape[1] - 2
    pieces = [padded[row_tap:row_tap + out_rows, col_tap:col_tap + out_cols] for row_tap in range(3) for col_tap in range(3)]
    return jnp.concatenate(pieces, axis=-1).reshape(out_rows * out_cols, -1)

def pad_both(field):
    return jnp.pad(field, ((1, 1), (1, 1), (0, 0)))

def flipped(weight, fan_channels):
    outputs = weight.shape[0]
    shaped = weight.reshape(outputs, 3, 3, fan_channels)[:, ::-1, ::-1, :]
    return jnp.transpose(shaped, (1, 2, 0, 3)).reshape(9 * outputs, fan_channels)

def one_scene(grad_field, second_pre, first_pre, camera, lidar_field, weight_a, weight_b):
    channels = grad_field.shape[-1]
    zero_value = jnp.zeros((), jnp.bfloat16)
    grad_b = jnp.where(second_pre > 0, grad_field, zero_value)
    hidden = jnp.maximum(first_pre, zero_value)
    wgrad_b = jnp.dot(grad_b.reshape(-1, channels).T, taps_of(pad_both(hidden)), preferred_element_type=jnp.float32)
    back_hidden = jnp.dot(taps_of(pad_both(grad_b)), flipped(weight_b, channels), preferred_element_type=jnp.float32)
    grad_a = jnp.where(first_pre.reshape(-1, channels) > 0, back_hidden, jnp.zeros((), jnp.float32)).astype(jnp.bfloat16)
    grad_a = grad_a.reshape(grad_field.shape)
    inputs = jnp.concatenate([camera, lidar_field], axis=-1)
    wgrad_a = jnp.dot(grad_a.reshape(-1, channels).T, taps_of(pad_both(inputs)), preferred_element_type=jnp.float32)
    back_inputs = jnp.dot(taps_of(pad_both(grad_a)), flipped(weight_a, inputs.shape[-1]), preferred_element_type=jnp.float32)
    back_camera = back_inputs[:, :CAM].astype(jnp.bfloat16)
    back_lidar = back_inputs[:, CAM:].astype(jnp.bfloat16)
    return (wgrad_a, wgrad_b, back_camera, back_lidar)

def reference(grad_out, pre_second, pre_first, camera_bev, lidar_bev, weight_a, weight_b, depth_weights, context, block_list, point_slot):
    cells_dev = ROWS_DEV * COLS
    owner_index = (jnp.arange(PIX) // PIX_DEV).astype(jnp.int32)
    source = (point_slot // (SLOTS * BLOCK)).astype(jnp.int32)
    slot_index = (point_slot // BLOCK % SLOTS).astype(jnp.int32)
    within = (point_slot % BLOCK).astype(jnp.int32)
    chosen = block_list[owner_index[None, :], source, slot_index]
    cell_index = (source * cells_dev + chosen * BLOCK + within).astype(jnp.int32)

    def per_scene(totals, scene_data):
        grad_field, second_pre, first_pre, camera, lidar_field, depth_scene, context_scene = scene_data
        wgrad_a, wgrad_b, back_camera, back_lidar = one_scene(grad_field, second_pre, first_pre, camera, lidar_field, weight_a, weight_b)
        gathered = jnp.take(back_camera, cell_index, axis=0).astype(jnp.float32)
        grad_ctx = jnp.einsum('dp,dpc->cp', depth_scene.astype(jnp.float32), gathered, precision=lax.Precision.HIGHEST)
        grad_dep = jnp.einsum('cp,dpc->dp', context_scene.astype(jnp.float32), gathered, precision=lax.Precision.HIGHEST)
        return ((totals[0] + wgrad_a, totals[1] + wgrad_b), (back_lidar.reshape(ROWS, COLS, LID), grad_ctx, grad_dep))
    start_totals = (jnp.zeros((CH, 9 * (CAM + LID)), jnp.float32), jnp.zeros((CH, 9 * CH), jnp.float32))
    totals, outputs = lax.scan(per_scene, start_totals, (grad_out, pre_second, pre_first, camera_bev, lidar_bev, depth_weights, context))
    norm_factor = 1.0 / math.sqrt(SCENES * ROWS * COLS)
    return (totals[0] * norm_factor, totals[1] * norm_factor, outputs[0], outputs[1], outputs[2])
```

```python
import functools
import math

import jax
import jax.numpy as jnp
from jax import lax
from jax.experimental import pallas as pl
from jax.experimental.pallas import tpu as pltpu
from jax.sharding import PartitionSpec as P

f32 = jnp.float32
bf16 = jnp.bfloat16
NN = (((1,), (0,)), ((), ()))
NT = (((1,), (1,)), ((), ()))
TN = (((0,), (0,)), ((), ()))


def mm(a, b, dims):
    return lax.dot_general(a, b, dims, preferred_element_type=f32)


def shifted_columns(rows, step, cols):
    if step == 0:
        return rows
    zero = jnp.zeros((1, rows.shape[1]), rows.dtype)
    out = []
    for r in range(rows.shape[0] // cols):
        row = rows[r * cols : (r + 1) * cols]
        out += [row[1:], zero] if step > 0 else [zero, row[:-1]]
    return jnp.concatenate(out, axis=0)

TILE = 128


def local_kernel(dims, own_ref, first_ref, before_ref, after_ref, lid_ref, cam_ref, wa_ref, wb_ref, list_ref, core_ref,
                 lidar_ref, blocks_ref, keep_ref, send_ref, g_ref, a_ref, gt_ref, at_ref):
    cols, ch, cam, parts = dims
    lid = lid_ref.shape[2]
    fan = cam + lid
    half = ch // 2
    ext = jnp.concatenate(
        [before_ref[0], before_ref[1], own_ref[0], own_ref[1], after_ref[0], after_ref[1]], axis=0
    ).astype(f32)
    for b in range(3):
        moved = shifted_columns(ext, b - 1, cols)
        g_ref[b] = moved.astype(bf16)
        gt_ref[b] = moved[cols : 5 * cols].T.astype(bf16)
    back = jnp.zeros((4 * cols, ch), f32)
    for a in range(3):
        for b in range(3):
            tap = (3 * (2 - a) + (2 - b)) * ch
            back += mm(g_ref[b, a * cols : (a + 4) * cols, :], wb_ref[:, tap : tap + ch], NN)
    first = jnp.concatenate([before_ref[2], first_ref[0], first_ref[1], after_ref[2]], axis=0).astype(f32)
    grad_a = jnp.where(first > 0, back, 0.0).astype(bf16).astype(f32)
    for b in range(3):
        moved = shifted_columns(grad_a, b - 1, cols)
        a_ref[b] = moved.astype(bf16)
        at_ref[b] = moved.T.astype(bf16)
    lidar = jnp.zeros((2 * cols, lid), f32)
    camera = jnp.zeros((cam, 2 * cols), f32)
    for a in range(3):
        for b in range(3):
            tap = (3 * (2 - a) + (2 - b)) * fan
            rows = a_ref[b, a * cols : (a + 2) * cols, :]
            lidar += mm(rows, wa_ref[tap + cam : tap + fan, :], NT)
            camera += mm(wa_ref[tap : tap + cam, :], rows, NT)
    for r in range(2):
        lidar_ref[r] = lidar[r * cols : (r + 1) * cols].astype(bf16)
    low = camera[:, :cols].astype(bf16)
    high = camera[:, cols:].astype(bf16)
    for k in range(blocks_ref.shape[0]):
        @pl.when(list_ref[k] > 0)
        def _():
            blocks_ref[k] = high

        @pl.when(list_ref[k] <= 0)
        def _():
            blocks_ref[k] = low

    second_core = core_ref[0] > 0
    per_part = keep_ref.shape[2] // TILE

    def put(value, tile):
        halves = value.reshape(ch // 16, 2, 8, value.shape[1])
        even = halves[:, 0].reshape(half, value.shape[1])
        odd = halves[:, 1].reshape(half, value.shape[1])
        mine = jnp.where(second_core, odd, even)
        other = jnp.where(second_core, even, odd).astype(bf16)
        for t in range(value.shape[1] // TILE):
            part, at = divmod(tile + t, per_part)
            here = slice(at * TILE, (at + 1) * TILE)
            keep_ref[part, :, here] = mine[:, t * TILE : (t + 1) * TILE]
            send_ref[part, :, here] = other[:, t * TILE : (t + 1) * TILE]

    hidden = jnp.maximum(jnp.concatenate([first_ref[0], first_ref[1]], axis=0), 0)
    lidar_in = jnp.concatenate([lid_ref[0], lid_ref[1]], axis=0)
    camera_in = jnp.concatenate([cam_ref[0], cam_ref[1]], axis=1)
    b_tiles, a_tiles = ch // TILE, lid // TILE
    packed = []
    for a in range(3):
        for b in range(3):
            tap = 3 * a + b
            window = slice((2 - a) * cols, (4 - a) * cols)
            put(mm(gt_ref[2 - b, :, window], hidden, NN), tap * b_tiles)
            put(mm(at_ref[2 - b, :, window], lidar_in, NN), 9 * b_tiles + tap * a_tiles)
            packed.append(mm(at_ref[2 - b, :, window], camera_in, NT))
    at = 9 * (b_tiles + a_tiles)
    spare = (parts * per_part - at) * TILE - 9 * cam
    packed.append(jnp.zeros((ch, spare), f32))
    put(jnp.concatenate(packed, axis=1), at)


def depth_kernel(blocks_ref, weight_ref, context_ref, slot_ref, gc_ref, gd_ref, wt_ref, st_ref, s_ref, m_ref, d_ref):
    sources, cam, cells_of = blocks_ref.shape
    depth, pix = slot_ref.shape
    wide = st_ref.shape[1]
    wt_ref[...] = jnp.concatenate([weight_ref[...].astype(f32), jnp.zeros((wide - depth, pix), f32)], axis=0).T
    st_ref[...] = jnp.concatenate([slot_ref[...], jnp.full((wide - depth, pix), -1, jnp.int32)], axis=0).T
    context_t = context_ref[...].astype(f32).T.astype(bf16)
    for s in range(sources):
        s_ref[:, s, :] = mm(context_t, blocks_ref[s], NN)
    cells = lax.broadcasted_iota(jnp.int32, (cells_of, wide), 0)
    places = lax.broadcasted_iota(jnp.int32, (sources, wide), 0)
    shift = cells_of.bit_length() - 1

    def pixels(g, carry):
        base = pl.multiple_of(g * 8, 8)
        slots = st_ref[pl.ds(base, 8), :]
        weights = wt_ref[pl.ds(base, 8), :]
        found_rows = []
        for k in range(8):
            slot = slots[k : k + 1]
            at_cell = jnp.where(cells == (slot & (cells_of - 1)), 1.0, 0.0).astype(bf16)
            here = places == (slot >> shift)
            m_ref[base + k] = mm(jnp.where(here, weights[k : k + 1], 0.0).astype(bf16), at_cell, NT)
            value = s_ref[base + k]
            top = value.astype(bf16)
            rest = (value - top.astype(f32)).astype(bf16)
            found = mm(jnp.concatenate([top, rest], axis=0), at_cell, NN)
            found = found[:sources] + found[sources:]
            found_rows.append(jnp.sum(jnp.where(here, found, 0.0), axis=0, keepdims=True))
        d_ref[pl.ds(base, 8), :] = jnp.concatenate(found_rows, axis=0)
        return carry

    lax.fori_loop(0, pix // 8, pixels, 0)
    gd_ref[...] = d_ref[...].T[:depth]
    total = jnp.zeros((cam, pix), f32)
    for s in range(sources):
        mass = m_ref[:, s, :]
        top = mass.astype(bf16)
        rest = (mass - top.astype(f32)).astype(bf16)
        total += mm(blocks_ref[s], top, NT) + mm(blocks_ref[s], rest, NT)
    gc_ref[...] = total


def call(kernel, outs, scratch, args, specs, flops, traffic, limit=40):
    return pl.pallas_call(
        kernel,
        out_shape=outs,
        in_specs=specs,
        out_specs=[VM] * len(outs),
        scratch_shapes=scratch,
        cost_estimate=pl.CostEstimate(flops=flops, bytes_accessed=traffic, transcendentals=0),
        compiler_params=pltpu.CompilerParams(vmem_limit_bytes=limit << 20),
    )(*args)


VM = pl.BlockSpec(memory_space=pltpu.VMEM)
SM = pl.BlockSpec(memory_space=pltpu.SMEM)


def neighbours(x, reverse):
    n = lax.axis_size("space")
    pairs = [(i, i + 1) for i in range(n - 1)]
    return lax.ppermute(x, "space", [(j, i) for i, j in pairs] if reverse else pairs)


def exchanged(x, axis, groups):
    return lax.all_to_all(x, axis, 0, 0, axis_index_groups=groups, tiled=True)


def summed(x):
    return jnp.sum(x.astype(f32), axis=0)


def shards(
    grad_out, pre_second, pre_first, camera_bev, lidar_bev, weight_a, weight_b,
    depth_weights, context, block_list, point_slot,
):
    _, rows, cols, ch = grad_out.shape
    cam, lid = camera_bev.shape[-1], lidar_bev.shape[-1]
    space, scenes = lax.axis_size("space"), lax.axis_size("scene")
    pix = point_slot.shape[1]
    place = space // 2
    reach = scenes // 2
    scale = 1.0 / math.sqrt(rows * cols * space * scenes)
    first = pre_first[0]
    grad_b = jnp.where(pre_second[0] > 0, grad_out[0], jnp.zeros((), bf16))
    before = neighbours(jnp.concatenate([grad_b, first[-1:]]), False)
    after = neighbours(jnp.concatenate([grad_b, first[:1]]), True)
    camera = jnp.swapaxes(camera_bev[0], 1, 2)
    listing = block_list[:, 0, 0]
    core = (lax.axis_index("space") % 2).reshape(1)

    tiles = 9 * (ch + lid) // TILE + -(-9 * cam // TILE)
    per_part = -(-tiles // reach) * TILE
    shape = jax.ShapeDtypeStruct
    lidar, blocks, keep, send = call(
        functools.partial(local_kernel, (cols, ch, cam, reach)),
        [
            shape((rows, cols, lid), bf16),
            shape((space, cam, cols), bf16),
            shape((reach, ch // 2, per_part), f32),
            shape((reach, ch // 2, per_part), bf16),
        ],
        [
            pltpu.VMEM((3, 6 * cols, ch), bf16),
            pltpu.VMEM((3, 4 * cols, ch), bf16),
            pltpu.VMEM((3, ch, 4 * cols), bf16),
            pltpu.VMEM((3, ch, 4 * cols), bf16),
        ],
        (grad_b, first, before, after, lidar_bev[0], camera, weight_a.T, weight_b, listing, core),
        [VM] * 8 + [SM] * 2,
        1_800_000_000,
        12_000_000,
    )
    incoming = exchanged(blocks, "space", None)
    other = lax.ppermute(send, "space", [(i, i ^ 1) for i in range(space)])
    pair = (keep + other.astype(f32)).astype(bf16)
    along_x = exchanged(pair, "scene", [[2 * i + h for i in range(reach)] for h in range(2)])
    part = summed(along_x).astype(bf16).reshape(place, 8, per_part)
    incoming, part = lax.optimization_barrier((incoming, part))
    along_yz = exchanged(part, "space", [[2 * i + c for i in range(place)] for c in range(2)])
    grad_context, grad_depth = call(
        depth_kernel,
        [shape((cam, pix), f32), shape(point_slot.shape, f32)],
        [
            pltpu.VMEM((pix, 128), f32),
            pltpu.VMEM((pix, 128), jnp.int32),
            pltpu.VMEM((pix, space, cols), f32),
            pltpu.VMEM((pix, space, cols), f32),
            pltpu.VMEM((pix, 128), f32),
        ],
        (incoming, depth_weights[0], context[0], point_slot),
        [VM] * 4,
        2_000_000_000,
        2_000_000,
    )
    own = summed(along_yz).astype(bf16)
    all_parts = exchanged(jnp.broadcast_to(own, (scenes, 8, per_part)), "scene", None)
    whole = summed(jnp.moveaxis(all_parts.reshape(reach, 2, 8, per_part), 1, 0))
    whole = jnp.moveaxis(whole, 0, 1).reshape(8, reach * per_part) * scale
    grad_wb = whole[:, : 9 * ch]
    lidar_part = whole[:, 9 * ch : 9 * (ch + lid)].reshape(8, 9, lid)
    camera_part = whole[:, 9 * (ch + lid) : 9 * (ch + lid + cam)].reshape(8, 9, cam)
    grad_wa = jnp.concatenate([camera_part, lidar_part], axis=2).reshape(8, 9 * (cam + lid))
    return grad_wa, grad_wb, lidar[None], grad_context[None], grad_depth[None]


def solution(mesh):
    field = P("scene", "space", None, None)
    pixels = P("scene", None, "space")
    return jax.shard_map(
        shards,
        mesh=mesh,
        in_specs=(field,) * 5 + (P(), P(), pixels, pixels, P(None, "space", None), P(None, "space")),
        out_specs=(P("space", None), P("space", None), field, pixels, pixels),
        check_vma=False,
    )
```

```python
import functools
import math

import jax
import jax.numpy as jnp
from jax import lax
from jax.experimental import pallas as pl
from jax.experimental.pallas import tpu as pltpu
from jax.sharding import PartitionSpec as P

f32 = jnp.float32
bf16 = jnp.bfloat16
NN = (((1,), (0,)), ((), ()))
NT = (((1,), (1,)), ((), ()))
TN = (((0,), (0,)), ((), ()))


def mm(a, b, dims):
    return lax.dot_general(a, b, dims, preferred_element_type=f32)


def shifted_columns(rows, step, cols):
    if step == 0:
        return rows
    zero = jnp.zeros((1, rows.shape[1]), rows.dtype)
    out = []
    for r in range(rows.shape[0] // cols):
        row = rows[r * cols : (r + 1) * cols]
        out += [row[1:], zero] if step > 0 else [zero, row[:-1]]
    return jnp.concatenate(out, axis=0)

TILE = 128


def local_kernel(dims, own_ref, before_ref, after_ref, first_hbm, lid_hbm, cam_hbm, wa_hbm, wb_hbm, spot_ref,
                 lidar_ref, blocks_hbm, keep_ref, send_ref,
                 g_ref, a_ref, gt_ref, at_ref, first_ref, lid_ref, cam_ref, wa_ref, wb_ref, pick_ref, sems, block_sems):
    cols, ch, cam, parts = dims
    lid = lid_ref.shape[2]
    fan = cam + lid
    half = ch // 2
    moves = [
        pltpu.make_async_copy(source, target, sems.at[k])
        for k, (source, target) in enumerate(
            [(wb_hbm, wb_ref), (first_hbm, first_ref), (wa_hbm, wa_ref), (lid_hbm, lid_ref), (cam_hbm, cam_ref)]
        )
    ]
    for move in moves:
        move.start()
    ext = jnp.concatenate(
        [before_ref[0], before_ref[1], own_ref[0], own_ref[1], after_ref[0], after_ref[1]], axis=0
    ).astype(f32)
    for b in range(3):
        moved = shifted_columns(ext, b - 1, cols)
        g_ref[b] = moved.astype(bf16)
        gt_ref[b] = moved[cols : 5 * cols].T.astype(bf16)
    moves[0].wait()
    back = jnp.zeros((4 * cols, ch), f32)
    for a in range(3):
        for b in range(3):
            tap = (3 * (2 - a) + (2 - b)) * ch
            back += mm(g_ref[b, a * cols : (a + 4) * cols, :], wb_ref[:, tap : tap + ch], NN)
    moves[1].wait()
    first = jnp.concatenate([before_ref[2], first_ref[0], first_ref[1], after_ref[2]], axis=0).astype(f32)
    grad_a = jnp.where(first > 0, back, 0.0).astype(bf16).astype(f32)
    for b in range(3):
        moved = shifted_columns(grad_a, b - 1, cols)
        a_ref[b] = moved.astype(bf16)
        at_ref[b] = moved.T.astype(bf16)
    moves[2].wait()
    lidar = jnp.zeros((2 * cols, lid), f32)
    camera = jnp.zeros((cam, 2 * cols), f32)
    for a in range(3):
        for b in range(3):
            tap = (3 * (2 - a) + (2 - b)) * fan
            rows = a_ref[b, a * cols : (a + 2) * cols, :]
            lidar += mm(rows, wa_ref[tap + cam : tap + fan, :], NT)
            camera += mm(wa_ref[tap : tap + cam, :], rows, NT)
    for r in range(2):
        lidar_ref[r] = lidar[r * cols : (r + 1) * cols].astype(bf16)
    for r in range(2):
        pick_ref[r] = camera[:, r * cols : (r + 1) * cols].astype(bf16)
    picks = [
        pltpu.make_async_copy(pick_ref.at[jnp.where(spot_ref[2 + k] > 0, 1, 0)], blocks_hbm.at[k], block_sems.at[k])
        for k in range(blocks_hbm.shape[0])
    ]
    for pick in picks:
        pick.start()

    moves[3].wait()
    moves[4].wait()
    second_core = spot_ref[0] > 0
    per_part = keep_ref.shape[2] // TILE

    def put(value, tile):
        halves = value.reshape(ch // 16, 2, 8, value.shape[1])
        even = halves[:, 0].reshape(half, value.shape[1])
        odd = halves[:, 1].reshape(half, value.shape[1])
        mine = jnp.where(second_core, odd, even)
        other = jnp.where(second_core, even, odd).astype(bf16)
        for t in range(value.shape[1] // TILE):
            part, at = divmod(tile + t, per_part)
            part = part ^ spot_ref[1]
            here = slice(at * TILE, (at + 1) * TILE)
            keep_ref[part, :, here] = mine[:, t * TILE : (t + 1) * TILE]
            send_ref[part, :, here] = other[:, t * TILE : (t + 1) * TILE]

    hidden = jnp.maximum(jnp.concatenate([first_ref[0], first_ref[1]], axis=0), 0)
    lidar_in = jnp.concatenate([lid_ref[0], lid_ref[1]], axis=0)
    camera_in = jnp.concatenate([cam_ref[0], cam_ref[1]], axis=1)
    b_tiles, a_tiles = ch // TILE, lid // TILE
    packed = []
    for a in range(3):
        for b in range(3):
            tap = 3 * a + b
            window = slice((2 - a) * cols, (4 - a) * cols)
            put(mm(gt_ref[2 - b, :, window], hidden, NN), tap * b_tiles)
            put(mm(at_ref[2 - b, :, window], lidar_in, NN), 9 * b_tiles + tap * a_tiles)
            packed.append(mm(at_ref[2 - b, :, window], camera_in, NT))
    at = 9 * (b_tiles + a_tiles)
    spare = (parts * per_part - at) * TILE - 9 * cam
    packed.append(jnp.zeros((ch, spare), f32))
    put(jnp.concatenate(packed, axis=1), at)
    for pick in picks:
        pick.wait()


def depth_kernel(blocks_ref, weight_ref, context_ref, slot_ref, gc_ref, gd_ref, wt_ref, st_ref, s_ref, m_ref, d_ref):
    sources, cam, cells_of = blocks_ref.shape
    depth, pix = slot_ref.shape
    wide = st_ref.shape[1]
    wt_ref[...] = jnp.concatenate([weight_ref[...].astype(f32), jnp.zeros((wide - depth, pix), f32)], axis=0).T
    st_ref[...] = jnp.concatenate([slot_ref[...], jnp.full((wide - depth, pix), -1, jnp.int32)], axis=0).T
    context_t = context_ref[...].astype(f32).T.astype(bf16)
    for s in range(sources):
        s_ref[:, s, :] = mm(context_t, blocks_ref[s], NN)
    cells = lax.broadcasted_iota(jnp.int32, (cells_of, wide), 0)
    places = lax.broadcasted_iota(jnp.int32, (sources, wide), 0)
    shift = cells_of.bit_length() - 1

    def pixels(g, carry):
        base = pl.multiple_of(g * 8, 8)
        slots = st_ref[pl.ds(base, 8), :]
        weights = wt_ref[pl.ds(base, 8), :]
        found_rows = []
        for k in range(8):
            slot = slots[k : k + 1]
            at_cell = jnp.where(cells == (slot & (cells_of - 1)), 1.0, 0.0).astype(bf16)
            here = places == (slot >> shift)
            m_ref[base + k] = mm(jnp.where(here, weights[k : k + 1], 0.0).astype(bf16), at_cell, NT)
            value = s_ref[base + k]
            top = value.astype(bf16)
            rest = (value - top.astype(f32)).astype(bf16)
            found = mm(jnp.concatenate([top, rest], axis=0), at_cell, NN)
            found = found[:sources] + found[sources:]
            found_rows.append(jnp.sum(jnp.where(here, found, 0.0), axis=0, keepdims=True))
        d_ref[pl.ds(base, 8), :] = jnp.concatenate(found_rows, axis=0)
        return carry

    lax.fori_loop(0, pix // 8, pixels, 0)
    gd_ref[...] = d_ref[...].T[:depth]
    total = jnp.zeros((cam, pix), f32)
    for s in range(sources):
        mass = m_ref[:, s, :]
        top = mass.astype(bf16)
        rest = (mass - top.astype(f32)).astype(bf16)
        total += mm(blocks_ref[s], top, NT) + mm(blocks_ref[s], rest, NT)
    gc_ref[...] = total


def first_sum(keep_ref, other_ref, a_ref, b_ref):
    rows = a_ref.shape[1]
    for k, (upper, lower) in enumerate([(1, 3), (2, 2)]):
        a_ref[k] = (keep_ref[upper, :rows] + other_ref[upper, :rows].astype(f32)).astype(bf16)
        b_ref[k] = (keep_ref[lower, rows:] + other_ref[lower, rows:].astype(f32)).astype(bf16)


def second_sum(keep_ref, other_ref, a_ref, b_ref, own_ref, a_out_ref, b_out_ref):
    rows = a_ref.shape[1]

    def held(part, here, came):
        return keep_ref[part, here] + other_ref[part, here].astype(f32) + came.astype(f32)

    upper, lower = slice(0, rows), slice(rows, 2 * rows)
    a_out_ref[...] = held(3, upper, a_ref[1]).astype(bf16)
    b_out_ref[...] = held(1, lower, b_ref[1]).astype(bf16)
    own_ref[upper] = held(0, upper, a_ref[0])
    own_ref[lower] = held(0, lower, b_ref[0])


def third_sum(own_ref, a_ref, b_ref, out_ref):
    rows = a_ref.shape[0]
    out_ref[:rows] = (own_ref[:rows] + a_ref[...].astype(f32)).astype(bf16)
    out_ref[rows:] = (own_ref[rows:] + b_ref[...].astype(f32)).astype(bf16)


def place_sum(parts_ref, out_ref):
    total = jnp.sum(parts_ref[...].astype(f32), axis=0).astype(bf16)
    for k in range(out_ref.shape[0]):
        out_ref[k] = total


def last_sum(dims, scale, parts_ref, wa_ref, wb_ref):
    ch, lid, cam = dims
    whole = jnp.concatenate(
        [
            (parts_ref[2 * x].astype(f32) + parts_ref[2 * x + 1].astype(f32)) * scale
            for x in range(parts_ref.shape[0] // 2)
        ],
        axis=1,
    )
    wb_ref[...] = whole[:, : 9 * ch]
    pieces = []
    for tap in range(9):
        at = 9 * (ch + lid) + tap * cam
        pieces += [whole[:, at : at + cam], whole[:, 9 * ch + tap * lid : 9 * ch + (tap + 1) * lid]]
    wa_ref[...] = jnp.concatenate(pieces, axis=1)


def call(kernel, outs, scratch, args, specs, flops, traffic, outs_at=None, limit=40):
    return pl.pallas_call(
        kernel,
        out_shape=outs,
        in_specs=specs,
        out_specs=outs_at or [VM] * len(outs),
        scratch_shapes=scratch,
        cost_estimate=pl.CostEstimate(flops=flops, bytes_accessed=traffic, transcendentals=0),
        compiler_params=pltpu.CompilerParams(vmem_limit_bytes=limit << 20),
    )(*[pltpu.with_memory_space_constraint(x, pltpu.HBM) if spec is HB else x for x, spec in zip(args, specs)])


def small(kernel, outs, args):
    outs = [jax.ShapeDtypeStruct(shape, dtype) for shape, dtype in outs]
    traffic = sum(x.size * x.dtype.itemsize for x in (*args, *outs))
    return call(kernel, outs, [], args, [VM] * len(args), traffic, traffic)


VM = pl.BlockSpec(memory_space=pltpu.VMEM)
SM = pl.BlockSpec(memory_space=pltpu.SMEM)
HB = pl.BlockSpec(memory_space=pltpu.HBM)


def neighbours(x, reverse):
    n = lax.axis_size("space")
    pairs = [(i, i + 1) for i in range(n - 1)]
    return lax.ppermute(x, "space", [(j, i) for i, j in pairs] if reverse else pairs)


def exchanged(x, axis, groups):
    return lax.all_to_all(x, axis, 0, 0, axis_index_groups=groups, tiled=True)


def swapped(x, axis, partner):
    return lax.ppermute(x, axis, [(i, partner(i)) for i in range(lax.axis_size(axis))])


def summed_along_x(keep, send):
    _, rows, per_part = keep.shape
    deep = rows // 2
    other = swapped(send, "space", lambda i: i ^ 1)
    a, b = small(first_sum, [((2, deep, per_part), bf16)] * 2, (keep, other))
    a, b = swapped(a, "scene", lambda i: i ^ 2), swapped(b, "scene", lambda i: i ^ 6)
    own, a, b = small(
        second_sum,
        [((2 * deep, per_part), f32), ((deep, per_part), bf16), ((deep, per_part), bf16)],
        (keep, other, a, b),
    )
    a, b = swapped(a, "scene", lambda i: i ^ 6), swapped(b, "scene", lambda i: i ^ 2)
    (part,) = small(third_sum, [((2 * deep, per_part), bf16)], (own, a, b))
    return part


def shards(
    grad_out, pre_second, pre_first, camera_bev, lidar_bev, weight_a, weight_b,
    depth_weights, context, block_list, point_slot,
):
    _, rows, cols, ch = grad_out.shape
    cam, lid = camera_bev.shape[-1], lidar_bev.shape[-1]
    space, scenes = lax.axis_size("space"), lax.axis_size("scene")
    pix = point_slot.shape[1]
    place = space // 2
    reach = scenes // 2
    scale = 1.0 / math.sqrt(rows * cols * space * scenes)
    first = pre_first[0]
    grad_b = jnp.where(pre_second[0] > 0, grad_out[0], jnp.zeros((), bf16))
    before = neighbours(jnp.concatenate([grad_b, first[-1:]]), False)
    after = neighbours(jnp.concatenate([grad_b, first[:1]]), True)
    camera = jnp.swapaxes(camera_bev[0], 1, 2)
    spot = jnp.concatenate(
        [(lax.axis_index("space") & 1).reshape(1), (lax.axis_index("scene") >> 1).reshape(1), block_list[:, 0, 0]]
    )

    tiles = 9 * (ch + lid) // TILE + -(-9 * cam // TILE)
    per_part = -(-tiles // reach) * TILE
    shape = jax.ShapeDtypeStruct
    lidar, blocks, keep, send = call(
        functools.partial(local_kernel, (cols, ch, cam, reach)),
        [
            shape((rows, cols, lid), bf16),
            pltpu.HBM((space, cam, cols), bf16),
            shape((reach, ch // 2, per_part), f32),
            shape((reach, ch // 2, per_part), bf16),
        ],
        [
            pltpu.VMEM((3, 6 * cols, ch), bf16),
            pltpu.VMEM((3, 4 * cols, ch), bf16),
            pltpu.VMEM((3, ch, 4 * cols), bf16),
            pltpu.VMEM((3, ch, 4 * cols), bf16),
            pltpu.VMEM(first.shape, bf16),
            pltpu.VMEM((rows, cols, lid), bf16),
            pltpu.VMEM(camera.shape, bf16),
            pltpu.VMEM(weight_a.shape[::-1], bf16),
            pltpu.VMEM(weight_b.shape, bf16),
            pltpu.VMEM((2, cam, cols), bf16),
            pltpu.SemaphoreType.DMA((5,)),
            pltpu.SemaphoreType.DMA((space,)),
        ],
        (grad_b, before, after, first, lidar_bev[0], camera, weight_a.T, weight_b, spot),
        [VM] * 3 + [HB] * 5 + [SM],
        1_800_000_000,
        12_000_000,
        outs_at=[VM, HB, VM, VM],
    )
    incoming = exchanged(blocks, "space", None)
    part = summed_along_x(keep, send)
    incoming, part = lax.optimization_barrier((incoming, part))
    along_yz = exchanged(
        part.reshape(place, 8, per_part), "space", [[2 * i + c for i in range(place)] for c in range(2)]
    )
    grad_context, grad_depth = call(
        depth_kernel,
        [shape((cam, pix), f32), shape(point_slot.shape, f32)],
        [
            pltpu.VMEM((pix, 128), f32),
            pltpu.VMEM((pix, 128), jnp.int32),
            pltpu.VMEM((pix, space, cols), f32),
            pltpu.VMEM((pix, space, cols), f32),
            pltpu.VMEM((pix, 128), f32),
        ],
        (incoming, depth_weights[0], context[0], point_slot),
        [VM] * 4,
        2_000_000_000,
        2_000_000,
    )
    along_yz, grad_context, grad_depth = lax.optimization_barrier((along_yz, grad_context, grad_depth))
    (spread,) = small(place_sum, [((scenes, 8, per_part), bf16)], (along_yz,))
    everything = exchanged(spread, "scene", None)
    grad_wa, grad_wb = small(
        functools.partial(last_sum, (ch, lid, cam), scale),
        [((8, 9 * (cam + lid)), f32), ((8, 9 * ch), f32)],
        (everything,),
    )
    return grad_wa, grad_wb, lidar[None], grad_context[None], grad_depth[None]


def solution(mesh):
    field = P("scene", "space", None, None)
    pixels = P("scene", None, "space")
    return jax.shard_map(
        shards,
        mesh=mesh,
        in_specs=(field,) * 5 + (P(), P(), pixels, pixels, P(None, "space", None), P(None, "space")),
        out_specs=(P("space", None), P("space", None), field, pixels, pixels),
        check_vma=False,
    )
```

```python
import functools
import math

import jax
import jax.numpy as jnp
from jax import lax
from jax.experimental import pallas as pl
from jax.experimental.pallas import tpu as pltpu
from jax.sharding import PartitionSpec as P


f32 = jnp.float32
bf16 = jnp.bfloat16
NN = (((1,), (0,)), ((), ()))
NT = (((1,), (1,)), ((), ()))


def mm(a, b, dims):
    return lax.dot_general(a, b, dims, preferred_element_type=f32)


def shifted_columns(rows, step, cols):
    if step == 0:
        return rows
    zero = jnp.zeros((1, rows.shape[1]), rows.dtype)
    out = []
    for r in range(rows.shape[0] // cols):
        row = rows[r * cols : (r + 1) * cols]
        out += [row[1:], zero] if step > 0 else [zero, row[:-1]]
    return jnp.concatenate(out, axis=0)


TILE = 128


def load_kernel(*refs):
    count = (len(refs) - 2) // 2
    moves = [pltpu.make_async_copy(refs[k], refs[count + 1 + k], refs[-1].at[k]) for k in range(count)]
    for move in moves:
        move.start()
    for move in moves:
        move.wait()


def local_kernel(dims, own_ref, before_ref, after_ref, first_ref, lid_ref, cam_ref, wa_ref, wb_ref, spot_ref,
                 lidar_ref, blocks_hbm, keep_ref, send_ref,
                 g_ref, a_ref, gt_ref, at_ref, pick_ref, block_sems):
    cols, ch, cam, parts = dims
    lid = lid_ref.shape[2]
    fan = cam + lid
    half = ch // 2
    ext = jnp.concatenate(
        [before_ref[0], before_ref[1], own_ref[0], own_ref[1], after_ref[0], after_ref[1]], axis=0
    ).astype(f32)
    for b in range(3):
        moved = shifted_columns(ext, b - 1, cols)
        g_ref[b] = moved.astype(bf16)
        gt_ref[b] = moved[cols : 5 * cols].T.astype(bf16)
    back = jnp.zeros((4 * cols, ch), f32)
    for a in range(3):
        for b in range(3):
            tap = (3 * (2 - a) + (2 - b)) * ch
            back += mm(g_ref[b, a * cols : (a + 4) * cols, :], wb_ref[:, tap : tap + ch], NN)
    first = jnp.concatenate([before_ref[2], first_ref[0], first_ref[1], after_ref[2]], axis=0).astype(f32)
    grad_a = jnp.where(first > 0, back, 0.0).astype(bf16).astype(f32)
    for b in range(3):
        moved = shifted_columns(grad_a, b - 1, cols)
        a_ref[b] = moved.astype(bf16)
        at_ref[b] = moved.T.astype(bf16)
    lidar = jnp.zeros((2 * cols, lid), f32)
    camera = jnp.zeros((cam, 2 * cols), f32)
    for a in range(3):
        for b in range(3):
            tap = (3 * (2 - a) + (2 - b)) * fan
            rows = a_ref[b, a * cols : (a + 2) * cols, :]
            lidar += mm(rows, wa_ref[tap + cam : tap + fan, :], NT)
            camera += mm(wa_ref[tap : tap + cam, :], rows, NT)
    for r in range(2):
        lidar_ref[r] = lidar[r * cols : (r + 1) * cols].astype(bf16)
    for r in range(2):
        pick_ref[r] = camera[:, r * cols : (r + 1) * cols].astype(bf16)
    picks = [
        pltpu.make_async_copy(pick_ref.at[jnp.where(spot_ref[2 + k] > 0, 1, 0)], blocks_hbm.at[k], block_sems.at[k])
        for k in range(blocks_hbm.shape[0])
    ]
    for pick in picks:
        pick.start()

    second_core = spot_ref[0] > 0
    per_part = keep_ref.shape[2] // TILE

    def put(value, tile):
        halves = value.reshape(ch // 16, 2, 8, value.shape[1])
        even = halves[:, 0].reshape(half, value.shape[1])
        odd = halves[:, 1].reshape(half, value.shape[1])
        mine = jnp.where(second_core, odd, even)
        other = jnp.where(second_core, even, odd).astype(bf16)
        for t in range(value.shape[1] // TILE):
            part, at = divmod(tile + t, per_part)
            part = part ^ spot_ref[1]
            here = slice(at * TILE, (at + 1) * TILE)
            keep_ref[part, :, here] = mine[:, t * TILE : (t + 1) * TILE]
            send_ref[part, :, here] = other[:, t * TILE : (t + 1) * TILE]

    hidden = jnp.maximum(jnp.concatenate([first_ref[0], first_ref[1]], axis=0), 0)
    lidar_in = jnp.concatenate([lid_ref[0], lid_ref[1]], axis=0)
    camera_in = jnp.concatenate([cam_ref[0], cam_ref[1]], axis=1)
    b_tiles, a_tiles = ch // TILE, lid // TILE
    packed = []
    for a in range(3):
        for b in range(3):
            tap = 3 * a + b
            window = slice((2 - a) * cols, (4 - a) * cols)
            put(mm(gt_ref[2 - b, :, window], hidden, NN), tap * b_tiles)
            put(mm(at_ref[2 - b, :, window], lidar_in, NN), 9 * b_tiles + tap * a_tiles)
            packed.append(mm(at_ref[2 - b, :, window], camera_in, NT))
    at = 9 * (b_tiles + a_tiles)
    spare = (parts * per_part - at) * TILE - 9 * cam
    packed.append(jnp.zeros((ch, spare), f32))
    put(jnp.concatenate(packed, axis=1), at)
    for pick in picks:
        pick.wait()


def depth_kernel(blocks_ref, weight_ref, context_ref, slot_ref, gc_ref, gd_ref, wt_ref, st_ref, s_ref, m_ref, d_ref):
    sources, cam, cells_of = blocks_ref.shape
    depth, pix = slot_ref.shape
    wide = st_ref.shape[1]
    wt_ref[...] = jnp.concatenate([weight_ref[...].astype(f32), jnp.zeros((wide - depth, pix), f32)], axis=0).T
    st_ref[...] = jnp.concatenate([slot_ref[...], jnp.full((wide - depth, pix), -1, jnp.int32)], axis=0).T
    context_t = context_ref[...].astype(f32).T.astype(bf16)
    pitch = s_ref.shape[0] // sources
    for s in range(sources):
        s_ref[s * pitch : s * pitch + pix, :] = mm(context_t, blocks_ref[s], NN)
    cells = lax.broadcasted_iota(jnp.int32, (cells_of, wide), 0)
    places = lax.broadcasted_iota(jnp.int32, (sources, wide), 0)
    shift = cells_of.bit_length() - 1

    def pixels(g, carry):
        base = pl.multiple_of(g * 8, 8)
        slots = st_ref[pl.ds(base, 8), :]
        weights = wt_ref[pl.ds(base, 8), :]
        found_rows = []
        for k in range(8):
            slot = slots[k : k + 1]
            at_cell = jnp.where(cells == (slot & (cells_of - 1)), 1.0, 0.0).astype(bf16)
            here = places == (slot >> shift)
            every = pl.ds(base + k, sources, stride=pitch)
            m_ref[every, :] = mm(jnp.where(here, weights[k : k + 1], 0.0).astype(bf16), at_cell, NT)
            found = mm(s_ref[every, :].astype(bf16), at_cell, NN)
            found_rows.append(jnp.sum(jnp.where(here, found, 0.0), axis=0, keepdims=True))
        d_ref[pl.ds(base, 8), :] = jnp.concatenate(found_rows, axis=0)
        return carry

    lax.fori_loop(0, pix // 8, pixels, 0)
    gd_ref[...] = d_ref[...].T[:depth]
    total = jnp.zeros((cam, pix), f32)
    for s in range(sources):
        total += mm(blocks_ref[s], m_ref[s * pitch : s * pitch + pix, :].astype(bf16), NT)
    gc_ref[...] = total


def first_sum(keep_ref, other_ref, a_ref, b_ref):
    rows = a_ref.shape[1]
    for k, (upper, lower) in enumerate([(1, 3), (2, 2)]):
        a_ref[k] = (keep_ref[upper, :rows] + other_ref[upper, :rows].astype(f32)).astype(bf16)
        b_ref[k] = (keep_ref[lower, rows:] + other_ref[lower, rows:].astype(f32)).astype(bf16)


def kept_sum(keep_ref, other_ref, own_ref, next_ref):
    rows = own_ref.shape[0] // 2
    upper, lower = slice(0, rows), slice(rows, 2 * rows)
    own_ref[...] = keep_ref[0] + other_ref[0].astype(f32)
    next_ref[upper] = keep_ref[3, upper] + other_ref[3, upper].astype(f32)
    next_ref[lower] = keep_ref[1, lower] + other_ref[1, lower].astype(f32)


def second_sum(own_ref, next_ref, a_ref, b_ref, out_ref, a_out_ref, b_out_ref):
    rows = a_ref.shape[1]
    upper, lower = slice(0, rows), slice(rows, 2 * rows)
    a_out_ref[...] = (next_ref[upper] + a_ref[1].astype(f32)).astype(bf16)
    b_out_ref[...] = (next_ref[lower] + b_ref[1].astype(f32)).astype(bf16)
    out_ref[upper] = own_ref[upper] + a_ref[0].astype(f32)
    out_ref[lower] = own_ref[lower] + b_ref[0].astype(f32)


def third_sum(own_ref, a_ref, b_ref, out_ref):
    rows = a_ref.shape[0]
    out_ref[:rows] = (own_ref[:rows] + a_ref[...].astype(f32)).astype(bf16)
    out_ref[rows:] = (own_ref[rows:] + b_ref[...].astype(f32)).astype(bf16)


def place_sum(parts_ref, out_ref):
    out_ref[...] = jnp.sum(parts_ref[...].astype(f32), axis=0).astype(bf16)


def pair_sum(one_ref, two_ref, out_ref):
    out_ref[...] = one_ref[...].astype(f32) + two_ref[...].astype(f32)


def last_sum(dims, scale, *refs):
    ch, lid, cam = dims
    *parts, spot_ref, wa_ref, wb_ref, all_ref = refs
    for k, part in enumerate(parts):
        all_ref[k ^ spot_ref[1]] = part[...]
    whole = jnp.concatenate([all_ref[x] for x in range(len(parts))], axis=1) * scale
    wb_ref[...] = whole[:, : 9 * ch]
    pieces = []
    for tap in range(9):
        at = 9 * (ch + lid) + tap * cam
        pieces += [whole[:, at : at + cam], whole[:, 9 * ch + tap * lid : 9 * ch + (tap + 1) * lid]]
    wa_ref[...] = jnp.concatenate(pieces, axis=1)


def call(kernel, outs, scratch, args, specs, flops, traffic, outs_at=None, limit=24):
    return pl.pallas_call(
        kernel,
        out_shape=outs,
        in_specs=specs,
        out_specs=outs_at or [VM] * len(outs),
        scratch_shapes=scratch,
        cost_estimate=pl.CostEstimate(flops=flops, bytes_accessed=traffic, transcendentals=0),
        compiler_params=pltpu.CompilerParams(vmem_limit_bytes=limit << 20),
    )(*[pltpu.with_memory_space_constraint(x, pltpu.HBM) if spec is HB else x for x, spec in zip(args, specs)])


def small(kernel, outs, args):
    outs = [jax.ShapeDtypeStruct(shape, dtype) for shape, dtype in outs]
    traffic = sum(x.size * x.dtype.itemsize for x in (*args, *outs))
    return call(kernel, outs, [], args, [VM] * len(args), traffic, traffic)


VM = pl.BlockSpec(memory_space=pltpu.VMEM)
SM = pl.BlockSpec(memory_space=pltpu.SMEM)
HB = pl.BlockSpec(memory_space=pltpu.HBM)


def neighbours(x, reverse):
    n = lax.axis_size("space")
    pairs = [(i, i + 1) for i in range(n - 1)]
    return lax.ppermute(x, "space", [(j, i) for i, j in pairs] if reverse else pairs)


def exchanged(x, axis, groups):
    return lax.all_to_all(x, axis, 0, 0, axis_index_groups=groups, tiled=True)


def swapped(x, axis, partner):
    return lax.ppermute(x, axis, [(i, partner(i)) for i in range(lax.axis_size(axis))])


def summed_along_x(keep, send):
    _, rows, per_part = keep.shape
    deep = rows // 2
    other = swapped(send, "space", lambda i: i ^ 1)
    a, b = small(first_sum, [((2, deep, per_part), bf16)] * 2, (keep, other))
    a, b = swapped(a, "scene", lambda i: i ^ 2), swapped(b, "scene", lambda i: i ^ 6)
    kept = small(kept_sum, [((2 * deep, per_part), f32)] * 2, (keep, other))
    own, a, b = small(
        second_sum,
        [((2 * deep, per_part), f32), ((deep, per_part), bf16), ((deep, per_part), bf16)],
        (*kept, a, b),
    )
    a, b = swapped(a, "scene", lambda i: i ^ 6), swapped(b, "scene", lambda i: i ^ 2)
    (part,) = small(third_sum, [((2 * deep, per_part), bf16)], (own, a, b))
    return part


def over_scenes(part, spot, dims, scale):
    ch, lid, cam = dims
    (own,) = small(pair_sum, [(part.shape, f32)], (part, swapped(part, "scene", lambda i: i ^ 1)))
    parts = [own] + [swapped(own, "scene", lambda i, k=k: i ^ 2 * k) for k in range(1, 4)]
    return call(
        functools.partial(last_sum, dims, scale),
        [jax.ShapeDtypeStruct((8, 9 * width), f32) for width in (cam + lid, ch)],
        [pltpu.VMEM((len(parts), *own.shape), f32)],
        (*parts, spot),
        [VM] * len(parts) + [SM],
        400_000,
        400_000,
    )


def shards(
    grad_out, pre_second, pre_first, camera_bev, lidar_bev, weight_a, weight_b,
    depth_weights, context, block_list, point_slot,
):
    _, rows, cols, ch = grad_out.shape
    cam, lid = camera_bev.shape[-1], lidar_bev.shape[-1]
    space, scenes = lax.axis_size("space"), lax.axis_size("scene")
    pix = point_slot.shape[1]
    place = space // 2
    reach = scenes // 2
    scale = 1.0 / math.sqrt(rows * cols * space * scenes)
    first = pre_first[0]
    grad_b = jnp.where(pre_second[0] > 0, grad_out[0], jnp.zeros((), bf16))
    before = neighbours(jnp.concatenate([grad_b, first[-1:]]), False)
    after = neighbours(jnp.concatenate([grad_b, first[:1]]), True)
    camera = jnp.swapaxes(camera_bev[0], 1, 2)
    spot = jnp.concatenate(
        [(lax.axis_index("space") & 1).reshape(1), (lax.axis_index("scene") >> 1).reshape(1), block_list[:, 0, 0]]
    )

    tiles = 9 * (ch + lid) // TILE + -(-9 * cam // TILE)
    per_part = -(-tiles // reach) * TILE
    shape = jax.ShapeDtypeStruct
    own_data = (first, lidar_bev[0], camera, weight_a.T, weight_b)
    loaded = call(
        load_kernel,
        [pltpu.VMEM(x.shape, x.dtype) for x in own_data],
        [pltpu.SemaphoreType.DMA((len(own_data),))],
        (*own_data, spot),
        [HB] * len(own_data) + [SM],
        2_000_000,
        3_000_000,
    )
    lidar, blocks, keep, send = call(
        functools.partial(local_kernel, (cols, ch, cam, reach)),
        [
            shape((rows, cols, lid), bf16),
            pltpu.HBM((space, cam, cols), bf16),
            shape((reach, ch // 2, per_part), f32),
            shape((reach, ch // 2, per_part), bf16),
        ],
        [
            pltpu.VMEM((3, 6 * cols, ch), bf16),
            pltpu.VMEM((3, 4 * cols, ch), bf16),
            pltpu.VMEM((3, ch, 4 * cols), bf16),
            pltpu.VMEM((3, ch, 4 * cols), bf16),
            pltpu.VMEM((2, cam, cols), bf16),
            pltpu.SemaphoreType.DMA((space,)),
        ],
        (grad_b, before, after, *loaded, spot),
        [VM] * 8 + [SM],
        1_800_000_000,
        12_000_000,
        outs_at=[VM, HB, VM, VM],
    )
    incoming = exchanged(blocks, "space", None)
    part = summed_along_x(keep, send)
    incoming, part = lax.optimization_barrier((incoming, part))
    along_yz = exchanged(
        part.reshape(place, 8, per_part), "space", [[2 * i + c for i in range(place)] for c in range(2)]
    )
    grad_context, grad_depth = call(
        depth_kernel,
        [shape((cam, pix), f32), shape(point_slot.shape, f32)],
        [
            pltpu.VMEM((pix, 128), f32),
            pltpu.VMEM((pix, 128), jnp.int32),
            pltpu.VMEM((space * (pix + 8), cols), f32),
            pltpu.VMEM((space * (pix + 8), cols), f32),
            pltpu.VMEM((pix, 128), f32),
        ],
        (incoming, depth_weights[0], context[0], point_slot),
        [VM] * 4,
        2_000_000_000,
        2_000_000,
    )
    along_yz, grad_context, grad_depth = lax.optimization_barrier((along_yz, grad_context, grad_depth))
    (part,) = small(place_sum, [((8, per_part), bf16)], (along_yz,))
    grad_wa, grad_wb = over_scenes(part, spot, (ch, lid, cam), scale)
    return grad_wa, grad_wb, lidar[None], grad_context[None], grad_depth[None]


def solution(mesh):
    field = P("scene", "space", None, None)
    pixels = P("scene", None, "space")
    return jax.shard_map(
        shards,
        mesh=mesh,
        in_specs=(field,) * 5 + (P(), P(), pixels, pixels, P(None, "space", None), P(None, "space")),
        out_specs=(P("space", None), P("space", None), field, pixels, pixels),
        check_vma=False,
    )
```

```python
import functools
import math

import jax
import jax.numpy as jnp
from jax import lax
from jax.experimental import pallas as pl
from jax.experimental.pallas import tpu as pltpu
from jax.sharding import PartitionSpec as P


f32 = jnp.float32
bf16 = jnp.bfloat16
NN = (((1,), (0,)), ((), ()))
NT = (((1,), (1,)), ((), ()))


def mm(a, b, dims):
    return lax.dot_general(a, b, dims, preferred_element_type=f32)


def shifted_columns(rows, step, cols):
    if step == 0:
        return rows
    zero = jnp.zeros((1, rows.shape[1]), rows.dtype)
    out = []
    for r in range(rows.shape[0] // cols):
        row = rows[r * cols : (r + 1) * cols]
        out += [row[1:], zero] if step > 0 else [zero, row[:-1]]
    return jnp.concatenate(out, axis=0)


TILE = 128


def started(sources, targets, sems):
    moves = [pltpu.make_async_copy(source, target, sems.at[k]) for k, (source, target) in enumerate(zip(sources, targets))]
    for move in moves:
        move.start()
    return moves


def passed(grad_ref, second_ref):
    return jnp.where(second_ref[...].astype(f32) > 0, grad_ref[...].astype(f32), 0.0).astype(bf16)


def halo_kernel(grad_hbm, second_hbm, first_hbm, down_ref, up_ref, grad_ref, second_ref, first_ref, sems):
    for move in started((grad_hbm, second_hbm, first_hbm), (grad_ref, second_ref, first_ref), sems):
        move.wait()
    rows = first_ref.shape[0]
    grad_b = passed(grad_ref, second_ref)
    down_ref[:rows] = grad_b
    up_ref[:rows] = grad_b
    down_ref[rows] = first_ref[rows - 1]
    up_ref[rows] = first_ref[0]


def load_kernel(*refs):
    count = (len(refs) - 3) // 2
    sources, own_ref, targets = refs[:count], refs[count + 1], refs[count + 2 : -3]
    grad_ref, second_ref, sems = refs[-3:]
    moves = started(sources, (grad_ref, second_ref, *targets), sems)
    moves[0].wait()
    moves[1].wait()
    own_ref[...] = passed(grad_ref, second_ref)
    for move in moves[2:]:
        move.wait()


def local_kernel(dims, own_ref, before_ref, after_ref, first_ref, lid_ref, cam_ref, wa_ref, wb_ref, spot_ref,
                 lidar_ref, blocks_hbm, keep_ref, send_ref,
                 g_ref, a_ref, gt_ref, at_ref, pick_ref, block_sems):
    cols, ch, cam, parts = dims
    lid = lid_ref.shape[2]
    fan = cam + lid
    half = ch // 2
    ext = jnp.concatenate(
        [before_ref[0], before_ref[1], own_ref[0], own_ref[1], after_ref[0], after_ref[1]], axis=0
    ).astype(f32)
    for b in range(3):
        moved = shifted_columns(ext, b - 1, cols)
        g_ref[b] = moved.astype(bf16)
        gt_ref[b] = moved[cols : 5 * cols].astype(bf16).T
    back = jnp.zeros((4 * cols, ch), f32)
    for a in range(3):
        for b in range(3):
            tap = (3 * (2 - a) + (2 - b)) * ch
            back += mm(g_ref[b, a * cols : (a + 4) * cols, :], wb_ref[:, tap : tap + ch], NN)
    first = jnp.concatenate([before_ref[2], first_ref[0], first_ref[1], after_ref[2]], axis=0).astype(f32)
    grad_a = jnp.where(first > 0, back, 0.0).astype(bf16).astype(f32)
    for b in range(3):
        moved = shifted_columns(grad_a, b - 1, cols)
        a_ref[b] = moved.astype(bf16)
        at_ref[b] = moved.astype(bf16).T
    lidar = jnp.zeros((2 * cols, lid), f32)
    camera = jnp.zeros((cam, 2 * cols), f32)
    for a in range(3):
        for b in range(3):
            tap = (3 * (2 - a) + (2 - b)) * fan
            rows = a_ref[b, a * cols : (a + 2) * cols, :]
            lidar += mm(rows, wa_ref[tap + cam : tap + fan, :], NT)
            camera += mm(wa_ref[tap : tap + cam, :], rows, NT)
    for r in range(2):
        lidar_ref[r] = lidar[r * cols : (r + 1) * cols].astype(bf16)
    for r in range(2):
        pick_ref[r] = camera[:, r * cols : (r + 1) * cols].astype(bf16)
    picks = [
        pltpu.make_async_copy(pick_ref.at[jnp.where(spot_ref[2 + k] > 0, 1, 0)], blocks_hbm.at[k], block_sems.at[k])
        for k in range(blocks_hbm.shape[0])
    ]
    for pick in picks:
        pick.start()

    second_core = spot_ref[0] > 0
    per_part = keep_ref.shape[2] // TILE

    def put(value, tile):
        halves = value.reshape(ch // 16, 2, 8, value.shape[1])
        even = halves[:, 0].reshape(half, value.shape[1])
        odd = halves[:, 1].reshape(half, value.shape[1])
        mine = jnp.where(second_core, odd, even)
        other = jnp.where(second_core, even, odd).astype(bf16)
        for t in range(value.shape[1] // TILE):
            part, at = divmod(tile + t, per_part)
            part = part ^ spot_ref[1]
            here = slice(at * TILE, (at + 1) * TILE)
            keep_ref[part, :, here] = mine[:, t * TILE : (t + 1) * TILE]
            send_ref[part, :, here] = other[:, t * TILE : (t + 1) * TILE]

    hidden = jnp.maximum(jnp.concatenate([first_ref[0], first_ref[1]], axis=0), 0)
    lidar_in = jnp.concatenate([lid_ref[0], lid_ref[1]], axis=0)
    camera_in = jnp.concatenate([cam_ref[0], cam_ref[1]], axis=1)
    b_tiles, a_tiles = ch // TILE, lid // TILE
    packed = []
    for a in range(3):
        for b in range(3):
            tap = 3 * a + b
            window = slice((2 - a) * cols, (4 - a) * cols)
            put(mm(gt_ref[2 - b, :, window], hidden, NN), tap * b_tiles)
            put(mm(at_ref[2 - b, :, window], lidar_in, NN), 9 * b_tiles + tap * a_tiles)
            packed.append(mm(at_ref[2 - b, :, window], camera_in, NT))
    at = 9 * (b_tiles + a_tiles)
    spare = (parts * per_part - at) * TILE - 9 * cam
    packed.append(jnp.zeros((ch, spare), f32))
    put(jnp.concatenate(packed, axis=1), at)
    for pick in picks:
        pick.wait()


def depth_kernel(blocks_ref, weight_ref, context_ref, slot_ref, gc_ref, gd_ref, wt_ref, st_ref, s_ref, m_ref, d_ref):
    sources, cam, cells_of = blocks_ref.shape
    depth, pix = slot_ref.shape
    wide = st_ref.shape[1]
    wt_ref[...] = jnp.concatenate([weight_ref[...].astype(f32), jnp.zeros((wide - depth, pix), f32)], axis=0).T
    st_ref[...] = jnp.concatenate([slot_ref[...], jnp.full((wide - depth, pix), -1, jnp.int32)], axis=0).T
    context_t = context_ref[...].astype(f32).T.astype(bf16)
    pitch = s_ref.shape[0] // sources
    for s in range(sources):
        s_ref[s * pitch : s * pitch + pix, :] = mm(context_t, blocks_ref[s], NN)
    cells = lax.broadcasted_iota(jnp.int32, (cells_of, wide), 0)
    places = lax.broadcasted_iota(jnp.int32, (sources, wide), 0)
    shift = cells_of.bit_length() - 1

    def pixels(g, carry):
        base = pl.multiple_of(g * 8, 8)
        slots = st_ref[pl.ds(base, 8), :]
        weights = wt_ref[pl.ds(base, 8), :]
        found_rows = []
        for k in range(8):
            slot = slots[k : k + 1]
            at_cell = jnp.where(cells == (slot & (cells_of - 1)), 1.0, 0.0).astype(bf16)
            here = places == (slot >> shift)
            every = pl.ds(base + k, sources, stride=pitch)
            m_ref[every, :] = mm(jnp.where(here, weights[k : k + 1], 0.0).astype(bf16), at_cell, NT)
            found = mm(s_ref[every, :].astype(bf16), at_cell, NN)
            found_rows.append(jnp.sum(jnp.where(here, found, 0.0), axis=0, keepdims=True))
        d_ref[pl.ds(base, 8), :] = jnp.concatenate(found_rows, axis=0)
        return carry

    lax.fori_loop(0, pix // 8, pixels, 0)
    gd_ref[...] = d_ref[...].T[:depth]
    total = jnp.zeros((cam, pix), f32)
    for s in range(sources):
        total += mm(blocks_ref[s], m_ref[s * pitch : s * pitch + pix, :].astype(bf16), NT)
    gc_ref[...] = total


def first_sum(keep_ref, other_ref, a_ref, b_ref):
    rows = a_ref.shape[1]
    for k, (upper, lower) in enumerate([(1, 3), (2, 2)]):
        a_ref[k] = (keep_ref[upper, :rows] + other_ref[upper, :rows].astype(f32)).astype(bf16)
        b_ref[k] = (keep_ref[lower, rows:] + other_ref[lower, rows:].astype(f32)).astype(bf16)


def kept_sum(keep_ref, other_ref, own_ref, next_ref):
    rows = own_ref.shape[0] // 2
    upper, lower = slice(0, rows), slice(rows, 2 * rows)
    own_ref[...] = keep_ref[0] + other_ref[0].astype(f32)
    next_ref[upper] = keep_ref[3, upper] + other_ref[3, upper].astype(f32)
    next_ref[lower] = keep_ref[1, lower] + other_ref[1, lower].astype(f32)


def second_sum(own_ref, next_ref, a_ref, b_ref, out_ref, a_out_ref, b_out_ref):
    rows = a_ref.shape[1]
    upper, lower = slice(0, rows), slice(rows, 2 * rows)
    a_out_ref[...] = (next_ref[upper] + a_ref[1].astype(f32)).astype(bf16)
    b_out_ref[...] = (next_ref[lower] + b_ref[1].astype(f32)).astype(bf16)
    out_ref[upper] = own_ref[upper] + a_ref[0].astype(f32)
    out_ref[lower] = own_ref[lower] + b_ref[0].astype(f32)


def third_sum(own_ref, a_ref, b_ref, out_ref):
    rows = a_ref.shape[0]
    out_ref[:rows] = (own_ref[:rows] + a_ref[...].astype(f32)).astype(bf16)
    out_ref[rows:] = (own_ref[rows:] + b_ref[...].astype(f32)).astype(bf16)


def place_sum(parts_ref, out_ref):
    out_ref[...] = jnp.sum(parts_ref[...].astype(f32), axis=0).astype(bf16)


def pair_sum(one_ref, two_ref, out_ref):
    out_ref[...] = one_ref[...].astype(f32) + two_ref[...].astype(f32)


def last_sum(dims, scale, *refs):
    ch, lid, cam = dims
    *parts, spot_ref, wa_ref, wb_ref, all_ref = refs
    for k, part in enumerate(parts):
        all_ref[k ^ spot_ref[1]] = part[...]
    whole = jnp.concatenate([all_ref[x] for x in range(len(parts))], axis=1) * scale
    wb_ref[...] = whole[:, : 9 * ch]
    pieces = []
    for tap in range(9):
        at = 9 * (ch + lid) + tap * cam
        pieces += [whole[:, at : at + cam], whole[:, 9 * ch + tap * lid : 9 * ch + (tap + 1) * lid]]
    wa_ref[...] = jnp.concatenate(pieces, axis=1)


def call(kernel, outs, scratch, args, specs, flops, traffic, outs_at=None, limit=24):
    return pl.pallas_call(
        kernel,
        out_shape=outs,
        in_specs=specs,
        out_specs=outs_at or [VM] * len(outs),
        scratch_shapes=scratch,
        cost_estimate=pl.CostEstimate(flops=flops, bytes_accessed=traffic, transcendentals=0),
        compiler_params=pltpu.CompilerParams(vmem_limit_bytes=limit << 20),
    )(*[pltpu.with_memory_space_constraint(x, pltpu.HBM) if spec is HB else x for x, spec in zip(args, specs)])


def small(kernel, outs, args):
    outs = [jax.ShapeDtypeStruct(shape, dtype) for shape, dtype in outs]
    traffic = sum(x.size * x.dtype.itemsize for x in (*args, *outs))
    return call(kernel, outs, [], args, [VM] * len(args), traffic, traffic)


VM = pl.BlockSpec(memory_space=pltpu.VMEM)
SM = pl.BlockSpec(memory_space=pltpu.SMEM)
HB = pl.BlockSpec(memory_space=pltpu.HBM)


def neighbours(x, reverse):
    n = lax.axis_size("space")
    pairs = [(i, i + 1) for i in range(n - 1)]
    return lax.ppermute(x, "space", [(j, i) for i, j in pairs] if reverse else pairs)


def exchanged(x, axis, groups):
    return lax.all_to_all(x, axis, 0, 0, axis_index_groups=groups, tiled=True)


def swapped(x, axis, partner):
    return lax.ppermute(x, axis, [(i, partner(i)) for i in range(lax.axis_size(axis))])


def summed_along_x(keep, send):
    _, rows, per_part = keep.shape
    deep = rows // 2
    other = swapped(send, "space", lambda i: i ^ 1)
    a, b = small(first_sum, [((2, deep, per_part), bf16)] * 2, (keep, other))
    a, b = swapped(a, "scene", lambda i: i ^ 2), swapped(b, "scene", lambda i: i ^ 6)
    kept = small(kept_sum, [((2 * deep, per_part), f32)] * 2, (keep, other))
    own, a, b = small(
        second_sum,
        [((2 * deep, per_part), f32), ((deep, per_part), bf16), ((deep, per_part), bf16)],
        (*kept, a, b),
    )
    a, b = swapped(a, "scene", lambda i: i ^ 6), swapped(b, "scene", lambda i: i ^ 2)
    (part,) = small(third_sum, [((2 * deep, per_part), bf16)], (own, a, b))
    return part


def over_scenes(part, spot, dims, scale):
    ch, lid, cam = dims
    (own,) = small(pair_sum, [(part.shape, f32)], (part, swapped(part, "scene", lambda i: i ^ 1)))
    parts = [own] + [swapped(own, "scene", lambda i, k=k: i ^ 2 * k) for k in range(1, 4)]
    return call(
        functools.partial(last_sum, dims, scale),
        [jax.ShapeDtypeStruct((8, 9 * width), f32) for width in (cam + lid, ch)],
        [pltpu.VMEM((len(parts), *own.shape), f32)],
        (*parts, spot),
        [VM] * len(parts) + [SM],
        400_000,
        400_000,
    )


def shards(
    grad_out, pre_second, pre_first, camera_bev, lidar_bev, weight_a, weight_b,
    depth_weights, context, block_list, point_slot,
):
    _, rows, cols, ch = grad_out.shape
    cam, lid = camera_bev.shape[-1], lidar_bev.shape[-1]
    space, scenes = lax.axis_size("space"), lax.axis_size("scene")
    pix = point_slot.shape[1]
    place = space // 2
    reach = scenes // 2
    scale = 1.0 / math.sqrt(rows * cols * space * scenes)
    first = pre_first[0]
    shape = jax.ShapeDtypeStruct
    down, up = call(
        halo_kernel,
        [shape((k, cols, ch), bf16) for k in (rows + 1, rows + 1)],
        [pltpu.VMEM(first.shape, bf16)] * 3 + [pltpu.SemaphoreType.DMA((3,))],
        (grad_out[0], pre_second[0], first),
        [HB] * 3,
        1_000_000,
        1_000_000,
    )
    before, after = neighbours(down, False), neighbours(up, True)
    camera = jnp.swapaxes(camera_bev[0], 1, 2)
    spot = jnp.concatenate(
        [(lax.axis_index("space") & 1).reshape(1), (lax.axis_index("scene") >> 1).reshape(1), block_list[:, 0, 0]]
    )

    tiles = 9 * (ch + lid) // TILE + -(-9 * cam // TILE)
    per_part = -(-tiles // reach) * TILE
    own_data = (first, lidar_bev[0], camera, weight_a.T, weight_b)
    grad_b, *loaded = call(
        load_kernel,
        [pltpu.VMEM(x.shape, x.dtype) for x in (first, *own_data)],
        [pltpu.VMEM(first.shape, bf16)] * 2 + [pltpu.SemaphoreType.DMA((2 + len(own_data),))],
        (grad_out[0], pre_second[0], *own_data, spot),
        [HB] * (2 + len(own_data)) + [SM],
        2_000_000,
        3_500_000,
    )
    lidar, blocks, keep, send = call(
        functools.partial(local_kernel, (cols, ch, cam, reach)),
        [
            shape((rows, cols, lid), bf16),
            pltpu.HBM((space, cam, cols), bf16),
            shape((reach, ch // 2, per_part), f32),
            shape((reach, ch // 2, per_part), bf16),
        ],
        [
            pltpu.VMEM((3, 6 * cols, ch), bf16),
            pltpu.VMEM((3, 4 * cols, ch), bf16),
            pltpu.VMEM((3, ch, 4 * cols), bf16),
            pltpu.VMEM((3, ch, 4 * cols), bf16),
            pltpu.VMEM((2, cam, cols), bf16),
            pltpu.SemaphoreType.DMA((space,)),
        ],
        (grad_b, before, after, *loaded, spot),
        [VM] * 8 + [SM],
        1_800_000_000,
        12_000_000,
        outs_at=[VM, HB, VM, VM],
    )
    incoming = exchanged(blocks, "space", None)
    part = summed_along_x(keep, send)
    incoming, part = lax.optimization_barrier((incoming, part))
    along_yz = exchanged(
        part.reshape(place, 8, per_part), "space", [[2 * i + c for i in range(place)] for c in range(2)]
    )
    grad_context, grad_depth = call(
        depth_kernel,
        [shape((cam, pix), f32), shape(point_slot.shape, f32)],
        [
            pltpu.VMEM((pix, 128), f32),
            pltpu.VMEM((pix, 128), jnp.int32),
            pltpu.VMEM((space * (pix + 8), cols), f32),
            pltpu.VMEM((space * (pix + 8), cols), f32),
            pltpu.VMEM((pix, 128), f32),
        ],
        (incoming, depth_weights[0], context[0], point_slot),
        [VM] * 4,
        2_000_000_000,
        2_000_000,
    )
    along_yz, grad_context, grad_depth = lax.optimization_barrier((along_yz, grad_context, grad_depth))
    (part,) = small(place_sum, [((8, per_part), bf16)], (along_yz,))
    grad_wa, grad_wb = over_scenes(part, spot, (ch, lid, cam), scale)
    return grad_wa, grad_wb, lidar[None], grad_context[None], grad_depth[None]


def solution(mesh):
    field = P("scene", "space", None, None)
    pixels = P("scene", None, "space")
    return jax.shard_map(
        shards,
        mesh=mesh,
        in_specs=(field,) * 5 + (P(), P(), pixels, pixels, P(None, "space", None), P(None, "space")),
        out_specs=(P("space", None), P("space", None), field, pixels, pixels),
        check_vma=False,
    )
```

```python
import functools
import math

import jax
import jax.numpy as jnp
from jax import lax
from jax.experimental import pallas as pl
from jax.experimental.pallas import tpu as pltpu
from jax.sharding import PartitionSpec as P


f32 = jnp.float32
bf16 = jnp.bfloat16
NN = (((1,), (0,)), ((), ()))
NT = (((1,), (1,)), ((), ()))


def mm(a, b, dims):
    return lax.dot_general(a, b, dims, preferred_element_type=f32)


def shifted_columns(rows, step, cols):
    if step == 0:
        return rows
    zero = jnp.zeros((1, rows.shape[1]), rows.dtype)
    out = []
    for r in range(rows.shape[0] // cols):
        row = rows[r * cols : (r + 1) * cols]
        out += [row[1:], zero] if step > 0 else [zero, row[:-1]]
    return jnp.concatenate(out, axis=0)


TILE = 128


def started(sources, targets, sems):
    moves = [pltpu.make_async_copy(source, target, sems.at[k]) for k, (source, target) in enumerate(zip(sources, targets))]
    for move in moves:
        move.start()
    return moves


def passed(grad_ref, second_ref):
    return jnp.where(second_ref[...].astype(f32) > 0, grad_ref[...].astype(f32), 0.0).astype(bf16)


def halo_kernel(grad_hbm, second_hbm, first_hbm, down_ref, up_ref, grad_ref, second_ref, first_ref, sems):
    for move in started((grad_hbm, second_hbm, first_hbm), (grad_ref, second_ref, first_ref), sems):
        move.wait()
    rows = first_ref.shape[0]
    grad_b = passed(grad_ref, second_ref)
    down_ref[:rows] = grad_b
    up_ref[:rows] = grad_b
    down_ref[rows] = first_ref[rows - 1]
    up_ref[rows] = first_ref[0]


def load_kernel(*refs):
    count = (len(refs) - 3) // 2
    sources, own_ref, targets = refs[:count], refs[count + 1], refs[count + 2 : -3]
    grad_ref, second_ref, sems = refs[-3:]
    moves = started(sources, (grad_ref, second_ref, *targets), sems)
    moves[0].wait()
    moves[1].wait()
    own_ref[...] = passed(grad_ref, second_ref)
    for move in moves[2:]:
        move.wait()


def local_kernel(dims, own_ref, before_ref, after_ref, first_ref, lid_ref, cam_ref, wa_ref, wb_ref, spot_ref,
                 lidar_hbm, blocks_hbm, keep_ref, send_hbm,
                 g_ref, a_ref, gt_ref, at_ref, pick_ref, lidar_ref, send_ref, block_sems, out_sems):
    cols, ch, cam, parts = dims
    lid = lid_ref.shape[2]
    fan = cam + lid
    half = ch // 2
    ext = jnp.concatenate(
        [before_ref[0], before_ref[1], own_ref[0], own_ref[1], after_ref[0], after_ref[1]], axis=0
    ).astype(f32)
    for b in range(3):
        moved = shifted_columns(ext, b - 1, cols)
        g_ref[b] = moved.astype(bf16)
        gt_ref[b] = moved[cols : 5 * cols].astype(bf16).T
    back = jnp.zeros((4 * cols, ch), f32)
    for a in range(3):
        for b in range(3):
            tap = (3 * (2 - a) + (2 - b)) * ch
            back += mm(g_ref[b, a * cols : (a + 4) * cols, :], wb_ref[:, tap : tap + ch], NN)
    first = jnp.concatenate([before_ref[2], first_ref[0], first_ref[1], after_ref[2]], axis=0).astype(f32)
    grad_a = jnp.where(first > 0, back, 0.0).astype(bf16).astype(f32)
    for b in range(3):
        moved = shifted_columns(grad_a, b - 1, cols)
        a_ref[b] = moved.astype(bf16)
        at_ref[b] = moved.astype(bf16).T
    lidar = jnp.zeros((2 * cols, lid), f32)
    camera = jnp.zeros((cam, 2 * cols), f32)
    for a in range(3):
        for b in range(3):
            tap = (3 * (2 - a) + (2 - b)) * fan
            rows = a_ref[b, a * cols : (a + 2) * cols, :]
            lidar += mm(rows, wa_ref[tap + cam : tap + fan, :], NT)
            camera += mm(wa_ref[tap : tap + cam, :], rows, NT)
    for r in range(2):
        lidar_ref[r] = lidar[r * cols : (r + 1) * cols].astype(bf16)
    leaving = [pltpu.make_async_copy(lidar_ref, lidar_hbm, out_sems.at[parts])]
    leaving[0].start()
    for r in range(2):
        pick_ref[r] = camera[:, r * cols : (r + 1) * cols].astype(bf16)
    picks = [
        pltpu.make_async_copy(pick_ref.at[jnp.where(spot_ref[2 + k] > 0, 1, 0)], blocks_hbm.at[k], block_sems.at[k])
        for k in range(blocks_hbm.shape[0])
    ]
    for pick in picks:
        pick.start()

    second_core = spot_ref[0] > 0
    per_part = keep_ref.shape[2] // TILE

    def put(value, tile):
        halves = value.reshape(ch // 16, 2, 8, value.shape[1])
        even = halves[:, 0].reshape(half, value.shape[1])
        odd = halves[:, 1].reshape(half, value.shape[1])
        mine = jnp.where(second_core, odd, even).astype(bf16)
        other = jnp.where(second_core, even, odd).astype(bf16)
        for t in range(value.shape[1] // TILE):
            part, at = divmod(tile + t, per_part)
            part = part ^ spot_ref[1]
            here = slice(at * TILE, (at + 1) * TILE)
            keep_ref[part, :, here] = mine[:, t * TILE : (t + 1) * TILE]
            send_ref[part, :, here] = other[:, t * TILE : (t + 1) * TILE]

    hidden = jnp.maximum(jnp.concatenate([first_ref[0], first_ref[1]], axis=0), 0)
    lidar_in = jnp.concatenate([lid_ref[0], lid_ref[1]], axis=0)
    camera_in = jnp.concatenate([cam_ref[0], cam_ref[1]], axis=1)
    b_tiles, a_tiles = ch // TILE, lid // TILE
    windows = [(2 - b, slice((2 - a) * cols, (4 - a) * cols)) for a in range(3) for b in range(3)]

    def leave(first_part, end):
        for part in range(first_part, end):
            place = part ^ spot_ref[1]
            leaving.append(pltpu.make_async_copy(send_ref.at[place], send_hbm.at[place], out_sems.at[part]))
            leaving[-1].start()

    for tap, (b, window) in enumerate(windows):
        put(mm(gt_ref[b, :, window], hidden, NN), tap * b_tiles)
    gone = 9 * b_tiles // per_part
    leave(0, gone)
    for tap, (b, window) in enumerate(windows):
        put(mm(at_ref[b, :, window], lidar_in, NN), 9 * b_tiles + tap * a_tiles)
    at = 9 * (b_tiles + a_tiles)
    leave(gone, at // per_part)
    packed = [mm(at_ref[b, :, window], camera_in, NT) for b, window in windows]
    spare = (parts * per_part - at) * TILE - 9 * cam
    packed.append(jnp.zeros((ch, spare), f32))
    put(jnp.concatenate(packed, axis=1), at)
    leave(at // per_part, parts)
    for move in leaving:
        move.wait()
    for pick in picks:
        pick.wait()


def depth_kernel(blocks_ref, weight_ref, context_ref, slot_ref, gc_ref, gd_ref, wt_ref, st_ref, s_ref, m_ref, d_ref):
    sources, cam, cells_of = blocks_ref.shape
    depth, pix = slot_ref.shape
    wide = st_ref.shape[1]
    wt_ref[...] = jnp.concatenate([weight_ref[...].astype(f32), jnp.zeros((wide - depth, pix), f32)], axis=0).T
    st_ref[...] = jnp.concatenate([slot_ref[...], jnp.full((wide - depth, pix), -1, jnp.int32)], axis=0).T
    context_t = context_ref[...].astype(f32).T.astype(bf16)
    pitch = s_ref.shape[0] // sources
    for s in range(sources):
        s_ref[s * pitch : s * pitch + pix, :] = mm(context_t, blocks_ref[s], NN)
    cells = lax.broadcasted_iota(jnp.int32, (cells_of, wide), 0)
    places = lax.broadcasted_iota(jnp.int32, (sources, wide), 0)
    shift = cells_of.bit_length() - 1

    def pixels(g, carry):
        base = pl.multiple_of(g * 8, 8)
        slots = st_ref[pl.ds(base, 8), :]
        weights = wt_ref[pl.ds(base, 8), :]
        found_rows = []
        for k in range(8):
            slot = slots[k : k + 1]
            at_cell = jnp.where(cells == (slot & (cells_of - 1)), 1.0, 0.0).astype(bf16)
            here = places == (slot >> shift)
            every = pl.ds(base + k, sources, stride=pitch)
            m_ref[every, :] = mm(jnp.where(here, weights[k : k + 1], 0.0).astype(bf16), at_cell, NT)
            found = mm(s_ref[every, :].astype(bf16), at_cell, NN)
            found_rows.append(jnp.sum(jnp.where(here, found, 0.0), axis=0, keepdims=True))
        d_ref[pl.ds(base, 8), :] = jnp.concatenate(found_rows, axis=0)
        return carry

    lax.fori_loop(0, pix // 8, pixels, 0)
    gd_ref[...] = d_ref[...].T[:depth]
    total = jnp.zeros((cam, pix), f32)
    for s in range(sources):
        total += mm(blocks_ref[s], m_ref[s * pitch : s * pitch + pix, :].astype(bf16), NT)
    gc_ref[...] = total


def added(keep_ref, other_ref, part, rows):
    return keep_ref[part, rows].astype(f32) + other_ref[part, rows].astype(f32)


def first_sum(keep_ref, other_ref, a_ref, b_ref):
    rows = a_ref.shape[1]
    for k, (upper, lower) in enumerate([(1, 3), (2, 2)]):
        a_ref[k] = added(keep_ref, other_ref, upper, slice(0, rows)).astype(bf16)
        b_ref[k] = added(keep_ref, other_ref, lower, slice(rows, 2 * rows)).astype(bf16)


def kept_sum(keep_ref, other_ref, own_ref, next_ref):
    rows = own_ref.shape[0] // 2
    for here, part in [(slice(0, rows), 3), (slice(rows, 2 * rows), 1)]:
        own_ref[here] = added(keep_ref, other_ref, 0, here)
        next_ref[here] = added(keep_ref, other_ref, part, here)


def second_sum(own_ref, next_ref, a_ref, b_ref, out_ref, a_out_ref, b_out_ref):
    rows = a_ref.shape[1]
    upper, lower = slice(0, rows), slice(rows, 2 * rows)
    a_out_ref[...] = (next_ref[upper] + a_ref[1].astype(f32)).astype(bf16)
    b_out_ref[...] = (next_ref[lower] + b_ref[1].astype(f32)).astype(bf16)
    out_ref[upper] = own_ref[upper] + a_ref[0].astype(f32)
    out_ref[lower] = own_ref[lower] + b_ref[0].astype(f32)


def third_sum(own_ref, a_ref, b_ref, out_ref):
    rows = a_ref.shape[0]
    out_ref[:rows] = (own_ref[:rows] + a_ref[...].astype(f32)).astype(bf16)
    out_ref[rows:] = (own_ref[rows:] + b_ref[...].astype(f32)).astype(bf16)


def place_sum(parts_ref, out_ref):
    out_ref[...] = jnp.sum(parts_ref[...].astype(f32), axis=0).astype(bf16)


def pair_sum(one_ref, two_ref, out_ref):
    total = one_ref[...].astype(f32) + two_ref[...].astype(f32)
    for k in range(out_ref.shape[0]):
        out_ref[k] = total


def last_sum(dims, scale, parts_ref, wa_ref, wb_ref):
    ch, lid, cam = dims
    whole = jnp.concatenate([parts_ref[x] for x in range(parts_ref.shape[0])], axis=1) * scale
    wb_ref[...] = whole[:, : 9 * ch]
    pieces = []
    for tap in range(9):
        at = 9 * (ch + lid) + tap * cam
        pieces += [whole[:, at : at + cam], whole[:, 9 * ch + tap * lid : 9 * ch + (tap + 1) * lid]]
    wa_ref[...] = jnp.concatenate(pieces, axis=1)


def call(kernel, outs, scratch, args, specs, flops, traffic, outs_at=None, limit=24):
    return pl.pallas_call(
        kernel,
        out_shape=outs,
        in_specs=specs,
        out_specs=outs_at or [VM] * len(outs),
        scratch_shapes=scratch,
        cost_estimate=pl.CostEstimate(flops=flops, bytes_accessed=traffic, transcendentals=0),
        compiler_params=pltpu.CompilerParams(vmem_limit_bytes=limit << 20),
    )(*[pltpu.with_memory_space_constraint(x, pltpu.HBM) if spec is HB else x for x, spec in zip(args, specs)])


def small(kernel, outs, args):
    outs = [jax.ShapeDtypeStruct(shape, dtype) for shape, dtype in outs]
    traffic = sum(x.size * x.dtype.itemsize for x in (*args, *outs))
    return call(kernel, outs, [], args, [VM] * len(args), traffic, traffic)


VM = pl.BlockSpec(memory_space=pltpu.VMEM)
SM = pl.BlockSpec(memory_space=pltpu.SMEM)
HB = pl.BlockSpec(memory_space=pltpu.HBM)


def neighbours(x, reverse):
    n = lax.axis_size("space")
    pairs = [(i, i + 1) for i in range(n - 1)]
    return lax.ppermute(x, "space", [(j, i) for i, j in pairs] if reverse else pairs)


def exchanged(x, axis, groups):
    return lax.all_to_all(x, axis, 0, 0, axis_index_groups=groups, tiled=True)


def swapped(x, axis, partner):
    return lax.ppermute(x, axis, [(i, partner(i)) for i in range(lax.axis_size(axis))])


def summed_along_x(keep, send):
    _, rows, per_part = keep.shape
    deep = rows // 2
    other = swapped(send, "space", lambda i: i ^ 1)
    a, b = small(first_sum, [((2, deep, per_part), bf16)] * 2, (keep, other))
    a, b = swapped(a, "scene", lambda i: i ^ 2), swapped(b, "scene", lambda i: i ^ 6)
    kept = small(kept_sum, [((2 * deep, per_part), f32)] * 2, (keep, other))
    own, a, b = small(
        second_sum,
        [((2 * deep, per_part), f32), ((deep, per_part), bf16), ((deep, per_part), bf16)],
        (*kept, a, b),
    )
    a, b = swapped(a, "scene", lambda i: i ^ 6), swapped(b, "scene", lambda i: i ^ 2)
    (part,) = small(third_sum, [((2 * deep, per_part), bf16)], (own, a, b))
    return part


def over_scenes(part, dims, scale):
    ch, lid, cam = dims
    reach = lax.axis_size("scene") // 2
    (spread,) = small(pair_sum, [((reach, *part.shape), f32)], (part, swapped(part, "scene", lambda i: i ^ 1)))
    parts = exchanged(spread, "scene", [[2 * i + h for i in range(reach)] for h in range(2)])
    return small(
        functools.partial(last_sum, dims, scale),
        [((part.shape[0], 9 * width), f32) for width in (cam + lid, ch)],
        (parts,),
    )


def shards(
    grad_out, pre_second, pre_first, camera_bev, lidar_bev, weight_a, weight_b,
    depth_weights, context, block_list, point_slot,
):
    _, rows, cols, ch = grad_out.shape
    cam, lid = camera_bev.shape[-1], lidar_bev.shape[-1]
    space, scenes = lax.axis_size("space"), lax.axis_size("scene")
    pix = point_slot.shape[1]
    place = space // 2
    reach = scenes // 2
    scale = 1.0 / math.sqrt(rows * cols * space * scenes)
    first = pre_first[0]
    shape = jax.ShapeDtypeStruct
    down, up = call(
        halo_kernel,
        [shape((k, cols, ch), bf16) for k in (rows + 1, rows + 1)],
        [pltpu.VMEM(first.shape, bf16)] * 3 + [pltpu.SemaphoreType.DMA((3,))],
        (grad_out[0], pre_second[0], first),
        [HB] * 3,
        1_000_000,
        1_000_000,
    )
    before, after = neighbours(down, False), neighbours(up, True)
    camera = jnp.swapaxes(camera_bev[0], 1, 2)
    spot = jnp.concatenate(
        [(lax.axis_index("space") & 1).reshape(1), (lax.axis_index("scene") >> 1).reshape(1), block_list[:, 0, 0]]
    )

    tiles = 9 * (ch + lid) // TILE + -(-9 * cam // TILE)
    per_part = -(-tiles // reach) * TILE
    own_data = (first, lidar_bev[0], camera, weight_a.T, weight_b)
    grad_b, *loaded = call(
        load_kernel,
        [pltpu.VMEM(x.shape, x.dtype) for x in (first, *own_data)],
        [pltpu.VMEM(first.shape, bf16)] * 2 + [pltpu.SemaphoreType.DMA((2 + len(own_data),))],
        (grad_out[0], pre_second[0], *own_data, spot),
        [HB] * (2 + len(own_data)) + [SM],
        2_000_000,
        3_500_000,
    )
    lidar, blocks, keep, send = call(
        functools.partial(local_kernel, (cols, ch, cam, reach)),
        [
            pltpu.HBM((rows, cols, lid), bf16),
            pltpu.HBM((space, cam, cols), bf16),
            shape((reach, ch // 2, per_part), bf16),
            pltpu.HBM((reach, ch // 2, per_part), bf16),
        ],
        [
            pltpu.VMEM((3, 6 * cols, ch), bf16),
            pltpu.VMEM((3, 4 * cols, ch), bf16),
            pltpu.VMEM((3, ch, 4 * cols), bf16),
            pltpu.VMEM((3, ch, 4 * cols), bf16),
            pltpu.VMEM((2, cam, cols), bf16),
            pltpu.VMEM((rows, cols, lid), bf16),
            pltpu.VMEM((reach, ch // 2, per_part), bf16),
            pltpu.SemaphoreType.DMA((space,)),
            pltpu.SemaphoreType.DMA((reach + 1,)),
        ],
        (grad_b, before, after, *loaded, spot),
        [VM] * 8 + [SM],
        1_800_000_000,
        12_000_000,
        outs_at=[HB, HB, VM, HB],
    )
    incoming = exchanged(blocks, "space", None)
    part = summed_along_x(keep, send)
    incoming, part = lax.optimization_barrier((incoming, part))
    along_yz = exchanged(
        part.reshape(place, 8, per_part), "space", [[2 * i + c for i in range(place)] for c in range(2)]
    )
    grad_context, grad_depth = call(
        depth_kernel,
        [shape((cam, pix), f32), shape(point_slot.shape, f32)],
        [
            pltpu.VMEM((pix, 128), f32),
            pltpu.VMEM((pix, 128), jnp.int32),
            pltpu.VMEM((space * (pix + 8), cols), f32),
            pltpu.VMEM((space * (pix + 8), cols), f32),
            pltpu.VMEM((pix, 128), f32),
        ],
        (incoming, depth_weights[0], context[0], point_slot),
        [VM] * 4,
        2_000_000_000,
        2_000_000,
    )
    along_yz, grad_context, grad_depth = lax.optimization_barrier((along_yz, grad_context, grad_depth))
    (part,) = small(place_sum, [((8, per_part), bf16)], (along_yz,))
    grad_wa, grad_wb = over_scenes(part, (ch, lid, cam), scale)
    return grad_wa, grad_wb, lidar[None], grad_context[None], grad_depth[None]


def solution(mesh):
    field = P("scene", "space", None, None)
    pixels = P("scene", None, "space")
    return jax.shard_map(
        shards,
        mesh=mesh,
        in_specs=(field,) * 5 + (P(), P(), pixels, pixels, P(None, "space", None), P(None, "space")),
        out_specs=(P("space", None), P("space", None), field, pixels, pixels),
        check_vma=False,
    )
```

```python
import functools
import math

import jax
import jax.numpy as jnp
from jax import lax
from jax.experimental import pallas as pl
from jax.experimental.pallas import tpu as pltpu
from jax.sharding import PartitionSpec as P


f32 = jnp.float32
bf16 = jnp.bfloat16
NN = (((1,), (0,)), ((), ()))
NT = (((1,), (1,)), ((), ()))


def mm(a, b, dims):
    return lax.dot_general(a, b, dims, preferred_element_type=f32)


def shifted_columns(rows, step, cols):
    if step == 0:
        return rows
    zero = jnp.zeros((1, rows.shape[1]), rows.dtype)
    out = []
    for r in range(rows.shape[0] // cols):
        row = rows[r * cols : (r + 1) * cols]
        out += [row[1:], zero] if step > 0 else [zero, row[:-1]]
    return jnp.concatenate(out, axis=0)


TILE = 128


def started(sources, targets, sems):
    moves = [pltpu.make_async_copy(source, target, sems.at[k]) for k, (source, target) in enumerate(zip(sources, targets))]
    for move in moves:
        move.start()
    return moves


def passed(grad_ref, second_ref):
    return jnp.where(second_ref[...].astype(f32) > 0, grad_ref[...].astype(f32), 0.0).astype(bf16)


def halo_kernel(grad_hbm, second_hbm, first_hbm, near_ref, far_ref, grad_ref, second_ref, first_ref, sems):
    for move in started((grad_hbm, second_hbm, first_hbm), (grad_ref, second_ref, first_ref), sems):
        move.wait()
    rows = first_ref.shape[0]
    odd = lax.axis_index("space") & 1
    grad_b = passed(grad_ref, second_ref)
    near_ref[:rows] = grad_b
    far_ref[:rows] = grad_b
    near_ref[rows] = first_ref[(rows - 1) * (1 - odd)]
    far_ref[rows] = first_ref[(rows - 1) * odd]


def load_kernel(*refs):
    count = (len(refs) - 3) // 2
    sources, own_ref, targets = refs[:count], refs[count + 1], refs[count + 2 : -3]
    grad_ref, second_ref, sems = refs[-3:]
    moves = started(sources, (grad_ref, second_ref, *targets), sems)
    moves[0].wait()
    moves[1].wait()
    own_ref[...] = passed(grad_ref, second_ref)
    for move in moves[2:]:
        move.wait()


def local_kernel(dims, own_ref, near_ref, far_ref, first_ref, lid_ref, cam_ref, wa_ref, wb_ref, spot_ref,
                 lidar_hbm, blocks_hbm, keep_ref, send_hbm,
                 g_ref, a_ref, gt_ref, at_ref, pick_ref, lidar_ref, send_ref, block_sems, out_sems):
    cols, ch, cam, parts = dims
    lid = lid_ref.shape[2]
    fan = cam + lid
    half = ch // 2
    second_core = spot_ref[0] > 0
    near = [near_ref[k].astype(f32) for k in range(3)]
    far = [far_ref[k].astype(f32) for k in range(3)]
    before = [jnp.where(second_core, n, f) for n, f in zip(near, far)]
    after = [jnp.where(second_core, f, n) for n, f in zip(near, far)]
    own = [own_ref[k].astype(f32) for k in range(2)]
    ext = jnp.concatenate([*before[:2], *own, *after[:2]], axis=0)
    for b in range(3):
        moved = shifted_columns(ext, b - 1, cols)
        g_ref[b] = moved.astype(bf16)
        gt_ref[b] = moved[cols : 5 * cols].astype(bf16).T
    back = jnp.zeros((4 * cols, ch), f32)
    for a in range(3):
        for b in range(3):
            tap = (3 * (2 - a) + (2 - b)) * ch
            back += mm(g_ref[b, a * cols : (a + 4) * cols, :], wb_ref[:, tap : tap + ch], NN)
    first = jnp.concatenate([before[2], first_ref[0].astype(f32), first_ref[1].astype(f32), after[2]], axis=0)
    grad_a = jnp.where(first > 0, back, 0.0).astype(bf16).astype(f32)
    for b in range(3):
        moved = shifted_columns(grad_a, b - 1, cols)
        a_ref[b] = moved.astype(bf16)
        at_ref[b] = moved.astype(bf16).T
    lidar = jnp.zeros((2 * cols, lid), f32)
    camera = jnp.zeros((cam, 2 * cols), f32)
    for a in range(3):
        for b in range(3):
            tap = (3 * (2 - a) + (2 - b)) * fan
            rows = a_ref[b, a * cols : (a + 2) * cols, :]
            lidar += mm(rows, wa_ref[tap + cam : tap + fan, :], NT)
            camera += mm(wa_ref[tap : tap + cam, :], rows, NT)
    for r in range(2):
        lidar_ref[r] = lidar[r * cols : (r + 1) * cols].astype(bf16)
    leaving = [pltpu.make_async_copy(lidar_ref, lidar_hbm, out_sems.at[parts])]
    leaving[0].start()
    for r in range(2):
        pick_ref[r] = camera[:, r * cols : (r + 1) * cols].astype(bf16)
    picks = [
        pltpu.make_async_copy(pick_ref.at[jnp.where(spot_ref[2 + k] > 0, 1, 0)], blocks_hbm.at[k], block_sems.at[k])
        for k in range(blocks_hbm.shape[0])
    ]
    for pick in picks:
        pick.start()

    per_part = keep_ref.shape[2] // TILE

    def put(value, tile):
        halves = value.reshape(ch // 16, 2, 8, value.shape[1])
        even = halves[:, 0].reshape(half, value.shape[1])
        odd = halves[:, 1].reshape(half, value.shape[1])
        mine = jnp.where(second_core, odd, even).astype(bf16)
        other = jnp.where(second_core, even, odd).astype(bf16)
        for t in range(value.shape[1] // TILE):
            part, at = divmod(tile + t, per_part)
            part = part ^ spot_ref[1]
            here = slice(at * TILE, (at + 1) * TILE)
            keep_ref[part, :, here] = mine[:, t * TILE : (t + 1) * TILE]
            send_ref[part, :, here] = other[:, t * TILE : (t + 1) * TILE]

    hidden = jnp.maximum(jnp.concatenate([first_ref[0], first_ref[1]], axis=0), 0)
    lidar_in = jnp.concatenate([lid_ref[0], lid_ref[1]], axis=0)
    camera_in = jnp.concatenate([cam_ref[0], cam_ref[1]], axis=1)
    b_tiles, a_tiles = ch // TILE, lid // TILE
    windows = [(2 - b, slice((2 - a) * cols, (4 - a) * cols)) for a in range(3) for b in range(3)]

    def leave(first_part, end):
        for part in range(first_part, end):
            place = part ^ spot_ref[1]
            leaving.append(pltpu.make_async_copy(send_ref.at[place], send_hbm.at[place], out_sems.at[part]))
            leaving[-1].start()

    for tap, (b, window) in enumerate(windows):
        put(mm(gt_ref[b, :, window], hidden, NN), tap * b_tiles)
    gone = 9 * b_tiles // per_part
    leave(0, gone)
    for tap, (b, window) in enumerate(windows):
        put(mm(at_ref[b, :, window], lidar_in, NN), 9 * b_tiles + tap * a_tiles)
    at = 9 * (b_tiles + a_tiles)
    leave(gone, at // per_part)
    packed = [mm(at_ref[b, :, window], camera_in, NT) for b, window in windows]
    spare = (parts * per_part - at) * TILE - 9 * cam
    packed.append(jnp.zeros((ch, spare), f32))
    put(jnp.concatenate(packed, axis=1), at)
    leave(at // per_part, parts)
    for move in leaving:
        move.wait()
    for pick in picks:
        pick.wait()


def depth_kernel(blocks_ref, weight_ref, context_ref, slot_ref, gc_ref, gd_ref, wt_ref, st_ref, s_ref, m_ref, d_ref):
    sources, cam, cells_of = blocks_ref.shape
    depth, pix = slot_ref.shape
    wide = st_ref.shape[1]
    wt_ref[...] = jnp.concatenate([weight_ref[...].astype(f32), jnp.zeros((wide - depth, pix), f32)], axis=0).T
    st_ref[...] = jnp.concatenate([slot_ref[...], jnp.full((wide - depth, pix), -1, jnp.int32)], axis=0).T
    context_t = context_ref[...].astype(f32).T.astype(bf16)
    pitch = s_ref.shape[0] // sources
    for s in range(sources):
        s_ref[s * pitch : s * pitch + pix, :] = mm(context_t, blocks_ref[s], NN)
    cells = lax.broadcasted_iota(jnp.int32, (cells_of, wide), 0)
    places = lax.broadcasted_iota(jnp.int32, (sources, wide), 0)
    shift = cells_of.bit_length() - 1

    def pixels(g, carry):
        base = pl.multiple_of(g * 8, 8)
        slots = st_ref[pl.ds(base, 8), :]
        weights = wt_ref[pl.ds(base, 8), :]
        found_rows = []
        for k in range(8):
            slot = slots[k : k + 1]
            at_cell = jnp.where(cells == (slot & (cells_of - 1)), 1.0, 0.0).astype(bf16)
            here = places == (slot >> shift)
            every = pl.ds(base + k, sources, stride=pitch)
            m_ref[every, :] = mm(jnp.where(here, weights[k : k + 1], 0.0).astype(bf16), at_cell, NT)
            found = mm(s_ref[every, :].astype(bf16), at_cell, NN)
            found_rows.append(jnp.sum(jnp.where(here, found, 0.0), axis=0, keepdims=True))
        d_ref[pl.ds(base, 8), :] = jnp.concatenate(found_rows, axis=0)
        return carry

    lax.fori_loop(0, pix // 8, pixels, 0)
    gd_ref[...] = d_ref[...].T[:depth]
    total = jnp.zeros((cam, pix), f32)
    for s in range(sources):
        total += mm(blocks_ref[s], m_ref[s * pitch : s * pitch + pix, :].astype(bf16), NT)
    gc_ref[...] = total


def added(keep_ref, other_ref, part, rows):
    return keep_ref[part, rows].astype(f32) + other_ref[part, rows].astype(f32)


def first_sum(keep_ref, other_ref, a_ref, b_ref):
    rows = a_ref.shape[1]
    for k, (upper, lower) in enumerate([(1, 3), (2, 2)]):
        a_ref[k] = added(keep_ref, other_ref, upper, slice(0, rows)).astype(bf16)
        b_ref[k] = added(keep_ref, other_ref, lower, slice(rows, 2 * rows)).astype(bf16)


def kept_sum(keep_ref, other_ref, own_ref, next_ref):
    rows = own_ref.shape[0] // 2
    for here, part in [(slice(0, rows), 3), (slice(rows, 2 * rows), 1)]:
        own_ref[here] = added(keep_ref, other_ref, 0, here)
        next_ref[here] = added(keep_ref, other_ref, part, here)


def second_sum(own_ref, next_ref, a_ref, b_ref, out_ref, a_out_ref, b_out_ref):
    rows = a_ref.shape[1]
    upper, lower = slice(0, rows), slice(rows, 2 * rows)
    a_out_ref[...] = (next_ref[upper] + a_ref[1].astype(f32)).astype(bf16)
    b_out_ref[...] = (next_ref[lower] + b_ref[1].astype(f32)).astype(bf16)
    out_ref[upper] = own_ref[upper] + a_ref[0].astype(f32)
    out_ref[lower] = own_ref[lower] + b_ref[0].astype(f32)


def third_sum(own_ref, a_ref, b_ref, out_ref):
    rows = a_ref.shape[0]
    out_ref[:rows] = (own_ref[:rows] + a_ref[...].astype(f32)).astype(bf16)
    out_ref[rows:] = (own_ref[rows:] + b_ref[...].astype(f32)).astype(bf16)


def place_sum(parts_ref, out_ref):
    out_ref[...] = jnp.sum(parts_ref[...].astype(f32), axis=0).astype(bf16)


def pair_sum(one_ref, two_ref, out_ref):
    out_ref[...] = one_ref[...].astype(f32) + two_ref[...].astype(f32)


def last_sum(dims, scale, *refs):
    ch, lid, cam = dims
    *parts, spot_ref, wa_ref, wb_ref, all_ref = refs
    for k, part in enumerate(parts):
        all_ref[k ^ spot_ref[1]] = part[...]
    whole = jnp.concatenate([all_ref[x] for x in range(len(parts))], axis=1) * scale
    wb_ref[...] = whole[:, : 9 * ch]
    pieces = []
    for tap in range(9):
        at = 9 * (ch + lid) + tap * cam
        pieces += [whole[:, at : at + cam], whole[:, 9 * ch + tap * lid : 9 * ch + (tap + 1) * lid]]
    wa_ref[...] = jnp.concatenate(pieces, axis=1)


def call(kernel, outs, scratch, args, specs, flops, traffic, outs_at=None, limit=24):
    return pl.pallas_call(
        kernel,
        out_shape=outs,
        in_specs=specs,
        out_specs=outs_at or [VM] * len(outs),
        scratch_shapes=scratch,
        cost_estimate=pl.CostEstimate(flops=flops, bytes_accessed=traffic, transcendentals=0),
        compiler_params=pltpu.CompilerParams(vmem_limit_bytes=limit << 20),
    )(*[pltpu.with_memory_space_constraint(x, pltpu.HBM) if spec is HB else x for x, spec in zip(args, specs)])


def small(kernel, outs, args):
    outs = [jax.ShapeDtypeStruct(shape, dtype) for shape, dtype in outs]
    traffic = sum(x.size * x.dtype.itemsize for x in (*args, *outs))
    return call(kernel, outs, [], args, [VM] * len(args), traffic, traffic)


VM = pl.BlockSpec(memory_space=pltpu.VMEM)
SM = pl.BlockSpec(memory_space=pltpu.SMEM)
HB = pl.BlockSpec(memory_space=pltpu.HBM)


def exchanged(x, axis, groups):
    return lax.all_to_all(x, axis, 0, 0, axis_index_groups=groups, tiled=True)


def swapped(x, axis, partner):
    return lax.ppermute(x, axis, [(i, partner(i)) for i in range(lax.axis_size(axis))])


def summed_along_x(keep, send):
    _, rows, per_part = keep.shape
    deep = rows // 2
    other = swapped(send, "space", lambda i: i ^ 1)
    a, b = small(first_sum, [((2, deep, per_part), bf16)] * 2, (keep, other))
    a, b = swapped(a, "scene", lambda i: i ^ 2), swapped(b, "scene", lambda i: i ^ 6)
    kept = small(kept_sum, [((2 * deep, per_part), f32)] * 2, (keep, other))
    own, a, b = small(
        second_sum,
        [((2 * deep, per_part), f32), ((deep, per_part), bf16), ((deep, per_part), bf16)],
        (*kept, a, b),
    )
    a, b = swapped(a, "scene", lambda i: i ^ 6), swapped(b, "scene", lambda i: i ^ 2)
    (part,) = small(third_sum, [((2 * deep, per_part), bf16)], (own, a, b))
    return part


def over_scenes(part, spot, dims, scale):
    ch, lid, cam = dims
    (own,) = small(pair_sum, [(part.shape, f32)], (part, swapped(part, "scene", lambda i: i ^ 1)))
    parts = [own] + [swapped(own, "scene", lambda i, k=k: i ^ 2 * k) for k in range(1, 4)]
    return call(
        functools.partial(last_sum, dims, scale),
        [jax.ShapeDtypeStruct((8, 9 * width), f32) for width in (cam + lid, ch)],
        [pltpu.VMEM((len(parts), *own.shape), f32)],
        (*parts, spot),
        [VM] * len(parts) + [SM],
        400_000,
        400_000,
    )


def shards(
    grad_out, pre_second, pre_first, camera_bev, lidar_bev, weight_a, weight_b,
    depth_weights, context, block_list, point_slot,
):
    _, rows, cols, ch = grad_out.shape
    cam, lid = camera_bev.shape[-1], lidar_bev.shape[-1]
    space, scenes = lax.axis_size("space"), lax.axis_size("scene")
    pix = point_slot.shape[1]
    place = space // 2
    reach = scenes // 2
    scale = 1.0 / math.sqrt(rows * cols * space * scenes)
    first = pre_first[0]
    shape = jax.ShapeDtypeStruct
    near, far = call(
        halo_kernel,
        [shape((k, cols, ch), bf16) for k in (rows + 1, rows + 1)],
        [pltpu.VMEM(first.shape, bf16)] * 3 + [pltpu.SemaphoreType.DMA((3,))],
        (grad_out[0], pre_second[0], first),
        [HB] * 3,
        1_000_000,
        1_000_000,
    )
    sides = [(i, i + 1) for i in range(1, space - 1, 2)]
    far = lax.ppermute(far, "space", sides + [(j, i) for i, j in sides])
    near = swapped(near, "space", lambda i: i ^ 1)
    camera = jnp.swapaxes(camera_bev[0], 1, 2)
    spot = jnp.concatenate(
        [(lax.axis_index("space") & 1).reshape(1), (lax.axis_index("scene") >> 1).reshape(1), block_list[:, 0, 0]]
    )

    tiles = 9 * (ch + lid) // TILE + -(-9 * cam // TILE)
    per_part = -(-tiles // reach) * TILE
    own_data = (first, lidar_bev[0], camera, weight_a.T, weight_b)
    grad_b, *loaded = call(
        load_kernel,
        [pltpu.VMEM(x.shape, x.dtype) for x in (first, *own_data)],
        [pltpu.VMEM(first.shape, bf16)] * 2 + [pltpu.SemaphoreType.DMA((2 + len(own_data),))],
        (grad_out[0], pre_second[0], *own_data, spot),
        [HB] * (2 + len(own_data)) + [SM],
        2_000_000,
        3_500_000,
    )
    lidar, blocks, keep, send = call(
        functools.partial(local_kernel, (cols, ch, cam, reach)),
        [
            pltpu.HBM((rows, cols, lid), bf16),
            pltpu.HBM((space, cam, cols), bf16),
            shape((reach, ch // 2, per_part), bf16),
            pltpu.HBM((reach, ch // 2, per_part), bf16),
        ],
        [
            pltpu.VMEM((3, 6 * cols, ch), bf16),
            pltpu.VMEM((3, 4 * cols, ch), bf16),
            pltpu.VMEM((3, ch, 4 * cols), bf16),
            pltpu.VMEM((3, ch, 4 * cols), bf16),
            pltpu.VMEM((2, cam, cols), bf16),
            pltpu.VMEM((rows, cols, lid), bf16),
            pltpu.VMEM((reach, ch // 2, per_part), bf16),
            pltpu.SemaphoreType.DMA((space,)),
            pltpu.SemaphoreType.DMA((reach + 1,)),
        ],
        (grad_b, near, far, *loaded, spot),
        [VM] * 8 + [SM],
        1_800_000_000,
        12_000_000,
        outs_at=[HB, HB, VM, HB],
    )
    incoming = exchanged(blocks, "space", None)
    part = summed_along_x(keep, send)
    incoming, part = lax.optimization_barrier((incoming, part))
    along_yz = exchanged(
        part.reshape(place, 8, per_part), "space", [[2 * i + c for i in range(place)] for c in range(2)]
    )
    grad_context, grad_depth = call(
        depth_kernel,
        [shape((cam, pix), f32), shape(point_slot.shape, f32)],
        [
            pltpu.VMEM((pix, 128), f32),
            pltpu.VMEM((pix, 128), jnp.int32),
            pltpu.VMEM((space * (pix + 8), cols), f32),
            pltpu.VMEM((space * (pix + 8), cols), f32),
            pltpu.VMEM((pix, 128), f32),
        ],
        (incoming, depth_weights[0], context[0], point_slot),
        [VM] * 4,
        2_000_000_000,
        2_000_000,
    )
    along_yz, grad_context, grad_depth = lax.optimization_barrier((along_yz, grad_context, grad_depth))
    (part,) = small(place_sum, [((8, per_part), bf16)], (along_yz,))
    grad_wa, grad_wb = over_scenes(part, spot, (ch, lid, cam), scale)
    return grad_wa, grad_wb, lidar[None], grad_context[None], grad_depth[None]


def solution(mesh):
    field = P("scene", "space", None, None)
    pixels = P("scene", None, "space")
    return jax.shard_map(
        shards,
        mesh=mesh,
        in_specs=(field,) * 5 + (P(), P(), pixels, pixels, P(None, "space", None), P(None, "space")),
        out_specs=(P("space", None), P("space", None), field, pixels, pixels),
        check_vma=False,
    )
```

```python
import functools
import math

import jax
import jax.numpy as jnp
from jax import lax
from jax.experimental import pallas as pl
from jax.experimental.pallas import tpu as pltpu
from jax.sharding import PartitionSpec as P


f32 = jnp.float32
bf16 = jnp.bfloat16
NN = (((1,), (0,)), ((), ()))
NT = (((1,), (1,)), ((), ()))


def mm(a, b, dims):
    return lax.dot_general(a, b, dims, preferred_element_type=f32)


def shifted_columns(rows, step, cols):
    if step == 0:
        return rows
    zero = jnp.zeros((1, rows.shape[1]), rows.dtype)
    out = []
    for r in range(rows.shape[0] // cols):
        row = rows[r * cols : (r + 1) * cols]
        out += [row[1:], zero] if step > 0 else [zero, row[:-1]]
    return jnp.concatenate(out, axis=0)


TILE = 128


def started(sources, targets, sems):
    moves = [pltpu.make_async_copy(source, target, sems.at[k]) for k, (source, target) in enumerate(zip(sources, targets))]
    for move in moves:
        move.start()
    return moves


def passed(grad_ref, second_ref):
    return jnp.where(second_ref[...].astype(f32) > 0, grad_ref[...].astype(f32), 0.0).astype(bf16)


def halo_kernel(grad_hbm, second_hbm, first_hbm, near_ref, far_ref, grad_ref, second_ref, first_ref, sems):
    for move in started((grad_hbm, second_hbm, first_hbm), (grad_ref, second_ref, first_ref), sems):
        move.wait()
    rows = first_ref.shape[0]
    odd = lax.axis_index("space") & 1
    grad_b = passed(grad_ref, second_ref)
    near_ref[:rows] = grad_b
    far_ref[:rows] = grad_b
    near_ref[rows] = first_ref[(rows - 1) * (1 - odd)]
    far_ref[rows] = first_ref[(rows - 1) * odd]


def back_weight(wb_ref, a, b):
    ch = wb_ref.shape[0]
    tap = (3 * (2 - a) + (2 - b)) * ch
    return wb_ref[:, tap : tap + ch]


def own_kernel(cols, grad_hbm, second_hbm, wb_hbm, start_ref, gt_ref, wb_ref, grad_ref, second_ref, g_ref, sems):
    moves = started((grad_hbm, second_hbm, wb_hbm), (grad_ref, second_ref, wb_ref), sems)
    moves[0].wait()
    moves[1].wait()
    own = passed(grad_ref, second_ref)
    own = jnp.concatenate([own[0], own[1]], axis=0).astype(f32)
    for b in range(3):
        g_ref[b] = shifted_columns(own, b - 1, cols).astype(bf16)
        gt_ref[b] = g_ref[b].T
    moves[2].wait()
    low, middle, high = [
        sum(mm(g_ref[b], back_weight(wb_ref, a, b), NN) for b in range(3)) for a in (2, 1, 0)
    ]
    start_ref[0:cols] = low[:cols]
    start_ref[cols : 2 * cols] = low[cols:] + middle[:cols]
    start_ref[2 * cols : 3 * cols] = middle[cols:] + high[:cols]
    start_ref[3 * cols :] = high[cols:]


def local_kernel(dims, near_ref, far_ref, start_ref, gt_own_ref, wb_ref, first_hbm, lid_hbm, cam_hbm, wa_hbm, list_hbm,
                 lidar_hbm, blocks_hbm, keep_ref, send_hbm,
                 gb_ref, ga_ref, a_ref, gt_ref, at_ref, first_ref, lid_ref, cam_ref, wa_ref, list_ref,
                 pick_ref, lidar_ref, send_ref, block_sems, out_sems, in_sems):
    cols, ch, cam, parts = dims
    lid = lid_ref.shape[2]
    fan = cam + lid
    half = ch // 2
    moves = started(
        (first_hbm, wa_hbm, list_hbm, lid_hbm, cam_hbm), (first_ref, wa_ref, list_ref, lid_ref, cam_ref), in_sems
    )
    second_core = (lax.axis_index("space") & 1) > 0
    column_place = lax.axis_index("scene") >> 1
    near = [near_ref[k].astype(f32) for k in range(3)]
    far = [far_ref[k].astype(f32) for k in range(3)]
    before = [jnp.where(second_core, n, f) for n, f in zip(near, far)]
    after = [jnp.where(second_core, f, n) for n, f in zip(near, far)]
    two_before = jnp.concatenate(before[:2], axis=0)
    two_after = jnp.concatenate(after[:2], axis=0)
    for b in range(3):
        gb_ref[b] = shifted_columns(two_before, b - 1, cols).astype(bf16)
        ga_ref[b] = shifted_columns(two_after, b - 1, cols).astype(bf16)
        gt_ref[b, :, :cols] = gb_ref[b, cols:, :].T
        gt_ref[b, :, cols : 3 * cols] = gt_own_ref[b]
        gt_ref[b, :, 3 * cols :] = ga_ref[b, :cols, :].T
    up = sum(mm(gb_ref[b], back_weight(wb_ref, 0, b), NN) for b in range(3))
    up_edge = sum(mm(gb_ref[b, cols:, :], back_weight(wb_ref, 1, b), NN) for b in range(3))
    down = sum(mm(ga_ref[b], back_weight(wb_ref, 2, b), NN) for b in range(3))
    down_edge = sum(mm(ga_ref[b, :cols, :], back_weight(wb_ref, 1, b), NN) for b in range(3))
    back = start_ref[...] + jnp.concatenate(
        [up[:cols] + up_edge, up[cols:], down[:cols], down[cols:] + down_edge], axis=0
    )
    moves[0].wait()
    first = jnp.concatenate([before[2], first_ref[0].astype(f32), first_ref[1].astype(f32), after[2]], axis=0)
    grad_a = jnp.where(first > 0, back, 0.0).astype(bf16).astype(f32)
    for b in range(3):
        moved = shifted_columns(grad_a, b - 1, cols)
        a_ref[b] = moved.astype(bf16)
        at_ref[b] = moved.astype(bf16).T
    moves[1].wait()
    lidar = jnp.zeros((2 * cols, lid), f32)
    camera = jnp.zeros((cam, 2 * cols), f32)
    for a in range(3):
        for b in range(3):
            tap = (3 * (2 - a) + (2 - b)) * fan
            rows = a_ref[b, a * cols : (a + 2) * cols, :]
            lidar += mm(rows, wa_ref[tap + cam : tap + fan, :], NT)
            camera += mm(wa_ref[tap : tap + cam, :], rows, NT)
    for r in range(2):
        lidar_ref[r] = lidar[r * cols : (r + 1) * cols].astype(bf16)
    leaving = [pltpu.make_async_copy(lidar_ref, lidar_hbm, out_sems.at[parts])]
    leaving[0].start()
    for r in range(2):
        pick_ref[r] = camera[:, r * cols : (r + 1) * cols].astype(bf16)
    moves[2].wait()
    picks = [
        pltpu.make_async_copy(pick_ref.at[jnp.where(list_ref[k] > 0, 1, 0)], blocks_hbm.at[k], block_sems.at[k])
        for k in range(blocks_hbm.shape[0])
    ]
    for pick in picks:
        pick.start()

    moves[3].wait()
    moves[4].wait()
    per_part = keep_ref.shape[2] // TILE

    def put(value, tile):
        halves = value.reshape(ch // 16, 2, 8, value.shape[1])
        even = halves[:, 0].reshape(half, value.shape[1])
        odd = halves[:, 1].reshape(half, value.shape[1])
        mine = jnp.where(second_core, odd, even).astype(bf16)
        other = jnp.where(second_core, even, odd).astype(bf16)
        for t in range(value.shape[1] // TILE):
            part, at = divmod(tile + t, per_part)
            part = part ^ column_place
            here = slice(at * TILE, (at + 1) * TILE)
            keep_ref[part, :, here] = mine[:, t * TILE : (t + 1) * TILE]
            send_ref[part, :, here] = other[:, t * TILE : (t + 1) * TILE]

    hidden = jnp.maximum(jnp.concatenate([first_ref[0], first_ref[1]], axis=0), 0)
    lidar_in = jnp.concatenate([lid_ref[0], lid_ref[1]], axis=0)
    camera_in = jnp.concatenate([cam_ref[0], cam_ref[1]], axis=1)
    b_tiles, a_tiles = ch // TILE, lid // TILE
    windows = [(2 - b, slice((2 - a) * cols, (4 - a) * cols)) for a in range(3) for b in range(3)]

    def leave(first_part, end):
        for part in range(first_part, end):
            place = part ^ column_place
            leaving.append(pltpu.make_async_copy(send_ref.at[place], send_hbm.at[place], out_sems.at[part]))
            leaving[-1].start()

    for tap, (b, window) in enumerate(windows):
        put(mm(gt_ref[b, :, window], hidden, NN), tap * b_tiles)
    gone = 9 * b_tiles // per_part
    leave(0, gone)
    for tap, (b, window) in enumerate(windows):
        put(mm(at_ref[b, :, window], lidar_in, NN), 9 * b_tiles + tap * a_tiles)
    at = 9 * (b_tiles + a_tiles)
    leave(gone, at // per_part)
    packed = [mm(at_ref[b, :, window], camera_in, NT) for b, window in windows]
    spare = (parts * per_part - at) * TILE - 9 * cam
    packed.append(jnp.zeros((ch, spare), f32))
    put(jnp.concatenate(packed, axis=1), at)
    leave(at // per_part, parts)
    for move in leaving:
        move.wait()
    for pick in picks:
        pick.wait()


def depth_kernel(blocks_ref, weight_ref, context_ref, slot_ref, gc_ref, gd_ref, wt_ref, st_ref, s_ref, m_ref, d_ref):
    sources, cam, cells_of = blocks_ref.shape
    depth, pix = slot_ref.shape
    wide = st_ref.shape[1]
    wt_ref[...] = jnp.concatenate([weight_ref[...].astype(f32), jnp.zeros((wide - depth, pix), f32)], axis=0).T
    st_ref[...] = jnp.concatenate([slot_ref[...], jnp.full((wide - depth, pix), -1, jnp.int32)], axis=0).T
    context_t = context_ref[...].astype(f32).T.astype(bf16)
    pitch = s_ref.shape[0] // sources
    for s in range(sources):
        s_ref[s * pitch : s * pitch + pix, :] = mm(context_t, blocks_ref[s], NN)
    cells = lax.broadcasted_iota(jnp.int32, (cells_of, wide), 0)
    places = lax.broadcasted_iota(jnp.int32, (sources, wide), 0)
    shift = cells_of.bit_length() - 1

    def pixels(g, carry):
        base = pl.multiple_of(g * 8, 8)
        slots = st_ref[pl.ds(base, 8), :]
        weights = wt_ref[pl.ds(base, 8), :]
        found_rows = []
        for k in range(8):
            slot = slots[k : k + 1]
            at_cell = jnp.where(cells == (slot & (cells_of - 1)), 1.0, 0.0).astype(bf16)
            here = places == (slot >> shift)
            every = pl.ds(base + k, sources, stride=pitch)
            m_ref[every, :] = mm(jnp.where(here, weights[k : k + 1], 0.0).astype(bf16), at_cell, NT)
            found = mm(s_ref[every, :].astype(bf16), at_cell, NN)
            found_rows.append(jnp.sum(jnp.where(here, found, 0.0), axis=0, keepdims=True))
        d_ref[pl.ds(base, 8), :] = jnp.concatenate(found_rows, axis=0)
        return carry

    lax.fori_loop(0, pix // 8, pixels, 0)
    gd_ref[...] = d_ref[...].T[:depth]
    total = jnp.zeros((cam, pix), f32)
    for s in range(sources):
        total += mm(blocks_ref[s], m_ref[s * pitch : s * pitch + pix, :].astype(bf16), NT)
    gc_ref[...] = total


def added(keep_ref, other_ref, part, rows):
    return keep_ref[part, rows].astype(f32) + other_ref[part, rows].astype(f32)


def first_sum(keep_ref, other_ref, a_ref, b_ref):
    rows = a_ref.shape[1]
    for k, (upper, lower) in enumerate([(1, 3), (2, 2)]):
        a_ref[k] = added(keep_ref, other_ref, upper, slice(0, rows)).astype(bf16)
        b_ref[k] = added(keep_ref, other_ref, lower, slice(rows, 2 * rows)).astype(bf16)


def kept_sum(keep_ref, other_ref, own_ref, next_ref):
    rows = own_ref.shape[0] // 2
    for here, part in [(slice(0, rows), 3), (slice(rows, 2 * rows), 1)]:
        own_ref[here] = added(keep_ref, other_ref, 0, here)
        next_ref[here] = added(keep_ref, other_ref, part, here)


def second_sum(own_ref, next_ref, a_ref, b_ref, out_ref, a_out_ref, b_out_ref):
    rows = a_ref.shape[1]
    upper, lower = slice(0, rows), slice(rows, 2 * rows)
    a_out_ref[...] = (next_ref[upper] + a_ref[1].astype(f32)).astype(bf16)
    b_out_ref[...] = (next_ref[lower] + b_ref[1].astype(f32)).astype(bf16)
    out_ref[upper] = own_ref[upper] + a_ref[0].astype(f32)
    out_ref[lower] = own_ref[lower] + b_ref[0].astype(f32)


def third_sum(own_ref, a_ref, b_ref, out_ref):
    rows = a_ref.shape[0]
    out_ref[:rows] = (own_ref[:rows] + a_ref[...].astype(f32)).astype(bf16)
    out_ref[rows:] = (own_ref[rows:] + b_ref[...].astype(f32)).astype(bf16)


def place_sum(parts_ref, out_ref):
    out_ref[...] = jnp.sum(parts_ref[...].astype(f32), axis=0).astype(bf16)


def pair_sum(one_ref, two_ref, out_ref):
    out_ref[...] = one_ref[...].astype(f32) + two_ref[...].astype(f32)


def last_sum(dims, scale, *refs):
    ch, lid, cam = dims
    *parts, wa_ref, wb_ref, all_ref = refs
    column_place = lax.axis_index("scene") >> 1
    for k, part in enumerate(parts):
        all_ref[k ^ column_place] = part[...]
    whole = jnp.concatenate([all_ref[x] for x in range(len(parts))], axis=1) * scale
    wb_ref[...] = whole[:, : 9 * ch]
    pieces = []
    for tap in range(9):
        at = 9 * (ch + lid) + tap * cam
        pieces += [whole[:, at : at + cam], whole[:, 9 * ch + tap * lid : 9 * ch + (tap + 1) * lid]]
    wa_ref[...] = jnp.concatenate(pieces, axis=1)


def call(kernel, outs, scratch, args, specs, flops, traffic, outs_at=None, limit=24):
    return pl.pallas_call(
        kernel,
        out_shape=outs,
        in_specs=specs,
        out_specs=outs_at or [VM] * len(outs),
        scratch_shapes=scratch,
        cost_estimate=pl.CostEstimate(flops=flops, bytes_accessed=traffic, transcendentals=0),
        compiler_params=pltpu.CompilerParams(vmem_limit_bytes=limit << 20),
    )(*[pltpu.with_memory_space_constraint(x, pltpu.HBM) if spec is HB else x for x, spec in zip(args, specs)])


def small(kernel, outs, args):
    outs = [jax.ShapeDtypeStruct(shape, dtype) for shape, dtype in outs]
    traffic = sum(x.size * x.dtype.itemsize for x in (*args, *outs))
    return call(kernel, outs, [], args, [VM] * len(args), traffic, traffic)


VM = pl.BlockSpec(memory_space=pltpu.VMEM)
SM = pl.BlockSpec(memory_space=pltpu.SMEM)
HB = pl.BlockSpec(memory_space=pltpu.HBM)


def exchanged(x, axis, groups):
    return lax.all_to_all(x, axis, 0, 0, axis_index_groups=groups, tiled=True)


def swapped(x, axis, partner):
    return lax.ppermute(x, axis, [(i, partner(i)) for i in range(lax.axis_size(axis))])


def summed_along_x(keep, send):
    _, rows, per_part = keep.shape
    deep = rows // 2
    other = swapped(send, "space", lambda i: i ^ 1)
    a, b = small(first_sum, [((2, deep, per_part), bf16)] * 2, (keep, other))
    a, b = swapped(a, "scene", lambda i: i ^ 2), swapped(b, "scene", lambda i: i ^ 6)
    kept = small(kept_sum, [((2 * deep, per_part), f32)] * 2, (keep, other))
    own, a, b = small(
        second_sum,
        [((2 * deep, per_part), f32), ((deep, per_part), bf16), ((deep, per_part), bf16)],
        (*kept, a, b),
    )
    a, b = swapped(a, "scene", lambda i: i ^ 6), swapped(b, "scene", lambda i: i ^ 2)
    (part,) = small(third_sum, [((2 * deep, per_part), bf16)], (own, a, b))
    return part


def over_scenes(part, dims, scale):
    ch, lid, cam = dims
    (own,) = small(pair_sum, [(part.shape, f32)], (part, swapped(part, "scene", lambda i: i ^ 1)))
    parts = [own]
    for k in range(1, 4):
        parts.append(swapped(own, "scene", lambda i: i ^ 2 * k))
    return call(
        functools.partial(last_sum, dims, scale),
        [jax.ShapeDtypeStruct((8, 9 * width), f32) for width in (cam + lid, ch)],
        [pltpu.VMEM((len(parts), *own.shape), f32)],
        parts,
        [VM] * len(parts),
        400_000,
        400_000,
    )


def shards(
    grad_out, pre_second, pre_first, camera_bev, lidar_bev, weight_a, weight_b,
    depth_weights, context, block_list, point_slot,
):
    _, rows, cols, ch = grad_out.shape
    cam, lid = camera_bev.shape[-1], lidar_bev.shape[-1]
    space, scenes = lax.axis_size("space"), lax.axis_size("scene")
    pix = point_slot.shape[1]
    place = space // 2
    reach = scenes // 2
    scale = 1.0 / math.sqrt(rows * cols * space * scenes)
    first = pre_first[0]
    shape = jax.ShapeDtypeStruct
    near, far = call(
        halo_kernel,
        [shape((k, cols, ch), bf16) for k in (rows + 1, rows + 1)],
        [pltpu.VMEM(first.shape, bf16)] * 3 + [pltpu.SemaphoreType.DMA((3,))],
        (grad_out[0], pre_second[0], first),
        [HB] * 3,
        1_000_000,
        1_000_000,
    )
    sides = [(i, i + 1) for i in range(1, space - 1, 2)]
    far = lax.ppermute(far, "space", sides + [(j, i) for i, j in sides])
    near = swapped(near, "space", lambda i: i ^ 1)
    camera = jnp.swapaxes(camera_bev[0], 1, 2)
    tiles = 9 * (ch + lid) // TILE + -(-9 * cam // TILE)
    per_part = -(-tiles // reach) * TILE
    start, gt_own, wb = call(
        functools.partial(own_kernel, cols),
        [
            pltpu.VMEM((4 * cols, ch), f32),
            pltpu.VMEM((3, ch, rows * cols), bf16),
            pltpu.VMEM(weight_b.shape, bf16),
        ],
        [
            pltpu.VMEM(first.shape, bf16),
            pltpu.VMEM(first.shape, bf16),
            pltpu.VMEM((3, rows * cols, ch), bf16),
            pltpu.SemaphoreType.DMA((3,)),
        ],
        (grad_out[0], pre_second[0], weight_b),
        [HB] * 3,
        300_000_000,
        2_500_000,
    )
    lidar, blocks, keep, send = call(
        functools.partial(local_kernel, (cols, ch, cam, reach)),
        [
            pltpu.HBM((rows, cols, lid), bf16),
            pltpu.HBM((space, cam, cols), bf16),
            shape((reach, ch // 2, per_part), bf16),
            pltpu.HBM((reach, ch // 2, per_part), bf16),
        ],
        [
            pltpu.VMEM((3, 2 * cols, ch), bf16),
            pltpu.VMEM((3, 2 * cols, ch), bf16),
            pltpu.VMEM((3, 4 * cols, ch), bf16),
            pltpu.VMEM((3, ch, 4 * cols), bf16),
            pltpu.VMEM((3, ch, 4 * cols), bf16),
            pltpu.VMEM(first.shape, bf16),
            pltpu.VMEM((rows, cols, lid), bf16),
            pltpu.VMEM(camera.shape, bf16),
            pltpu.VMEM(weight_a.shape[::-1], bf16),
            pltpu.SMEM((space,), jnp.int32),
            pltpu.VMEM((2, cam, cols), bf16),
            pltpu.VMEM((rows, cols, lid), bf16),
            pltpu.VMEM((reach, ch // 2, per_part), bf16),
            pltpu.SemaphoreType.DMA((space,)),
            pltpu.SemaphoreType.DMA((reach + 1,)),
            pltpu.SemaphoreType.DMA((5,)),
        ],
        (near, far, start, gt_own, wb, first, lidar_bev[0], camera, weight_a.T, block_list[:, 0, 0]),
        [VM] * 5 + [HB] * 5,
        1_500_000_000,
        12_000_000,
        outs_at=[HB, HB, VM, HB],
    )
    incoming = exchanged(blocks, "space", None)
    part = summed_along_x(keep, send)
    incoming, part = lax.optimization_barrier((incoming, part))
    along_yz = exchanged(
        part.reshape(place, 8, per_part), "space", [[2 * i + c for i in range(place)] for c in range(2)]
    )
    grad_context, grad_depth = call(
        depth_kernel,
        [shape((cam, pix), f32), shape(point_slot.shape, f32)],
        [
            pltpu.VMEM((pix, 128), f32),
            pltpu.VMEM((pix, 128), jnp.int32),
            pltpu.VMEM((space * (pix + 8), cols), f32),
            pltpu.VMEM((space * (pix + 8), cols), f32),
            pltpu.VMEM((pix, 128), f32),
        ],
        (incoming, depth_weights[0], context[0], point_slot),
        [VM] * 4,
        2_000_000_000,
        2_000_000,
    )
    along_yz, grad_context, grad_depth = lax.optimization_barrier((along_yz, grad_context, grad_depth))
    (part,) = small(place_sum, [((8, per_part), bf16)], (along_yz,))
    grad_wa, grad_wb = over_scenes(part, (ch, lid, cam), scale)
    return grad_wa, grad_wb, lidar[None], grad_context[None], grad_depth[None]


def solution(mesh):
    field = P("scene", "space", None, None)
    pixels = P("scene", None, "space")
    return jax.shard_map(
        shards,
        mesh=mesh,
        in_specs=(field,) * 5 + (P(), P(), pixels, pixels, P(None, "space", None), P(None, "space")),
        out_specs=(P("space", None), P("space", None), field, pixels, pixels),
        check_vma=False,
    )
```

```python
import functools
import math

import jax
import jax.numpy as jnp
from jax import lax
from jax.experimental import pallas as pl
from jax.experimental.pallas import tpu as pltpu
from jax.sharding import PartitionSpec as P


f32 = jnp.float32
bf16 = jnp.bfloat16
NN = (((1,), (0,)), ((), ()))
NT = (((1,), (1,)), ((), ()))


def mm(a, b, dims):
    return lax.dot_general(a, b, dims, preferred_element_type=f32)


def shifted_columns(rows, step, cols):
    if step == 0:
        return rows
    zero = jnp.zeros((1, rows.shape[1]), rows.dtype)
    out = []
    for r in range(rows.shape[0] // cols):
        row = rows[r * cols : (r + 1) * cols]
        out += [row[1:], zero] if step > 0 else [zero, row[:-1]]
    return jnp.concatenate(out, axis=0)


TILE = 128


def started(sources, targets, sems):
    moves = [pltpu.make_async_copy(source, target, sems.at[k]) for k, (source, target) in enumerate(zip(sources, targets))]
    for move in moves:
        move.start()
    return moves


def passed(grad_ref, second_ref):
    return jnp.where(second_ref[...].astype(f32) > 0, grad_ref[...].astype(f32), 0.0).astype(bf16)


def halo_kernel(grad_hbm, second_hbm, first_hbm, near_ref, far_ref, grad_ref, second_ref, first_ref, sems):
    for move in started((grad_hbm, second_hbm, first_hbm), (grad_ref, second_ref, first_ref), sems):
        move.wait()
    rows = first_ref.shape[0]
    odd = lax.axis_index("space") & 1
    grad_b = passed(grad_ref, second_ref)
    near_ref[:rows] = grad_b
    far_ref[:rows] = grad_b
    near_ref[rows] = first_ref[(rows - 1) * (1 - odd)]
    far_ref[rows] = first_ref[(rows - 1) * odd]


def back_weight(wb_ref, a, b):
    ch = wb_ref.shape[0]
    tap = (3 * (2 - a) + (2 - b)) * ch
    return wb_ref[:, tap : tap + ch]


def own_kernel(cols, grad_hbm, second_hbm, wb_hbm, start_ref, gt_ref, wb_ref, grad_ref, second_ref, g_ref, sems):
    moves = started((grad_hbm, second_hbm, wb_hbm), (grad_ref, second_ref, wb_ref), sems)
    moves[0].wait()
    moves[1].wait()
    own = passed(grad_ref, second_ref)
    own = jnp.concatenate([own[0], own[1]], axis=0).astype(f32)
    for b in range(3):
        g_ref[b] = shifted_columns(own, b - 1, cols).astype(bf16)
        gt_ref[b] = g_ref[b].T
    moves[2].wait()
    low, middle, high = [
        sum(mm(g_ref[b], back_weight(wb_ref, a, b), NN) for b in range(3)) for a in (2, 1, 0)
    ]
    start_ref[0:cols] = low[:cols]
    start_ref[cols : 2 * cols] = low[cols:] + middle[:cols]
    start_ref[2 * cols : 3 * cols] = middle[cols:] + high[:cols]
    start_ref[3 * cols :] = high[cols:]


def local_kernel(dims, near_ref, far_ref, start_ref, gt_own_ref, wb_ref, first_hbm, lid_hbm, cam_hbm, wa_hbm, list_hbm,
                 lidar_hbm, blocks_hbm, keep_ref, send_hbm,
                 gb_ref, ga_ref, a_ref, gt_ref, at_ref, first_ref, lid_ref, cam_ref, wa_ref, list_ref,
                 pick_ref, lidar_ref, send_ref, block_sems, out_sems, in_sems):
    cols, ch, cam, parts = dims
    lid = lid_ref.shape[2]
    fan = cam + lid
    half = ch // 2
    moves = started(
        (first_hbm, wa_hbm, list_hbm, lid_hbm, cam_hbm), (first_ref, wa_ref, list_ref, lid_ref, cam_ref), in_sems
    )
    second_core = (lax.axis_index("space") & 1) > 0
    column_place = lax.axis_index("scene") >> 1
    near = [near_ref[k].astype(f32) for k in range(3)]
    far = [far_ref[k].astype(f32) for k in range(3)]
    before = [jnp.where(second_core, n, f) for n, f in zip(near, far)]
    after = [jnp.where(second_core, f, n) for n, f in zip(near, far)]
    two_before = jnp.concatenate(before[:2], axis=0)
    two_after = jnp.concatenate(after[:2], axis=0)
    for b in range(3):
        gb_ref[b] = shifted_columns(two_before, b - 1, cols).astype(bf16)
        ga_ref[b] = shifted_columns(two_after, b - 1, cols).astype(bf16)
        gt_ref[b, :, :cols] = gb_ref[b, cols:, :].T
        gt_ref[b, :, cols : 3 * cols] = gt_own_ref[b]
        gt_ref[b, :, 3 * cols :] = ga_ref[b, :cols, :].T
    up = sum(mm(gb_ref[b], back_weight(wb_ref, 0, b), NN) for b in range(3))
    up_edge = sum(mm(gb_ref[b, cols:, :], back_weight(wb_ref, 1, b), NN) for b in range(3))
    down = sum(mm(ga_ref[b], back_weight(wb_ref, 2, b), NN) for b in range(3))
    down_edge = sum(mm(ga_ref[b, :cols, :], back_weight(wb_ref, 1, b), NN) for b in range(3))
    back = start_ref[...] + jnp.concatenate(
        [up[:cols] + up_edge, up[cols:], down[:cols], down[cols:] + down_edge], axis=0
    )
    moves[0].wait()
    first = jnp.concatenate([before[2], first_ref[0].astype(f32), first_ref[1].astype(f32), after[2]], axis=0)
    grad_a = jnp.where(first > 0, back, 0.0).astype(bf16).astype(f32)
    for b in range(3):
        moved = shifted_columns(grad_a, b - 1, cols)
        a_ref[b] = moved.astype(bf16)
        at_ref[b] = moved.astype(bf16).T
    moves[1].wait()
    lidar = jnp.zeros((2 * cols, lid), f32)
    camera = jnp.zeros((cam, 2 * cols), f32)
    for a in range(3):
        for b in range(3):
            tap = (3 * (2 - a) + (2 - b)) * fan
            rows = a_ref[b, a * cols : (a + 2) * cols, :]
            lidar += mm(rows, wa_ref[tap + cam : tap + fan, :], NT)
            camera += mm(wa_ref[tap : tap + cam, :], rows, NT)
    for r in range(2):
        lidar_ref[r] = lidar[r * cols : (r + 1) * cols].astype(bf16)
    leaving = [pltpu.make_async_copy(lidar_ref, lidar_hbm, out_sems.at[parts])]
    leaving[0].start()
    for r in range(2):
        pick_ref[r] = camera[:, r * cols : (r + 1) * cols].astype(bf16)
    moves[2].wait()
    picks = [
        pltpu.make_async_copy(pick_ref.at[jnp.where(list_ref[k] > 0, 1, 0)], blocks_hbm.at[k], block_sems.at[k])
        for k in range(blocks_hbm.shape[0])
    ]
    for pick in picks:
        pick.start()

    moves[3].wait()
    moves[4].wait()
    per_part = keep_ref.shape[2] // TILE

    def put(value, tile):
        halves = value.reshape(ch // 16, 2, 8, value.shape[1])
        even = halves[:, 0].reshape(half, value.shape[1])
        odd = halves[:, 1].reshape(half, value.shape[1])
        mine = jnp.where(second_core, odd, even).astype(bf16)
        other = jnp.where(second_core, even, odd).astype(bf16)
        for t in range(value.shape[1] // TILE):
            part, at = divmod(tile + t, per_part)
            part = part ^ column_place
            here = slice(at * TILE, (at + 1) * TILE)
            keep_ref[part, :, here] = mine[:, t * TILE : (t + 1) * TILE]
            send_ref[part, :, here] = other[:, t * TILE : (t + 1) * TILE]

    hidden = jnp.maximum(jnp.concatenate([first_ref[0], first_ref[1]], axis=0), 0)
    lidar_in = jnp.concatenate([lid_ref[0], lid_ref[1]], axis=0)
    camera_in = jnp.concatenate([cam_ref[0], cam_ref[1]], axis=1)
    b_tiles, a_tiles = ch // TILE, lid // TILE
    windows = [(2 - b, slice((2 - a) * cols, (4 - a) * cols)) for a in range(3) for b in range(3)]

    def leave(first_part, end):
        for part in range(first_part, end):
            place = part ^ column_place
            leaving.append(pltpu.make_async_copy(send_ref.at[place], send_hbm.at[place], out_sems.at[part]))
            leaving[-1].start()

    for tap, (b, window) in enumerate(windows):
        put(mm(gt_ref[b, :, window], hidden, NN), tap * b_tiles)
    gone = 9 * b_tiles // per_part
    leave(0, gone)
    for tap, (b, window) in enumerate(windows):
        put(mm(at_ref[b, :, window], lidar_in, NN), 9 * b_tiles + tap * a_tiles)
    at = 9 * (b_tiles + a_tiles)
    leave(gone, at // per_part)
    packed = [mm(at_ref[b, :, window], camera_in, NT) for b, window in windows]
    spare = (parts * per_part - at) * TILE - 9 * cam
    packed.append(jnp.zeros((ch, spare), f32))
    put(jnp.concatenate(packed, axis=1), at)
    leave(at // per_part, parts)
    for move in leaving:
        move.wait()
    for pick in picks:
        pick.wait()


def turned_slots(slot_ref, wide):
    depth, pix = slot_ref.shape
    return jnp.concatenate([slot_ref[...], jnp.full((wide - depth, pix), -1, jnp.int32)], axis=0).T


def one_hots(slot, cells, places):
    count = cells.shape[0]
    at_cell = jnp.where(cells == (slot & (count - 1)), 1.0, 0.0).astype(bf16)
    return at_cell, places == (slot >> (count.bit_length() - 1))


def mass_kernel(weight_ref, slot_ref, out_ref, wt_ref, st_ref, m_ref):
    sources, pix, cells_of = out_ref.shape
    depth, wide = slot_ref.shape[0], st_ref.shape[1]
    pitch = m_ref.shape[0] // sources
    wt_ref[...] = jnp.concatenate([weight_ref[...].astype(f32), jnp.zeros((wide - depth, pix), f32)], axis=0).T
    st_ref[...] = turned_slots(slot_ref, wide)
    cells = lax.broadcasted_iota(jnp.int32, (cells_of, wide), 0)
    places = lax.broadcasted_iota(jnp.int32, (sources, wide), 0)

    def pixels(g, carry):
        base = pl.multiple_of(g * 8, 8)
        slots = st_ref[pl.ds(base, 8), :]
        weights = wt_ref[pl.ds(base, 8), :]
        for k in range(8):
            at_cell, here = one_hots(slots[k : k + 1], cells, places)
            m_ref[pl.ds(base + k, sources, stride=pitch), :] = mm(
                jnp.where(here, weights[k : k + 1], 0.0).astype(bf16), at_cell, NT
            )
        return carry

    lax.fori_loop(0, pix // 8, pixels, 0)
    for s in range(sources):
        out_ref[s] = m_ref[s * pitch : s * pitch + pix, :].astype(bf16)


def depth_kernel(blocks_ref, mass_ref, context_ref, slot_ref, gc_ref, gd_ref, st_ref, s_ref, d_ref):
    sources, cam, cells_of = blocks_ref.shape
    depth, pix = slot_ref.shape
    wide = st_ref.shape[1]
    pitch = s_ref.shape[0] // sources
    st_ref[...] = turned_slots(slot_ref, wide)
    context_t = context_ref[...].astype(f32).T.astype(bf16)
    total = jnp.zeros((cam, pix), f32)
    for s in range(sources):
        s_ref[s * pitch : s * pitch + pix, :] = mm(context_t, blocks_ref[s], NN)
        total += mm(blocks_ref[s], mass_ref[s], NT)
    gc_ref[...] = total
    cells = lax.broadcasted_iota(jnp.int32, (cells_of, wide), 0)
    places = lax.broadcasted_iota(jnp.int32, (sources, wide), 0)

    def pixels(g, carry):
        base = pl.multiple_of(g * 8, 8)
        slots = st_ref[pl.ds(base, 8), :]
        found_rows = []
        for k in range(8):
            at_cell, here = one_hots(slots[k : k + 1], cells, places)
            found = mm(s_ref[pl.ds(base + k, sources, stride=pitch), :].astype(bf16), at_cell, NN)
            found_rows.append(jnp.sum(jnp.where(here, found, 0.0), axis=0, keepdims=True))
        d_ref[pl.ds(base, 8), :] = jnp.concatenate(found_rows, axis=0)
        return carry

    lax.fori_loop(0, pix // 8, pixels, 0)
    gd_ref[...] = d_ref[...].T[:depth]


def added(keep_ref, other_ref, part, rows):
    return keep_ref[part, rows].astype(f32) + other_ref[part, rows].astype(f32)


def first_sum(keep_ref, other_ref, a_ref, b_ref):
    rows = a_ref.shape[1]
    for k, (upper, lower) in enumerate([(1, 3), (2, 2)]):
        a_ref[k] = added(keep_ref, other_ref, upper, slice(0, rows)).astype(bf16)
        b_ref[k] = added(keep_ref, other_ref, lower, slice(rows, 2 * rows)).astype(bf16)


def kept_sum(keep_ref, other_ref, own_ref, next_ref):
    rows = own_ref.shape[0] // 2
    for here, part in [(slice(0, rows), 3), (slice(rows, 2 * rows), 1)]:
        own_ref[here] = added(keep_ref, other_ref, 0, here)
        next_ref[here] = added(keep_ref, other_ref, part, here)


def second_sum(own_ref, next_ref, a_ref, b_ref, out_ref, a_out_ref, b_out_ref):
    rows = a_ref.shape[1]
    upper, lower = slice(0, rows), slice(rows, 2 * rows)
    a_out_ref[...] = (next_ref[upper] + a_ref[1].astype(f32)).astype(bf16)
    b_out_ref[...] = (next_ref[lower] + b_ref[1].astype(f32)).astype(bf16)
    out_ref[upper] = own_ref[upper] + a_ref[0].astype(f32)
    out_ref[lower] = own_ref[lower] + b_ref[0].astype(f32)


def third_sum(own_ref, a_ref, b_ref, out_ref):
    rows = a_ref.shape[0]
    out_ref[:rows] = (own_ref[:rows] + a_ref[...].astype(f32)).astype(bf16)
    out_ref[rows:] = (own_ref[rows:] + b_ref[...].astype(f32)).astype(bf16)


def y_sum(parts_ref, out_ref):
    total = jnp.sum(parts_ref[...].astype(f32), axis=0).astype(bf16)
    for z in range(out_ref.shape[1]):
        for h in range(out_ref.shape[0]):
            out_ref[h, z] = total[8 * z : 8 * z + 8]


def z_sum(parts_ref, out_ref):
    out_ref[...] = jnp.sum(parts_ref[...].astype(f32), axis=0)


def last_sum(dims, scale, *refs):
    ch, lid, cam = dims
    *parts, wa_ref, wb_ref, all_ref = refs
    column_place = lax.axis_index("scene") >> 1
    for k, part in enumerate(parts):
        all_ref[k ^ column_place] = part[...]
    whole = jnp.concatenate([all_ref[x] for x in range(len(parts))], axis=1) * scale
    wb_ref[...] = whole[:, : 9 * ch]
    pieces = []
    for tap in range(9):
        at = 9 * (ch + lid) + tap * cam
        pieces += [whole[:, at : at + cam], whole[:, 9 * ch + tap * lid : 9 * ch + (tap + 1) * lid]]
    wa_ref[...] = jnp.concatenate(pieces, axis=1)


def call(kernel, outs, scratch, args, specs, flops, traffic, outs_at=None, limit=24):
    return pl.pallas_call(
        kernel,
        out_shape=outs,
        in_specs=specs,
        out_specs=outs_at or [VM] * len(outs),
        scratch_shapes=scratch,
        cost_estimate=pl.CostEstimate(flops=flops, bytes_accessed=traffic, transcendentals=0),
        compiler_params=pltpu.CompilerParams(vmem_limit_bytes=limit << 20),
    )(*[pltpu.with_memory_space_constraint(x, pltpu.HBM) if spec is HB else x for x, spec in zip(args, specs)])


def small(kernel, outs, args):
    outs = [jax.ShapeDtypeStruct(shape, dtype) for shape, dtype in outs]
    traffic = sum(x.size * x.dtype.itemsize for x in (*args, *outs))
    return call(kernel, outs, [], args, [VM] * len(args), traffic, traffic)


VM = pl.BlockSpec(memory_space=pltpu.VMEM)
SM = pl.BlockSpec(memory_space=pltpu.SMEM)
HB = pl.BlockSpec(memory_space=pltpu.HBM)


def exchanged(x, axis, groups):
    return lax.all_to_all(x, axis, 0, 0, axis_index_groups=groups, tiled=True)


def swapped(x, axis, partner):
    return lax.ppermute(x, axis, [(i, partner(i)) for i in range(lax.axis_size(axis))])


def summed_along_x(keep, send):
    _, rows, per_part = keep.shape
    deep = rows // 2
    other = swapped(send, "space", lambda i: i ^ 1)
    a, b = small(first_sum, [((2, deep, per_part), bf16)] * 2, (keep, other))
    a, b = swapped(a, "scene", lambda i: i ^ 2), swapped(b, "scene", lambda i: i ^ 6)
    kept = small(kept_sum, [((2 * deep, per_part), f32)] * 2, (keep, other))
    own, a, b = small(
        second_sum,
        [((2 * deep, per_part), f32), ((deep, per_part), bf16), ((deep, per_part), bf16)],
        (*kept, a, b),
    )
    a, b = swapped(a, "scene", lambda i: i ^ 6), swapped(b, "scene", lambda i: i ^ 2)
    (part,) = small(third_sum, [((2 * deep, per_part), bf16)], (own, a, b))
    return part


def along_x(own, dims, scale):
    ch, lid, cam = dims
    parts = [own]
    for k in range(1, 4):
        parts.append(swapped(own, "scene", lambda i: i ^ 2 * k))
    return call(
        functools.partial(last_sum, dims, scale),
        [jax.ShapeDtypeStruct((8, 9 * width), f32) for width in (cam + lid, ch)],
        [pltpu.VMEM((len(parts), *own.shape), f32)],
        parts,
        [VM] * len(parts),
        400_000,
        400_000,
    )


def shards(
    grad_out, pre_second, pre_first, camera_bev, lidar_bev, weight_a, weight_b,
    depth_weights, context, block_list, point_slot,
):
    _, rows, cols, ch = grad_out.shape
    cam, lid = camera_bev.shape[-1], lidar_bev.shape[-1]
    space, scenes = lax.axis_size("space"), lax.axis_size("scene")
    pix = point_slot.shape[1]
    place = space // 2
    reach = scenes // 2
    scale = 1.0 / math.sqrt(rows * cols * space * scenes)
    first = pre_first[0]
    shape = jax.ShapeDtypeStruct
    near, far = call(
        halo_kernel,
        [shape((k, cols, ch), bf16) for k in (rows + 1, rows + 1)],
        [pltpu.VMEM(first.shape, bf16)] * 3 + [pltpu.SemaphoreType.DMA((3,))],
        (grad_out[0], pre_second[0], first),
        [HB] * 3,
        1_000_000,
        1_000_000,
    )
    sides = [(i, i + 1) for i in range(1, space - 1, 2)]
    far = lax.ppermute(far, "space", sides + [(j, i) for i, j in sides])
    near = swapped(near, "space", lambda i: i ^ 1)
    camera = jnp.swapaxes(camera_bev[0], 1, 2)
    tiles = 9 * (ch + lid) // TILE + -(-9 * cam // TILE)
    per_part = -(-tiles // reach) * TILE
    start, gt_own, wb = call(
        functools.partial(own_kernel, cols),
        [
            pltpu.VMEM((4 * cols, ch), f32),
            pltpu.VMEM((3, ch, rows * cols), bf16),
            pltpu.VMEM(weight_b.shape, bf16),
        ],
        [
            pltpu.VMEM(first.shape, bf16),
            pltpu.VMEM(first.shape, bf16),
            pltpu.VMEM((3, rows * cols, ch), bf16),
            pltpu.SemaphoreType.DMA((3,)),
        ],
        (grad_out[0], pre_second[0], weight_b),
        [HB] * 3,
        300_000_000,
        2_500_000,
    )
    lidar, blocks, keep, send = call(
        functools.partial(local_kernel, (cols, ch, cam, reach)),
        [
            pltpu.HBM((rows, cols, lid), bf16),
            pltpu.HBM((space, cam, cols), bf16),
            shape((reach, ch // 2, per_part), bf16),
            pltpu.HBM((reach, ch // 2, per_part), bf16),
        ],
        [
            pltpu.VMEM((3, 2 * cols, ch), bf16),
            pltpu.VMEM((3, 2 * cols, ch), bf16),
            pltpu.VMEM((3, 4 * cols, ch), bf16),
            pltpu.VMEM((3, ch, 4 * cols), bf16),
            pltpu.VMEM((3, ch, 4 * cols), bf16),
            pltpu.VMEM(first.shape, bf16),
            pltpu.VMEM((rows, cols, lid), bf16),
            pltpu.VMEM(camera.shape, bf16),
            pltpu.VMEM(weight_a.shape[::-1], bf16),
            pltpu.SMEM((space,), jnp.int32),
            pltpu.VMEM((2, cam, cols), bf16),
            pltpu.VMEM((rows, cols, lid), bf16),
            pltpu.VMEM((reach, ch // 2, per_part), bf16),
            pltpu.SemaphoreType.DMA((space,)),
            pltpu.SemaphoreType.DMA((reach + 1,)),
            pltpu.SemaphoreType.DMA((5,)),
        ],
        (near, far, start, gt_own, wb, first, lidar_bev[0], camera, weight_a.T, block_list[:, 0, 0]),
        [VM] * 5 + [HB] * 5,
        1_500_000_000,
        12_000_000,
        outs_at=[HB, HB, VM, HB],
    )
    incoming = exchanged(blocks, "space", None)
    table = pltpu.VMEM((space * (pix + 8), cols), f32)
    (mass,) = call(
        mass_kernel,
        [shape((space, pix, cols), bf16)],
        [pltpu.VMEM((pix, 128), f32), pltpu.VMEM((pix, 128), jnp.int32), table],
        (depth_weights[0], point_slot),
        [VM] * 2,
        500_000_000,
        2_000_000,
    )
    part = summed_along_x(keep, send)
    incoming, part = lax.optimization_barrier((incoming, part))
    deep = place // reach
    along_y = exchanged(
        part.reshape(reach, deep * 8, per_part),
        "space",
        [[y * 2 * deep + r for y in range(reach)] for r in range(2 * deep)],
    )
    grad_context, grad_depth = call(
        depth_kernel,
        [shape((cam, pix), f32), shape(point_slot.shape, f32)],
        [pltpu.VMEM((pix, 128), jnp.int32), table, pltpu.VMEM((pix, 128), f32)],
        (incoming, mass, context[0], point_slot),
        [VM] * 4,
        1_500_000_000,
        2_000_000,
    )
    along_y, grad_context, grad_depth = lax.optimization_barrier((along_y, grad_context, grad_depth))
    (spread,) = small(y_sum, [((2, deep, 8, per_part), bf16)], (along_y,))
    along_z = lax.all_to_all(
        spread.reshape(2 * deep, 8, per_part),
        ("space", "scene"),
        0,
        0,
        axis_index_groups=[
            [((y * deep + z) * 2 + c) * scenes + 2 * x + h for h in range(2) for z in range(deep)]
            for y in range(reach)
            for c in range(2)
            for x in range(reach)
        ],
        tiled=True,
    )
    (own,) = small(z_sum, [((8, per_part), f32)], (along_z,))
    grad_wa, grad_wb = along_x(own, (ch, lid, cam), scale)
    return grad_wa, grad_wb, lidar[None], grad_context[None], grad_depth[None]


def solution(mesh):
    field = P("scene", "space", None, None)
    pixels = P("scene", None, "space")
    return jax.shard_map(
        shards,
        mesh=mesh,
        in_specs=(field,) * 5 + (P(), P(), pixels, pixels, P(None, "space", None), P(None, "space")),
        out_specs=(P("space", None), P("space", None), field, pixels, pixels),
        check_vma=False,
    )
```

```python
import functools
import math

import jax
import jax.numpy as jnp
from jax import lax
from jax.experimental import pallas as pl
from jax.experimental.pallas import tpu as pltpu
from jax.sharding import PartitionSpec as P


f32 = jnp.float32
bf16 = jnp.bfloat16
NN = (((1,), (0,)), ((), ()))
NT = (((1,), (1,)), ((), ()))


def mm(a, b, dims):
    return lax.dot_general(a, b, dims, preferred_element_type=f32)


def shifted_columns(rows, step, cols):
    if step == 0:
        return rows
    zero = jnp.zeros((1, rows.shape[1]), rows.dtype)
    out = []
    for r in range(rows.shape[0] // cols):
        row = rows[r * cols : (r + 1) * cols]
        out += [row[1:], zero] if step > 0 else [zero, row[:-1]]
    return jnp.concatenate(out, axis=0)


TILE = 128


def started(sources, targets, sems):
    moves = [pltpu.make_async_copy(source, target, sems.at[k]) for k, (source, target) in enumerate(zip(sources, targets))]
    for move in moves:
        move.start()
    return moves


def passed(grad_ref, second_ref):
    return jnp.where(second_ref[...].astype(f32) > 0, grad_ref[...].astype(f32), 0.0).astype(bf16)


def halo_kernel(grad_hbm, second_hbm, first_hbm, near_ref, far_ref, grad_ref, second_ref, first_ref, sems):
    for move in started((grad_hbm, second_hbm, first_hbm), (grad_ref, second_ref, first_ref), sems):
        move.wait()
    rows = first_ref.shape[0]
    odd = lax.axis_index("space") & 1
    grad_b = passed(grad_ref, second_ref)
    near_ref[:rows] = grad_b
    far_ref[:rows] = grad_b
    near_ref[rows] = first_ref[(rows - 1) * (1 - odd)]
    far_ref[rows] = first_ref[(rows - 1) * odd]


def back_weight(wb_ref, a, b):
    ch = wb_ref.shape[0]
    tap = (3 * (2 - a) + (2 - b)) * ch
    return wb_ref[:, tap : tap + ch]


def own_kernel(cols, grad_hbm, second_hbm, wb_hbm, start_ref, gt_ref, wb_ref, grad_ref, second_ref, g_ref, sems):
    moves = started((grad_hbm, second_hbm, wb_hbm), (grad_ref, second_ref, wb_ref), sems)
    moves[0].wait()
    moves[1].wait()
    own = passed(grad_ref, second_ref)
    own = jnp.concatenate([own[0], own[1]], axis=0).astype(f32)
    for b in range(3):
        g_ref[b] = shifted_columns(own, b - 1, cols).astype(bf16)
        gt_ref[b] = g_ref[b].T
    moves[2].wait()
    low, middle, high = [
        sum(mm(g_ref[b], back_weight(wb_ref, a, b), NN) for b in range(3)) for a in (2, 1, 0)
    ]
    start_ref[0:cols] = low[:cols]
    start_ref[cols : 2 * cols] = low[cols:] + middle[:cols]
    start_ref[2 * cols : 3 * cols] = middle[cols:] + high[:cols]
    start_ref[3 * cols :] = high[cols:]


def local_kernel(dims, near_ref, far_ref, start_ref, gt_own_ref, wb_ref, first_hbm, lid_hbm, cam_hbm, wa_hbm, list_hbm,
                 lidar_hbm, blocks_hbm, keep_ref, send_hbm,
                 gb_ref, ga_ref, a_ref, gt_ref, at_ref, first_ref, lid_ref, cam_ref, wa_ref, list_ref,
                 pick_ref, lidar_ref, send_ref, block_sems, out_sems, in_sems):
    cols, ch, cam, parts = dims
    lid = lid_ref.shape[2]
    fan = cam + lid
    half = ch // 2
    moves = started(
        (first_hbm, wa_hbm, list_hbm, lid_hbm, cam_hbm), (first_ref, wa_ref, list_ref, lid_ref, cam_ref), in_sems
    )
    second_core = (lax.axis_index("space") & 1) > 0
    column_place = lax.axis_index("scene") >> 1
    near = [near_ref[k].astype(f32) for k in range(3)]
    far = [far_ref[k].astype(f32) for k in range(3)]
    before = [jnp.where(second_core, n, f) for n, f in zip(near, far)]
    after = [jnp.where(second_core, f, n) for n, f in zip(near, far)]
    two_before = jnp.concatenate(before[:2], axis=0)
    two_after = jnp.concatenate(after[:2], axis=0)
    for b in range(3):
        gb_ref[b] = shifted_columns(two_before, b - 1, cols).astype(bf16)
        ga_ref[b] = shifted_columns(two_after, b - 1, cols).astype(bf16)
        gt_ref[b, :, :cols] = gb_ref[b, cols:, :].T
        gt_ref[b, :, cols : 3 * cols] = gt_own_ref[b]
        gt_ref[b, :, 3 * cols :] = ga_ref[b, :cols, :].T
    up = sum(mm(gb_ref[b], back_weight(wb_ref, 0, b), NN) for b in range(3))
    up_edge = sum(mm(gb_ref[b, cols:, :], back_weight(wb_ref, 1, b), NN) for b in range(3))
    down = sum(mm(ga_ref[b], back_weight(wb_ref, 2, b), NN) for b in range(3))
    down_edge = sum(mm(ga_ref[b, :cols, :], back_weight(wb_ref, 1, b), NN) for b in range(3))
    back = start_ref[...] + jnp.concatenate(
        [up[:cols] + up_edge, up[cols:], down[:cols], down[cols:] + down_edge], axis=0
    )
    moves[0].wait()
    first = jnp.concatenate([before[2], first_ref[0].astype(f32), first_ref[1].astype(f32), after[2]], axis=0)
    grad_a = jnp.where(first > 0, back, 0.0).astype(bf16).astype(f32)
    for b in range(3):
        moved = shifted_columns(grad_a, b - 1, cols)
        a_ref[b] = moved.astype(bf16)
        at_ref[b] = moved.astype(bf16).T
    moves[1].wait()
    lidar = jnp.zeros((2 * cols, lid), f32)
    camera = jnp.zeros((cam, 2 * cols), f32)
    for a in range(3):
        for b in range(3):
            tap = (3 * (2 - a) + (2 - b)) * fan
            rows = a_ref[b, a * cols : (a + 2) * cols, :]
            lidar += mm(rows, wa_ref[tap + cam : tap + fan, :], NT)
            camera += mm(wa_ref[tap : tap + cam, :], rows, NT)
    for r in range(2):
        lidar_ref[r] = lidar[r * cols : (r + 1) * cols].astype(bf16)
    leaving = [pltpu.make_async_copy(lidar_ref, lidar_hbm, out_sems.at[parts])]
    leaving[0].start()
    for r in range(2):
        pick_ref[r] = camera[:, r * cols : (r + 1) * cols].astype(bf16)
    moves[2].wait()
    picks = [
        pltpu.make_async_copy(pick_ref.at[jnp.where(list_ref[k] > 0, 1, 0)], blocks_hbm.at[k], block_sems.at[k])
        for k in range(blocks_hbm.shape[0])
    ]
    for pick in picks:
        pick.start()

    moves[3].wait()
    moves[4].wait()
    per_part = keep_ref.shape[2] // TILE

    def put(value, tile):
        halves = value.reshape(ch // 16, 2, 8, value.shape[1])
        even = halves[:, 0].reshape(half, value.shape[1])
        odd = halves[:, 1].reshape(half, value.shape[1])
        mine = jnp.where(second_core, odd, even).astype(bf16)
        other = jnp.where(second_core, even, odd).astype(bf16)
        for t in range(value.shape[1] // TILE):
            part, at = divmod(tile + t, per_part)
            part = part ^ column_place
            here = slice(at * TILE, (at + 1) * TILE)
            keep_ref[part, :, here] = mine[:, t * TILE : (t + 1) * TILE]
            send_ref[part, :, here] = other[:, t * TILE : (t + 1) * TILE]

    hidden = jnp.maximum(jnp.concatenate([first_ref[0], first_ref[1]], axis=0), 0)
    lidar_in = jnp.concatenate([lid_ref[0], lid_ref[1]], axis=0)
    camera_in = jnp.concatenate([cam_ref[0], cam_ref[1]], axis=1)
    b_tiles, a_tiles = ch // TILE, lid // TILE
    windows = [(2 - b, slice((2 - a) * cols, (4 - a) * cols)) for a in range(3) for b in range(3)]

    def leave(first_part, end):
        for part in range(first_part, end):
            place = part ^ column_place
            leaving.append(pltpu.make_async_copy(send_ref.at[place], send_hbm.at[place], out_sems.at[part]))
            leaving[-1].start()

    for tap, (b, window) in enumerate(windows):
        put(mm(gt_ref[b, :, window], hidden, NN), tap * b_tiles)
    gone = 9 * b_tiles // per_part
    leave(0, gone)
    for tap, (b, window) in enumerate(windows):
        put(mm(at_ref[b, :, window], lidar_in, NN), 9 * b_tiles + tap * a_tiles)
    at = 9 * (b_tiles + a_tiles)
    leave(gone, at // per_part)
    packed = [mm(at_ref[b, :, window], camera_in, NT) for b, window in windows]
    spare = (parts * per_part - at) * TILE - 9 * cam
    packed.append(jnp.zeros((ch, spare), f32))
    put(jnp.concatenate(packed, axis=1), at)
    leave(at // per_part, parts)
    for move in leaving:
        move.wait()
    for pick in picks:
        pick.wait()


def turned_slots(slot_ref, wide):
    depth, pix = slot_ref.shape
    return jnp.concatenate([slot_ref[...], jnp.full((wide - depth, pix), -1, jnp.int32)], axis=0).T


def one_hots(slot, cells, places):
    count = cells.shape[0]
    at_cell = jnp.where(cells == (slot & (count - 1)), 1.0, 0.0).astype(bf16)
    return at_cell, places == (slot >> (count.bit_length() - 1))


def mass_kernel(weight_ref, slot_ref, out_ref, wt_ref, st_ref, m_ref):
    sources, pix, cells_of = out_ref.shape
    depth, wide = slot_ref.shape[0], st_ref.shape[1]
    pitch = m_ref.shape[0] // sources
    wt_ref[...] = jnp.concatenate([weight_ref[...].astype(f32), jnp.zeros((wide - depth, pix), f32)], axis=0).T
    st_ref[...] = turned_slots(slot_ref, wide)
    cells = lax.broadcasted_iota(jnp.int32, (cells_of, wide), 0)
    places = lax.broadcasted_iota(jnp.int32, (sources, wide), 0)

    def pixels(g, carry):
        base = pl.multiple_of(g * 8, 8)
        slots = st_ref[pl.ds(base, 8), :]
        weights = wt_ref[pl.ds(base, 8), :]
        for k in range(8):
            at_cell, here = one_hots(slots[k : k + 1], cells, places)
            m_ref[pl.ds(base + k, sources, stride=pitch), :] = mm(
                jnp.where(here, weights[k : k + 1], 0.0).astype(bf16), at_cell, NT
            )
        return carry

    lax.fori_loop(0, pix // 8, pixels, 0)
    for s in range(sources):
        out_ref[s] = m_ref[s * pitch : s * pitch + pix, :].astype(bf16)


def depth_kernel(blocks_ref, mass_ref, context_ref, slot_ref, gc_ref, gd_ref, st_ref, s_ref, d_ref):
    sources, cam, cells_of = blocks_ref.shape
    depth, pix = slot_ref.shape
    wide = st_ref.shape[1]
    pitch = s_ref.shape[0] // sources
    st_ref[...] = turned_slots(slot_ref, wide)
    context_t = context_ref[...].astype(f32).T.astype(bf16)
    total = jnp.zeros((cam, pix), f32)
    for s in range(sources):
        s_ref[s * pitch : s * pitch + pix, :] = mm(context_t, blocks_ref[s], NN)
        total += mm(blocks_ref[s], mass_ref[s], NT)
    gc_ref[...] = total
    cells = lax.broadcasted_iota(jnp.int32, (cells_of, wide), 0)
    places = lax.broadcasted_iota(jnp.int32, (sources, wide), 0)

    def pixels(g, carry):
        base = pl.multiple_of(g * 8, 8)
        slots = st_ref[pl.ds(base, 8), :]
        found_rows = []
        for k in range(8):
            at_cell, here = one_hots(slots[k : k + 1], cells, places)
            found = mm(s_ref[pl.ds(base + k, sources, stride=pitch), :].astype(bf16), at_cell, NN)
            found_rows.append(jnp.sum(jnp.where(here, found, 0.0), axis=0, keepdims=True))
        d_ref[pl.ds(base, 8), :] = jnp.concatenate(found_rows, axis=0)
        return carry

    lax.fori_loop(0, pix // 8, pixels, 0)
    gd_ref[...] = d_ref[...].T[:depth]


def added(keep_ref, other_ref, part, rows):
    return keep_ref[part, rows].astype(f32) + other_ref[part, rows].astype(f32)


def first_sum(keep_ref, other_ref, a_ref, b_ref):
    rows = a_ref.shape[1]
    for k, (upper, lower) in enumerate([(1, 3), (2, 2)]):
        a_ref[k] = added(keep_ref, other_ref, upper, slice(0, rows)).astype(bf16)
        b_ref[k] = added(keep_ref, other_ref, lower, slice(rows, 2 * rows)).astype(bf16)


def kept_sum(keep_ref, other_ref, own_ref, next_ref):
    rows = own_ref.shape[0] // 2
    for here, part in [(slice(0, rows), 3), (slice(rows, 2 * rows), 1)]:
        own_ref[here] = added(keep_ref, other_ref, 0, here)
        next_ref[here] = added(keep_ref, other_ref, part, here)


def second_sum(own_ref, next_ref, a_ref, b_ref, out_ref, a_out_ref, b_out_ref):
    rows = a_ref.shape[1]
    upper, lower = slice(0, rows), slice(rows, 2 * rows)
    a_out_ref[...] = (next_ref[upper] + a_ref[1].astype(f32)).astype(bf16)
    b_out_ref[...] = (next_ref[lower] + b_ref[1].astype(f32)).astype(bf16)
    out_ref[upper] = own_ref[upper] + a_ref[0].astype(f32)
    out_ref[lower] = own_ref[lower] + b_ref[0].astype(f32)


def third_sum(y_shift, own_ref, a_ref, b_ref, a_out_ref, b_out_ref, own_out_ref, next_ref, all_ref):
    rows = a_ref.shape[0]
    count, deep = all_ref.shape[:2]
    me = lax.axis_index("space") >> y_shift
    for y in range(count):
        came = a_ref if y * deep < rows else b_ref
        at = y * deep % rows
        all_ref[y ^ me] = own_ref[y * deep : (y + 1) * deep] + came[at : at + deep].astype(f32)
    upper, lower = slice(0, deep // 2), slice(deep // 2, deep)
    for k, (one, two) in enumerate([(1, 3), (2, 2)]):
        a_out_ref[k] = all_ref[one, upper].astype(bf16)
        b_out_ref[k] = all_ref[two, lower].astype(bf16)
    own_out_ref[...] = all_ref[0]
    next_ref[upper] = all_ref[3, upper]
    next_ref[lower] = all_ref[1, lower]


def y_sum(own_ref, a_ref, b_ref, out_ref):
    came = jnp.concatenate([a_ref[...].astype(f32), b_ref[...].astype(f32)], axis=0)
    total = (own_ref[...] + came).astype(bf16)
    for z in range(out_ref.shape[1]):
        for h in range(out_ref.shape[0]):
            out_ref[h, z] = total[8 * z : 8 * z + 8]


def z_sum(parts_ref, out_ref):
    out_ref[...] = jnp.sum(parts_ref[...].astype(f32), axis=0)


def last_sum(dims, scale, *refs):
    ch, lid, cam = dims
    *parts, wa_ref, wb_ref, all_ref = refs
    column_place = lax.axis_index("scene") >> 1
    for k, part in enumerate(parts):
        all_ref[k ^ column_place] = part[...]
    whole = jnp.concatenate([all_ref[x] for x in range(len(parts))], axis=1) * scale
    wb_ref[...] = whole[:, : 9 * ch]
    pieces = []
    for tap in range(9):
        at = 9 * (ch + lid) + tap * cam
        pieces += [whole[:, at : at + cam], whole[:, 9 * ch + tap * lid : 9 * ch + (tap + 1) * lid]]
    wa_ref[...] = jnp.concatenate(pieces, axis=1)


def call(kernel, outs, scratch, args, specs, flops, traffic, outs_at=None, limit=24):
    return pl.pallas_call(
        kernel,
        out_shape=outs,
        in_specs=specs,
        out_specs=outs_at or [VM] * len(outs),
        scratch_shapes=scratch,
        cost_estimate=pl.CostEstimate(flops=flops, bytes_accessed=traffic, transcendentals=0),
        compiler_params=pltpu.CompilerParams(vmem_limit_bytes=limit << 20),
    )(*[pltpu.with_memory_space_constraint(x, pltpu.HBM) if spec is HB else x for x, spec in zip(args, specs)])


def small(kernel, outs, args):
    outs = [jax.ShapeDtypeStruct(shape, dtype) for shape, dtype in outs]
    traffic = sum(x.size * x.dtype.itemsize for x in (*args, *outs))
    return call(kernel, outs, [], args, [VM] * len(args), traffic, traffic)


VM = pl.BlockSpec(memory_space=pltpu.VMEM)
SM = pl.BlockSpec(memory_space=pltpu.SMEM)
HB = pl.BlockSpec(memory_space=pltpu.HBM)


def exchanged(x, axis, groups):
    return lax.all_to_all(x, axis, 0, 0, axis_index_groups=groups, tiled=True)


def swapped(x, axis, partner):
    return lax.ppermute(x, axis, [(i, partner(i)) for i in range(lax.axis_size(axis))])


def summed_along_x(keep, send):
    _, rows, per_part = keep.shape
    deep = rows // 2
    other = swapped(send, "space", lambda i: i ^ 1)
    a, b = small(first_sum, [((2, deep, per_part), bf16)] * 2, (keep, other))
    a, b = swapped(a, "scene", lambda i: i ^ 2), swapped(b, "scene", lambda i: i ^ 6)
    kept = small(kept_sum, [((2 * deep, per_part), f32)] * 2, (keep, other))
    own, a, b = small(
        second_sum,
        [((2 * deep, per_part), f32), ((deep, per_part), bf16), ((deep, per_part), bf16)],
        (*kept, a, b),
    )
    a, b = swapped(a, "scene", lambda i: i ^ 6), swapped(b, "scene", lambda i: i ^ 2)
    return own, a, b


def summed_along_y(own, a, b, row):
    rows, per_part = own.shape
    deep = rows // 4
    halves = [((2, deep // 2, per_part), bf16)] * 2 + [((deep, per_part), f32)] * 2
    a, b, *kept = call(
        functools.partial(third_sum, row.bit_length() - 1),
        [jax.ShapeDtypeStruct(*spec) for spec in halves],
        [pltpu.VMEM((4, deep, per_part), f32)],
        (own, a, b),
        [VM] * 3,
        2_000_000,
        2_000_000,
    )
    a, b = swapped(a, "space", lambda i: i ^ row), swapped(b, "space", lambda i: i ^ 3 * row)
    own, a, b = small(
        second_sum,
        [((deep, per_part), f32), ((deep // 2, per_part), bf16), ((deep // 2, per_part), bf16)],
        (*kept, a, b),
    )
    a, b = swapped(a, "space", lambda i: i ^ 3 * row), swapped(b, "space", lambda i: i ^ row)
    (spread,) = small(y_sum, [((2, deep // 8, 8, per_part), bf16)], (own, a, b))
    return spread


def along_x(own, dims, scale):
    ch, lid, cam = dims
    parts = [own]
    for k in range(1, 4):
        parts.append(swapped(own, "scene", lambda i: i ^ 2 * k))
    return call(
        functools.partial(last_sum, dims, scale),
        [jax.ShapeDtypeStruct((8, 9 * width), f32) for width in (cam + lid, ch)],
        [pltpu.VMEM((len(parts), *own.shape), f32)],
        parts,
        [VM] * len(parts),
        400_000,
        400_000,
    )


def shards(
    grad_out, pre_second, pre_first, camera_bev, lidar_bev, weight_a, weight_b,
    depth_weights, context, block_list, point_slot,
):
    _, rows, cols, ch = grad_out.shape
    cam, lid = camera_bev.shape[-1], lidar_bev.shape[-1]
    space, scenes = lax.axis_size("space"), lax.axis_size("scene")
    pix = point_slot.shape[1]
    place = space // 2
    reach = scenes // 2
    scale = 1.0 / math.sqrt(rows * cols * space * scenes)
    first = pre_first[0]
    shape = jax.ShapeDtypeStruct
    near, far = call(
        halo_kernel,
        [shape((k, cols, ch), bf16) for k in (rows + 1, rows + 1)],
        [pltpu.VMEM(first.shape, bf16)] * 3 + [pltpu.SemaphoreType.DMA((3,))],
        (grad_out[0], pre_second[0], first),
        [HB] * 3,
        1_000_000,
        1_000_000,
    )
    sides = [(i, i + 1) for i in range(1, space - 1, 2)]
    far = lax.ppermute(far, "space", sides + [(j, i) for i, j in sides])
    near = swapped(near, "space", lambda i: i ^ 1)
    camera = jnp.swapaxes(camera_bev[0], 1, 2)
    tiles = 9 * (ch + lid) // TILE + -(-9 * cam // TILE)
    per_part = -(-tiles // reach) * TILE
    start, gt_own, wb = call(
        functools.partial(own_kernel, cols),
        [
            pltpu.VMEM((4 * cols, ch), f32),
            pltpu.VMEM((3, ch, rows * cols), bf16),
            pltpu.VMEM(weight_b.shape, bf16),
        ],
        [
            pltpu.VMEM(first.shape, bf16),
            pltpu.VMEM(first.shape, bf16),
            pltpu.VMEM((3, rows * cols, ch), bf16),
            pltpu.SemaphoreType.DMA((3,)),
        ],
        (grad_out[0], pre_second[0], weight_b),
        [HB] * 3,
        300_000_000,
        2_500_000,
    )
    lidar, blocks, keep, send = call(
        functools.partial(local_kernel, (cols, ch, cam, reach)),
        [
            pltpu.HBM((rows, cols, lid), bf16),
            pltpu.HBM((space, cam, cols), bf16),
            shape((reach, ch // 2, per_part), bf16),
            pltpu.HBM((reach, ch // 2, per_part), bf16),
        ],
        [
            pltpu.VMEM((3, 2 * cols, ch), bf16),
            pltpu.VMEM((3, 2 * cols, ch), bf16),
            pltpu.VMEM((3, 4 * cols, ch), bf16),
            pltpu.VMEM((3, ch, 4 * cols), bf16),
            pltpu.VMEM((3, ch, 4 * cols), bf16),
            pltpu.VMEM(first.shape, bf16),
            pltpu.VMEM((rows, cols, lid), bf16),
            pltpu.VMEM(camera.shape, bf16),
            pltpu.VMEM(weight_a.shape[::-1], bf16),
            pltpu.SMEM((space,), jnp.int32),
            pltpu.VMEM((2, cam, cols), bf16),
            pltpu.VMEM((rows, cols, lid), bf16),
            pltpu.VMEM((reach, ch // 2, per_part), bf16),
            pltpu.SemaphoreType.DMA((space,)),
            pltpu.SemaphoreType.DMA((reach + 1,)),
            pltpu.SemaphoreType.DMA((5,)),
        ],
        (near, far, start, gt_own, wb, first, lidar_bev[0], camera, weight_a.T, block_list[:, 0, 0]),
        [VM] * 5 + [HB] * 5,
        1_500_000_000,
        12_000_000,
        outs_at=[HB, HB, VM, HB],
    )
    incoming = exchanged(blocks, "space", None)
    table = pltpu.VMEM((space * (pix + 8), cols), f32)
    (mass,) = call(
        mass_kernel,
        [shape((space, pix, cols), bf16)],
        [pltpu.VMEM((pix, 128), f32), pltpu.VMEM((pix, 128), jnp.int32), table],
        (depth_weights[0], point_slot),
        [VM] * 2,
        500_000_000,
        2_000_000,
    )
    deep = place // reach
    spread = summed_along_y(*summed_along_x(keep, send), 2 * deep)
    incoming, spread = lax.optimization_barrier((incoming, spread))
    grad_context, grad_depth = call(
        depth_kernel,
        [shape((cam, pix), f32), shape(point_slot.shape, f32)],
        [pltpu.VMEM((pix, 128), jnp.int32), table, pltpu.VMEM((pix, 128), f32)],
        (incoming, mass, context[0], point_slot),
        [VM] * 4,
        1_500_000_000,
        2_000_000,
    )
    along_z = lax.all_to_all(
        spread.reshape(2 * deep, 8, per_part),
        ("space", "scene"),
        0,
        0,
        axis_index_groups=[
            [((y * deep + z) * 2 + c) * scenes + 2 * x + h for h in range(2) for z in range(deep)]
            for y in range(reach)
            for c in range(2)
            for x in range(reach)
        ],
        tiled=True,
    )
    along_z, grad_context, grad_depth = lax.optimization_barrier((along_z, grad_context, grad_depth))
    (own,) = small(z_sum, [((8, per_part), f32)], (along_z,))
    grad_wa, grad_wb = along_x(own, (ch, lid, cam), scale)
    return grad_wa, grad_wb, lidar[None], grad_context[None], grad_depth[None]


def solution(mesh):
    field = P("scene", "space", None, None)
    pixels = P("scene", None, "space")
    return jax.shard_map(
        shards,
        mesh=mesh,
        in_specs=(field,) * 5 + (P(), P(), pixels, pixels, P(None, "space", None), P(None, "space")),
        out_specs=(P("space", None), P("space", None), field, pixels, pixels),
        check_vma=False,
    )
```

```python
import functools
import math

import jax
import jax.numpy as jnp
from jax import lax
from jax.experimental import pallas as pl
from jax.experimental.pallas import tpu as pltpu
from jax.sharding import PartitionSpec as P


f32 = jnp.float32
bf16 = jnp.bfloat16
NN = (((1,), (0,)), ((), ()))
NT = (((1,), (1,)), ((), ()))


def mm(a, b, dims):
    return lax.dot_general(a, b, dims, preferred_element_type=f32)


def shifted_columns(rows, step, cols):
    if step == 0:
        return rows
    zero = jnp.zeros((1, rows.shape[1]), rows.dtype)
    out = []
    for r in range(rows.shape[0] // cols):
        row = rows[r * cols : (r + 1) * cols]
        out += [row[1:], zero] if step > 0 else [zero, row[:-1]]
    return jnp.concatenate(out, axis=0)


TILE = 128


def started(sources, targets, sems):
    moves = [pltpu.make_async_copy(source, target, sems.at[k]) for k, (source, target) in enumerate(zip(sources, targets))]
    for move in moves:
        move.start()
    return moves


def passed(grad_ref, second_ref):
    return jnp.where(second_ref[...].astype(f32) > 0, grad_ref[...].astype(f32), 0.0).astype(bf16)


def halo_kernel(grad_hbm, second_hbm, first_hbm, near_ref, far_ref, grad_ref, second_ref, first_ref, sems):
    for move in started((grad_hbm, second_hbm, first_hbm), (grad_ref, second_ref, first_ref), sems):
        move.wait()
    rows = first_ref.shape[0]
    odd = lax.axis_index("space") & 1
    grad_b = passed(grad_ref, second_ref)
    near_ref[:rows] = grad_b
    far_ref[:rows] = grad_b
    near_ref[rows] = first_ref[(rows - 1) * (1 - odd)]
    far_ref[rows] = first_ref[(rows - 1) * odd]


def back_weight(wb_ref, a, b):
    ch = wb_ref.shape[0]
    tap = (3 * (2 - a) + (2 - b)) * ch
    return wb_ref[:, tap : tap + ch]


def own_kernel(cols, grad_hbm, second_hbm, wb_hbm, start_ref, gt_ref, wb_ref, grad_ref, second_ref, g_ref, sems):
    moves = started((grad_hbm, second_hbm, wb_hbm), (grad_ref, second_ref, wb_ref), sems)
    moves[0].wait()
    moves[1].wait()
    own = passed(grad_ref, second_ref)
    own = jnp.concatenate([own[0], own[1]], axis=0).astype(f32)
    for b in range(3):
        g_ref[b] = shifted_columns(own, b - 1, cols).astype(bf16)
        gt_ref[b] = g_ref[b].T
    moves[2].wait()
    low, middle, high = [
        sum(mm(g_ref[b], back_weight(wb_ref, a, b), NN) for b in range(3)) for a in (2, 1, 0)
    ]
    start_ref[0:cols] = low[:cols]
    start_ref[cols : 2 * cols] = low[cols:] + middle[:cols]
    start_ref[2 * cols : 3 * cols] = middle[cols:] + high[:cols]
    start_ref[3 * cols :] = high[cols:]


def local_kernel(dims, near_ref, far_ref, start_ref, gt_own_ref, wb_ref, first_hbm, lid_hbm, cam_hbm, wa_hbm, list_hbm,
                 lidar_hbm, blocks_hbm, keep_ref, send_hbm,
                 gb_ref, ga_ref, a_ref, gt_ref, at_ref, first_ref, lid_ref, cam_ref, wa_ref, list_ref,
                 pick_ref, lidar_ref, send_ref, block_sems, out_sems, in_sems):
    cols, ch, cam, parts = dims
    lid = lid_ref.shape[2]
    fan = cam + lid
    half = ch // 2
    moves = started(
        (first_hbm, wa_hbm, list_hbm, lid_hbm, cam_hbm), (first_ref, wa_ref, list_ref, lid_ref, cam_ref), in_sems
    )
    second_core = (lax.axis_index("space") & 1) > 0
    column_place = lax.axis_index("scene") >> 1
    near = [near_ref[k].astype(f32) for k in range(3)]
    far = [far_ref[k].astype(f32) for k in range(3)]
    before = [jnp.where(second_core, n, f) for n, f in zip(near, far)]
    after = [jnp.where(second_core, f, n) for n, f in zip(near, far)]
    two_before = jnp.concatenate(before[:2], axis=0)
    two_after = jnp.concatenate(after[:2], axis=0)
    for b in range(3):
        gb_ref[b] = shifted_columns(two_before, b - 1, cols).astype(bf16)
        ga_ref[b] = shifted_columns(two_after, b - 1, cols).astype(bf16)
        gt_ref[b, :, :cols] = gb_ref[b, cols:, :].T
        gt_ref[b, :, cols : 3 * cols] = gt_own_ref[b]
        gt_ref[b, :, 3 * cols :] = ga_ref[b, :cols, :].T
    up = sum(mm(gb_ref[b], back_weight(wb_ref, 0, b), NN) for b in range(3))
    up_edge = sum(mm(gb_ref[b, cols:, :], back_weight(wb_ref, 1, b), NN) for b in range(3))
    down = sum(mm(ga_ref[b], back_weight(wb_ref, 2, b), NN) for b in range(3))
    down_edge = sum(mm(ga_ref[b, :cols, :], back_weight(wb_ref, 1, b), NN) for b in range(3))
    back = start_ref[...] + jnp.concatenate(
        [up[:cols] + up_edge, up[cols:], down[:cols], down[cols:] + down_edge], axis=0
    )
    moves[0].wait()
    first = jnp.concatenate([before[2], first_ref[0].astype(f32), first_ref[1].astype(f32), after[2]], axis=0)
    grad_a = jnp.where(first > 0, back, 0.0).astype(bf16).astype(f32)
    for b in range(3):
        moved = shifted_columns(grad_a, b - 1, cols)
        a_ref[b] = moved.astype(bf16)
        at_ref[b] = moved.astype(bf16).T
    moves[1].wait()
    lidar = jnp.zeros((2 * cols, lid), f32)
    camera = jnp.zeros((cam, 2 * cols), f32)
    for a in range(3):
        for b in range(3):
            tap = (3 * (2 - a) + (2 - b)) * fan
            rows = a_ref[b, a * cols : (a + 2) * cols, :]
            lidar += mm(rows, wa_ref[tap + cam : tap + fan, :], NT)
            camera += mm(wa_ref[tap : tap + cam, :], rows, NT)
    for r in range(2):
        lidar_ref[r] = lidar[r * cols : (r + 1) * cols].astype(bf16)
    leaving = [pltpu.make_async_copy(lidar_ref, lidar_hbm, out_sems.at[parts])]
    leaving[0].start()
    for r in range(2):
        pick_ref[r] = camera[:, r * cols : (r + 1) * cols].astype(bf16)
    moves[2].wait()
    picks = [
        pltpu.make_async_copy(pick_ref.at[jnp.where(list_ref[k] > 0, 1, 0)], blocks_hbm.at[k], block_sems.at[k])
        for k in range(blocks_hbm.shape[0])
    ]
    for pick in picks:
        pick.start()

    moves[3].wait()
    moves[4].wait()
    per_part = keep_ref.shape[2] // TILE

    def put(value, tile):
        halves = value.reshape(ch // 16, 2, 8, value.shape[1])
        even = halves[:, 0].reshape(half, value.shape[1])
        odd = halves[:, 1].reshape(half, value.shape[1])
        mine = jnp.where(second_core, odd, even).astype(bf16)
        other = jnp.where(second_core, even, odd).astype(bf16)
        for t in range(value.shape[1] // TILE):
            part, at = divmod(tile + t, per_part)
            part = part ^ column_place
            here = slice(at * TILE, (at + 1) * TILE)
            keep_ref[part, :, here] = mine[:, t * TILE : (t + 1) * TILE]
            send_ref[part, :, here] = other[:, t * TILE : (t + 1) * TILE]

    hidden = jnp.maximum(jnp.concatenate([first_ref[0], first_ref[1]], axis=0), 0)
    lidar_in = jnp.concatenate([lid_ref[0], lid_ref[1]], axis=0)
    camera_in = jnp.concatenate([cam_ref[0], cam_ref[1]], axis=1)
    b_tiles, a_tiles = ch // TILE, lid // TILE
    windows = [(2 - b, slice((2 - a) * cols, (4 - a) * cols)) for a in range(3) for b in range(3)]

    def leave(first_part, end):
        for part in range(first_part, end):
            place = part ^ column_place
            leaving.append(pltpu.make_async_copy(send_ref.at[place], send_hbm.at[place], out_sems.at[part]))
            leaving[-1].start()

    for tap, (b, window) in enumerate(windows):
        put(mm(gt_ref[b, :, window], hidden, NN), tap * b_tiles)
    gone = 9 * b_tiles // per_part
    leave(0, gone)
    for tap, (b, window) in enumerate(windows):
        put(mm(at_ref[b, :, window], lidar_in, NN), 9 * b_tiles + tap * a_tiles)
    at = 9 * (b_tiles + a_tiles)
    leave(gone, at // per_part)
    packed = [mm(at_ref[b, :, window], camera_in, NT) for b, window in windows]
    spare = (parts * per_part - at) * TILE - 9 * cam
    packed.append(jnp.zeros((ch, spare), f32))
    put(jnp.concatenate(packed, axis=1), at)
    leave(at // per_part, parts)
    for move in leaving:
        move.wait()
    for pick in picks:
        pick.wait()


def depth_kernel(blocks_ref, weight_ref, context_ref, slot_ref, gc_ref, gd_ref, wt_ref, st_ref, s_ref, m_ref, d_ref):
    sources, cam, cells_of = blocks_ref.shape
    depth, pix = slot_ref.shape
    wide = st_ref.shape[1]
    wt_ref[...] = jnp.concatenate([weight_ref[...].astype(f32), jnp.zeros((wide - depth, pix), f32)], axis=0).T
    st_ref[...] = jnp.concatenate([slot_ref[...], jnp.full((wide - depth, pix), -1, jnp.int32)], axis=0).T
    context_t = context_ref[...].astype(f32).T.astype(bf16)
    pitch = s_ref.shape[0] // sources
    for s in range(sources):
        s_ref[s * pitch : s * pitch + pix, :] = mm(context_t, blocks_ref[s], NN)
    cells = lax.broadcasted_iota(jnp.int32, (cells_of, wide), 0)
    places = lax.broadcasted_iota(jnp.int32, (sources, wide), 0)
    shift = cells_of.bit_length() - 1

    def pixels(g, carry):
        base = pl.multiple_of(g * 8, 8)
        slots = st_ref[pl.ds(base, 8), :]
        weights = wt_ref[pl.ds(base, 8), :]
        found_rows = []
        for k in range(8):
            slot = slots[k : k + 1]
            at_cell = jnp.where(cells == (slot & (cells_of - 1)), 1.0, 0.0).astype(bf16)
            here = places == (slot >> shift)
            every = pl.ds(base + k, sources, stride=pitch)
            m_ref[every, :] = mm(jnp.where(here, weights[k : k + 1], 0.0).astype(bf16), at_cell, NT)
            found = mm(s_ref[every, :].astype(bf16), at_cell, NN)
            found_rows.append(jnp.sum(jnp.where(here, found, 0.0), axis=0, keepdims=True))
        d_ref[pl.ds(base, 8), :] = jnp.concatenate(found_rows, axis=0)
        return carry

    lax.fori_loop(0, pix // 8, pixels, 0, unroll=2)
    gd_ref[...] = d_ref[...].T[:depth]
    total = jnp.zeros((cam, pix), f32)
    for s in range(sources):
        total += mm(blocks_ref[s], m_ref[s * pitch : s * pitch + pix, :].astype(bf16), NT)
    gc_ref[...] = total


def added(keep_ref, other_ref, part, rows):
    return keep_ref[part, rows].astype(f32) + other_ref[part, rows].astype(f32)


def first_sum(keep_ref, other_ref, a_ref, b_ref):
    rows = a_ref.shape[1]
    for k, (upper, lower) in enumerate([(1, 3), (2, 2)]):
        a_ref[k] = added(keep_ref, other_ref, upper, slice(0, rows)).astype(bf16)
        b_ref[k] = added(keep_ref, other_ref, lower, slice(rows, 2 * rows)).astype(bf16)


def kept_sum(keep_ref, other_ref, own_ref, next_ref):
    rows = own_ref.shape[0] // 2
    for here, part in [(slice(0, rows), 3), (slice(rows, 2 * rows), 1)]:
        own_ref[here] = added(keep_ref, other_ref, 0, here)
        next_ref[here] = added(keep_ref, other_ref, part, here)


def second_sum(first_row, own_ref, next_ref, came_ref, out_ref, send_ref):
    here = slice(first_row, first_row + out_ref.shape[0])
    send_ref[...] = (next_ref[here] + came_ref[1].astype(f32)).astype(bf16)
    out_ref[...] = own_ref[here] + came_ref[0].astype(f32)


def third_sum(own_a_ref, own_b_ref, a_ref, b_ref, out_ref):
    rows = a_ref.shape[0]
    out_ref[:rows] = (own_a_ref[...] + a_ref[...].astype(f32)).astype(bf16)
    out_ref[rows:] = (own_b_ref[...] + b_ref[...].astype(f32)).astype(bf16)


def place_sum(parts_ref, out_ref):
    out_ref[...] = jnp.sum(parts_ref[...].astype(f32), axis=0).astype(bf16)


def pair_sum(one_ref, two_ref, out_ref):
    out_ref[...] = one_ref[...].astype(f32) + two_ref[...].astype(f32)


def last_sum(dims, scale, *refs):
    ch, lid, cam = dims
    *parts, wa_ref, wb_ref, all_ref = refs
    column_place = lax.axis_index("scene") >> 1
    for k, part in enumerate(parts):
        all_ref[k ^ column_place] = part[...]
    whole = jnp.concatenate([all_ref[x] for x in range(len(parts))], axis=1) * scale
    wb_ref[...] = whole[:, : 9 * ch]
    pieces = []
    for tap in range(9):
        at = 9 * (ch + lid) + tap * cam
        pieces += [whole[:, at : at + cam], whole[:, 9 * ch + tap * lid : 9 * ch + (tap + 1) * lid]]
    wa_ref[...] = jnp.concatenate(pieces, axis=1)


def call(kernel, outs, scratch, args, specs, flops, traffic, outs_at=None, limit=24):
    return pl.pallas_call(
        kernel,
        out_shape=outs,
        in_specs=specs,
        out_specs=outs_at or [VM] * len(outs),
        scratch_shapes=scratch,
        cost_estimate=pl.CostEstimate(flops=flops, bytes_accessed=traffic, transcendentals=0),
        compiler_params=pltpu.CompilerParams(vmem_limit_bytes=limit << 20),
    )(*[pltpu.with_memory_space_constraint(x, pltpu.HBM) if spec is HB else x for x, spec in zip(args, specs)])


def small(kernel, outs, args):
    outs = [jax.ShapeDtypeStruct(shape, dtype) for shape, dtype in outs]
    traffic = sum(x.size * x.dtype.itemsize for x in (*args, *outs))
    return call(kernel, outs, [], args, [VM] * len(args), traffic, traffic)


VM = pl.BlockSpec(memory_space=pltpu.VMEM)
SM = pl.BlockSpec(memory_space=pltpu.SMEM)
HB = pl.BlockSpec(memory_space=pltpu.HBM)


def exchanged(x, axis, groups):
    return lax.all_to_all(x, axis, 0, 0, axis_index_groups=groups, tiled=True)


def swapped(x, axis, partner):
    return lax.ppermute(x, axis, [(i, partner(i)) for i in range(lax.axis_size(axis))])


def summed_along_x(keep, send):
    _, rows, per_part = keep.shape
    deep = rows // 2
    other = swapped(send, "space", lambda i: i ^ 1)
    a, b = small(first_sum, [((2, deep, per_part), bf16)] * 2, (keep, other))
    a = swapped(a, "scene", lambda i: i ^ 2)
    b = swapped(b, "scene", lambda i: i ^ 6)
    kept = small(kept_sum, [((2 * deep, per_part), f32)] * 2, (keep, other))
    halves = [((deep, per_part), f32), ((deep, per_part), bf16)]
    own_a, a = small(functools.partial(second_sum, 0), halves, (*kept, a))
    a = swapped(a, "scene", lambda i: i ^ 6)
    own_b, b = small(functools.partial(second_sum, deep), halves, (*kept, b))
    b = swapped(b, "scene", lambda i: i ^ 2)
    (part,) = small(third_sum, [((2 * deep, per_part), bf16)], (own_a, own_b, a, b))
    return part


def over_scenes(part, dims, scale):
    ch, lid, cam = dims
    (own,) = small(pair_sum, [(part.shape, f32)], (part, swapped(part, "scene", lambda i: i ^ 1)))
    parts = [own]
    for k in range(1, 4):
        parts.append(swapped(own, "scene", lambda i: i ^ 2 * k))
    return call(
        functools.partial(last_sum, dims, scale),
        [jax.ShapeDtypeStruct((8, 9 * width), f32) for width in (cam + lid, ch)],
        [pltpu.VMEM((len(parts), *own.shape), f32)],
        parts,
        [VM] * len(parts),
        400_000,
        400_000,
    )


def shards(
    grad_out, pre_second, pre_first, camera_bev, lidar_bev, weight_a, weight_b,
    depth_weights, context, block_list, point_slot,
):
    _, rows, cols, ch = grad_out.shape
    cam, lid = camera_bev.shape[-1], lidar_bev.shape[-1]
    space, scenes = lax.axis_size("space"), lax.axis_size("scene")
    pix = point_slot.shape[1]
    place = space // 2
    reach = scenes // 2
    scale = 1.0 / math.sqrt(rows * cols * space * scenes)
    first = pre_first[0]
    shape = jax.ShapeDtypeStruct
    near, far = call(
        halo_kernel,
        [shape((k, cols, ch), bf16) for k in (rows + 1, rows + 1)],
        [pltpu.VMEM(first.shape, bf16)] * 3 + [pltpu.SemaphoreType.DMA((3,))],
        (grad_out[0], pre_second[0], first),
        [HB] * 3,
        1_000_000,
        1_000_000,
    )
    sides = [(i, i + 1) for i in range(1, space - 1, 2)]
    far = lax.ppermute(far, "space", sides + [(j, i) for i, j in sides])
    near = swapped(near, "space", lambda i: i ^ 1)
    camera = jnp.swapaxes(camera_bev[0], 1, 2)
    tiles = 9 * (ch + lid) // TILE + -(-9 * cam // TILE)
    per_part = -(-tiles // reach) * TILE
    start, gt_own, wb = call(
        functools.partial(own_kernel, cols),
        [
            pltpu.VMEM((4 * cols, ch), f32),
            pltpu.VMEM((3, ch, rows * cols), bf16),
            pltpu.VMEM(weight_b.shape, bf16),
        ],
        [
            pltpu.VMEM(first.shape, bf16),
            pltpu.VMEM(first.shape, bf16),
            pltpu.VMEM((3, rows * cols, ch), bf16),
            pltpu.SemaphoreType.DMA((3,)),
        ],
        (grad_out[0], pre_second[0], weight_b),
        [HB] * 3,
        300_000_000,
        2_500_000,
    )
    lidar, blocks, keep, send = call(
        functools.partial(local_kernel, (cols, ch, cam, reach)),
        [
            pltpu.HBM((rows, cols, lid), bf16),
            pltpu.HBM((space, cam, cols), bf16),
            shape((reach, ch // 2, per_part), bf16),
            pltpu.HBM((reach, ch // 2, per_part), bf16),
        ],
        [
            pltpu.VMEM((3, 2 * cols, ch), bf16),
            pltpu.VMEM((3, 2 * cols, ch), bf16),
            pltpu.VMEM((3, 4 * cols, ch), bf16),
            pltpu.VMEM((3, ch, 4 * cols), bf16),
            pltpu.VMEM((3, ch, 4 * cols), bf16),
            pltpu.VMEM(first.shape, bf16),
            pltpu.VMEM((rows, cols, lid), bf16),
            pltpu.VMEM(camera.shape, bf16),
            pltpu.VMEM(weight_a.shape[::-1], bf16),
            pltpu.SMEM((space,), jnp.int32),
            pltpu.VMEM((2, cam, cols), bf16),
            pltpu.VMEM((rows, cols, lid), bf16),
            pltpu.VMEM((reach, ch // 2, per_part), bf16),
            pltpu.SemaphoreType.DMA((space,)),
            pltpu.SemaphoreType.DMA((reach + 1,)),
            pltpu.SemaphoreType.DMA((5,)),
        ],
        (near, far, start, gt_own, wb, first, lidar_bev[0], camera, weight_a.T, block_list[:, 0, 0]),
        [VM] * 5 + [HB] * 5,
        1_500_000_000,
        12_000_000,
        outs_at=[HB, HB, VM, HB],
    )
    incoming = exchanged(blocks, "space", None)
    part = summed_along_x(keep, send)
    incoming, part = lax.optimization_barrier((incoming, part))
    along_yz = exchanged(
        part.reshape(place, 8, per_part), "space", [[2 * i + c for i in range(place)] for c in range(2)]
    )
    grad_context, grad_depth = call(
        depth_kernel,
        [shape((cam, pix), f32), shape(point_slot.shape, f32)],
        [
            pltpu.VMEM((pix, 128), f32),
            pltpu.VMEM((pix, 128), jnp.int32),
            pltpu.VMEM((space * (pix + 8), cols), f32),
            pltpu.VMEM((space * (pix + 8), cols), f32),
            pltpu.VMEM((pix, 128), f32),
        ],
        (incoming, depth_weights[0], context[0], point_slot),
        [VM] * 4,
        2_000_000_000,
        2_000_000,
    )
    along_yz, grad_context, grad_depth = lax.optimization_barrier((along_yz, grad_context, grad_depth))
    (part,) = small(place_sum, [((8, per_part), bf16)], (along_yz,))
    grad_wa, grad_wb = over_scenes(part, (ch, lid, cam), scale)
    return grad_wa, grad_wb, lidar[None], grad_context[None], grad_depth[None]


def solution(mesh):
    field = P("scene", "space", None, None)
    pixels = P("scene", None, "space")
    return jax.shard_map(
        shards,
        mesh=mesh,
        in_specs=(field,) * 5 + (P(), P(), pixels, pixels, P(None, "space", None), P(None, "space")),
        out_specs=(P("space", None), P("space", None), field, pixels, pixels),
        check_vma=False,
    )
```
